256 devices in a mesh: section: 8 (over y, core), gx: 8 (over z), gy: 4 (over x).
Axes of the slice: x: 4, y: 4, z: 8, core: 2. Of those that a mesh axis runs over, the one named last changes fastest.
Arguments:
- load_index: int32 [8], P('section'), may hold values from 0 to 63
- load_table: float32 [64, 3], replicated, may hold values from -4 to 4
- toughness: float32 [8, 128, 64, 128], P('section', 'gx', 'gy'), may hold values from 0.3 to 3
- clamp_mask: int32 [128, 64, 128], P('gx', 'gy'), may hold values 0 or 1
- load_mask: int32 [128, 64, 128], P('gx', 'gy'), may hold values 0 or 1
- crack_mask: int32 [128, 64, 128], P('gx', 'gy'), may hold values 0 or 1
Outputs:
- displacement: float32 [8, 3, 128, 64, 128], P('section', None, 'gx', 'gy')
- damage: float32 [8, 128, 64, 128], P('section', 'gx', 'gy')
- section_residuals: float32 [8, 8], P('section')
The draws below stay inside these ranges and needn't reach their ends.
All inputs are finite; a program needn't handle non-finite values. No bound on the sum of `clamp_mask` or of `load_mask` or of `crack_mask` on one device may be relied on, other than what follows from the above.
Results may differ from the reference program's by a relative error of at most 0.0003.
Values sent between devices are 32-bit elements; how exact they have to be, the bound alone decides.
A program may use at most 64 MiB of HBM per device.

```python
import math
import jax
import jax.numpy as jnp
from jax import lax

CASE_DEV = 1
LOADS = 64
CASES = 8
SECTIONS = 8
NX = 128
NY = 64
NZ = 128
N_SECTION = 8


def with_ends(array, rng, low, high):
    dims = array.shape
    spot = [jax.random.randint(jax.random.fold_in(rng, axis), (), 0, dims[axis]) for axis in range(len(dims))]
    array = array.at[tuple(spot)].set(low)
    longest = dims.index(max(dims))
    spot[longest] = (spot[longest] + 1) % dims[longest]
    return array.at[tuple(spot)].set(high)


def steps_of(key, dims, cuts, least, high):
    def one(position, blocks):
        heights = jax.random.uniform(jax.random.fold_in(jax.random.fold_in(key, 6), position), (blocks,), jnp.float32, least / len(cuts), high / len(cuts))
        return jnp.repeat(jnp.exp(heights), dims[position] // blocks).reshape((-1,) + (1,) * (len(dims) - position - 1))

    level = one(*cuts[0])
    for cut in cuts[1:]:
        level = level * one(*cut)
    return level


def centred(stream_key, dims, scale, most, kind=jnp.bfloat16):
    values = jax.random.normal(stream_key, dims, jnp.float32) * scale
    return jnp.minimum(jnp.maximum(values, -most), most).astype(kind)


def setup_inputs(seed: int = 0) -> dict:
    keys = jax.random.split(jax.random.key(seed), 7)
    return {
        "load_index": with_ends(jax.random.randint(keys[0], (CASES,), 0, LOADS), jax.random.fold_in(keys[0], 1), 0, LOADS - 1).astype(jnp.int32),
        "load_table": centred(keys[1], (LOADS, 3), 1.0, 4.0, jnp.float32),
        "toughness": jnp.clip(jnp.exp(math.log(3.0) - 2.3025851 * jax.random.uniform(keys[2], (SECTIONS, NX, NY, NZ), jnp.float32) ** steps_of(keys[2], (SECTIONS, NX, NY, NZ), ((0, 8), (1, 8), (2, 4)), -0.2, 0.2)), 0.3, 3.0),
        "clamp_mask": with_ends((jax.random.randint(keys[3], (NX, NY, NZ), 0, 8) < 1).astype(jnp.int32), jax.random.fold_in(keys[3], 1), 0, 1),
        "load_mask": with_ends((jax.random.randint(keys[4], (NX, NY, NZ), 0, 8) < 1).astype(jnp.int32), jax.random.fold_in(keys[4], 1), 0, 1),
        "crack_mask": with_ends((jax.random.randint(keys[5], (NX, NY, NZ), 0, 32) < 1).astype(jnp.int32), jax.random.fold_in(keys[5], 1), 0, 1),
    }


lame_lambda = 1.0
shear_modulus = 1.0
relax_weight = 0.6
stiff_floor = 0.001
eigen_guard = 1e-08
neighbour_offsets = ((1, 0, 0), (-1, 0, 0), (0, 1, 0), (0, -1, 0), (0, 0, 1), (0, 0, -1))

def unit_offset(axis_index, sign):
    return tuple((sign if other == axis_index else 0 for other in range(3)))

def shifted(padded, offset):
    span_first = padded.shape[-3] - 2
    span_second = padded.shape[-2] - 2
    span_third = padded.shape[-1] - 2
    return padded[..., 1 + offset[0]:1 + offset[0] + span_first, 1 + offset[1]:1 + offset[1] + span_second, 1 + offset[2]:1 + offset[2] + span_third]

def component(field, index):
    return field[..., index, :, :, :]

def elastic_parts(moved_pad, damage_pad):
    stiff_pad = jnp.square(1.0 - damage_pad) + stiff_floor
    centre = shifted(stiff_pad, (0, 0, 0))
    current = shifted(moved_pad, (0, 0, 0))
    laplace = jnp.zeros_like(current)
    weights = jnp.zeros_like(centre)
    for offset in neighbour_offsets:
        face = 0.5 * (centre + shifted(stiff_pad, offset))
        weights = weights + face
        laplace = laplace + jnp.expand_dims(face, -4) * (shifted(moved_pad, offset) - current)
    divergence = jnp.zeros_like(centre)
    pairs = []
    for axis_index in range(3):
        forward = unit_offset(axis_index, 1)
        backward = unit_offset(axis_index, -1)
        part = component(moved_pad, axis_index)
        divergence = divergence + 0.5 * (shifted(part, forward) - shifted(part, backward))
        pairs.append(shifted(stiff_pad, forward) + shifted(stiff_pad, backward))
    flow = centre * divergence
    diagonal = shear_modulus * jnp.expand_dims(weights, -4) + 0.25 * (lame_lambda + shear_modulus) * jnp.stack(pairs, axis=-4)
    return (current, laplace, flow, diagonal)

def flow_gradient(flow_pad):
    parts = [0.5 * (shifted(flow_pad, unit_offset(axis_index, 1)) - shifted(flow_pad, unit_offset(axis_index, -1))) for axis_index in range(3)]
    return jnp.stack(parts, axis=-4)

def spectral_energy(strain_xx, strain_yy, strain_zz, strain_xy, strain_xz, strain_yz):
    middle_value = (strain_xx + strain_yy + strain_zz) / 3.0
    dev_xx = strain_xx - middle_value
    dev_yy = strain_yy - middle_value
    dev_zz = strain_zz - middle_value
    shear_sum = jnp.square(strain_xy) + jnp.square(strain_xz) + jnp.square(strain_yz)
    spread = jnp.square(dev_xx) + jnp.square(dev_yy) + jnp.square(dev_zz) + 2.0 * shear_sum
    radius = jnp.sqrt(spread / 6.0)
    guarded = spread / 6.0 + eigen_guard
    determinant = dev_xx * (dev_yy * dev_zz - jnp.square(strain_yz)) - strain_xy * (strain_xy * dev_zz - strain_yz * strain_xz) + strain_xz * (strain_xy * strain_yz - dev_yy * strain_xz)
    ratio = jnp.clip(determinant / (2.0 * guarded * jnp.sqrt(guarded)), -1.0, 1.0)
    angle = jnp.arccos(ratio) / 3.0
    largest = middle_value + 2.0 * radius * jnp.cos(angle)
    smallest = middle_value + 2.0 * radius * jnp.cos(angle + 2.0 * jnp.pi / 3.0)
    between = 3.0 * middle_value - largest - smallest
    positive = jnp.square(jax.nn.relu(largest)) + jnp.square(jax.nn.relu(between)) + jnp.square(jax.nn.relu(smallest))
    return 0.5 * lame_lambda * jnp.square(jax.nn.relu(3.0 * middle_value)) + shear_modulus * positive

def damage_update(moved_pad, damage_pad, toughness_cell, crack_cell):
    grads = [[0.5 * (shifted(component(moved_pad, first), unit_offset(second, 1)) - shifted(component(moved_pad, first), unit_offset(second, -1))) for second in range(3)] for first in range(3)]
    energy = spectral_energy(grads[0][0], grads[1][1], grads[2][2], 0.5 * (grads[0][1] + grads[1][0]), 0.5 * (grads[0][2] + grads[2][0]), 0.5 * (grads[1][2] + grads[2][1]))
    beside_all = jnp.zeros_like(energy)
    for offset in neighbour_offsets:
        beside_all = beside_all + shifted(damage_pad, offset)
    updated = (2.0 * energy + toughness_cell * beside_all) / (toughness_cell + 2.0 * energy + 6.0 * toughness_cell)
    return jnp.where(crack_cell > 0.5, 1.0, updated)

def pad_all(field):
    return jnp.pad(field, [(0, 0)] * (field.ndim - 3) + [(1, 1), (1, 1), (1, 1)])

def sweep(moved, damage, load_vector, toughness_cell, fixed, load, crack):
    damage_pad = pad_all(damage)
    current, laplace, flow, diagonal = elastic_parts(pad_all(moved), damage_pad)
    gradient = flow_gradient(pad_all(flow))
    residual = shear_modulus * laplace + (lame_lambda + shear_modulus) * gradient
    prescribed = load[None] * load_vector[:, None, None, None]
    relaxed = current + relax_weight * residual / diagonal
    new_moved = jnp.where(fixed[None] > 0.5, prescribed, relaxed)
    squares = jnp.sum((1.0 - fixed)[None] * jnp.square(residual))
    new_damage = damage_update(pad_all(new_moved), damage_pad, toughness_cell, crack)
    return (new_moved, new_damage, squares)

def reference(load_index, load_table, toughness, clamp_mask, load_mask, crack_mask):
    clamp = clamp_mask.astype(jnp.float32)
    load = load_mask.astype(jnp.float32)
    crack = crack_mask.astype(jnp.float32)
    fixed = jnp.maximum(clamp, load)
    cells = float(NX * NY * NZ)
    columns = jnp.arange(N_SECTION, dtype=jnp.int32)

    def one_case(item):
        case_index, table_row = item
        load_vector = load_table[table_row]
        home = (case_index // CASE_DEV).astype(jnp.int32)
        moved = load[None] * load_vector[:, None, None, None]
        norms = jnp.zeros((N_SECTION,), jnp.float32)

        def advance(round_index, carry):
            moved_now, damage_now, norms_now = carry
            section_index = ((home + round_index) % N_SECTION).astype(jnp.int32)
            field = lax.dynamic_index_in_dim(toughness, section_index, 0, keepdims=False)
            moved_next, damage_next, squares = sweep(moved_now, damage_now, load_vector, field, fixed, load, crack)
            entry = jnp.sqrt(squares / (3.0 * cells))
            norms_next = norms_now + (columns == section_index).astype(jnp.float32) * entry
            return (moved_next, damage_next, norms_next)
        return lax.fori_loop(0, N_SECTION, advance, (moved, crack, norms))
    moved, damage, norms = lax.map(one_case, (jnp.arange(CASES, dtype=jnp.int32), load_index))
    return (moved, damage, norms)
```

```python
import functools

import jax
import jax.numpy as jnp
from jax import lax
from jax.experimental import pallas as pl
from jax.experimental.pallas import tpu as pltpu
from jax.sharding import PartitionSpec as P

MESH = pl.DeviceIdType.MESH
relax_weight = 0.6
stiff_floor = 0.001
eigen_guard = 1e-08
outside_stiff = 1.001

cos_third = (
    0.8660254053677892, 0.166666399623719, -0.0481050217302989, 0.024608831949810825,
    -0.015124763172089219, 0.009420074574188678, -0.004972568153766589,
    0.0017909605462136829, -0.0003093201852607309,
)
sin_third = (
    0.49999999939158213, -0.038675031951822925, 0.015381770818675887, -0.00862700282428075,
    0.005525819902144846, -0.0035154216998851246, 0.0018763805597984632,
    -0.0006797757027300123, 0.00011778274999869613,
)

PITCH = 24
LEAD = 8
HALO = 2


def row_of(x, y):
    return (x + HALO) * PITCH + LEAD + y


def polynomial(coefficients, t):
    value = coefficients[-1]
    for coefficient in coefficients[-2::-1]:
        value = value * t + coefficient
    return value


def twice_energy(a, b, c, d, e, f):
    trace = a + b + c
    middle = trace * (1.0 / 3.0)
    a, b, c = a - middle, b - middle, c - middle
    dd, ee, ff = d * d, e * e, f * f
    spread = (a * a + b * b + c * c) * (1.0 / 6.0) + (dd + ee + ff) * (1.0 / 3.0)
    guarded = spread + 4.0 * eigen_guard
    determinant = a * (b * c - ff) - d * (d * c - f * e) + e * (d * f - b * e)
    inverse = lax.rsqrt(guarded)
    ratio = determinant * (0.5 * inverse) * (inverse * inverse)
    size = jnp.minimum(jnp.abs(ratio), 1.0)
    radius = jnp.sqrt(spread)
    first = radius * polynomial(cos_third, size)
    first = jnp.where(ratio < 0.0, -first, first)
    rest = radius * (1.7320508075688772 * jnp.sqrt(1.0 - size)) * polynomial(sin_third, size)
    largest = jnp.maximum(middle + 2.0 * first, 0.0)
    base = middle - first
    second = jnp.maximum(base + rest, 0.0)
    third = jnp.maximum(base - rest, 0.0)
    volume = jnp.maximum(trace, 0.0)
    energy = 0.25 * (volume * volume) + 0.5 * (
        largest * largest + second * second + third * third
    )
    return energy, trace


def kernel(
    sizes, bx, by, cells,
    index_ref, loads_ref, tough_ref, clamp_ref, load_ref, crack_ref,
    disp_ref, dam_ref, table_ref,
    u, df, kk, lf, clamp_v, load_v, crack_v, g,
    pa, ra, pb, rb, pc, rc, row_v, rows_v,
    local_sem, a_send, a_recv, b_send, b_recv, t_send, t_recv, s_send, s_recv,
):
    ns, nx, ny = sizes
    me_s = lax.axis_index("section")
    me_x = lax.axis_index("gx")
    me_y = lax.axis_index("gy")
    nz = u.shape[-1]
    rows = u.shape[1]

    copies = [
        pltpu.make_async_copy(source, target, local_sem.at[i])
        for i, (source, target) in enumerate(
            ((load_ref, load_v), (clamp_ref, clamp_v), (crack_ref, crack_v), (tough_ref, g.at[0]))
        )
    ]
    for copy in copies:
        copy.start()

    halo_pieces = [(i * PITCH, 8) for i in range(bx + 2 * HALO + 1)]
    halo_pieces += [(row_of(x, 0), by) for x in (-2, -1, bx, bx + 1)]
    for start, size in halo_pieces:
        for i in range(u.shape[0]):
            u[i, pl.ds(start, size), :] = jnp.zeros((size, nz), jnp.float32)
        for i in range(df.shape[0]):
            df[i, pl.ds(start, size), :] = jnp.zeros((size, nz), jnp.float32)
        lf[0, pl.ds(start, size), :] = jnp.zeros((size, nz), jnp.float32)
        lf[1, pl.ds(start, size), :] = jnp.ones((size, nz), jnp.float32)
        kk[pl.ds(start, size), :] = jnp.full((size, nz), outside_stiff, jnp.float32)

    def there(dx, dy):
        return (
            (me_x + dx >= 0) & (me_x + dx < nx) & (me_y + dy >= 0) & (me_y + dy < ny)
        )

    corners = ((-1, -1), (-1, 1), (1, -1), (1, 1))
    sides_x = ((-1, 0), (1, 0))
    sides_y = ((0, -1), (0, 1))
    neighbours = sides_x + sides_y + corners

    barrier = pltpu.get_barrier_semaphore()
    for dx, dy in neighbours:
        @pl.when(there(dx, dy))
        def _(dx=dx, dy=dy):
            pl.semaphore_signal(
                barrier, inc=1, device_id={"gx": me_x + dx, "gy": me_y + dy}, device_id_type=MESH
            )
    for r in range(1, ns):
        pl.semaphore_signal(
            barrier, inc=1, device_id={"section": lax.rem(me_s + r, ns)}, device_id_type=MESH
        )

    for i in (0, 1, 2):
        copies[i].wait()

    def begin(x, carry):
        here = pl.ds(row_of(x, 0), by)
        held = pl.ds(x * by, by)
        load = load_v[held, :].astype(jnp.float32)
        clamp = clamp_v[held, :].astype(jnp.float32)
        crack = crack_v[held, :].astype(jnp.float32)
        lf[0, here, :] = load
        lf[1, here, :] = jnp.maximum(load, clamp)
        df[0, here, :] = crack
        kk[here, :] = (1.0 - crack) * (1.0 - crack) + stiff_floor
        return carry

    lax.fori_loop(0, bx, begin, 0, unroll=4)

    across = 1 + (me_x > 0).astype(jnp.int32) + (me_x < nx - 1).astype(jnp.int32)
    along = 1 + (me_y > 0).astype(jnp.int32) + (me_y < ny - 1).astype(jnp.int32)
    pl.semaphore_wait(barrier, across * along - 1 + (ns - 1))

    def remote(source, target, send, recv, dx, dy):
        return pltpu.make_async_remote_copy(
            src_ref=source, dst_ref=target, send_sem=send, recv_sem=recv,
            device_id={"gx": me_x + dx, "gy": me_y + dy}, device_id_type=MESH,
        )

    def b_copies(field, base, q, dx, dy):
        found = []
        if dy == 0:
            for layer in range(HALO):
                x = layer if dx < 0 else bx - HALO + layer
                to = bx + layer if dx < 0 else layer - HALO
                i = (0 if dx < 0 else 2) + layer
                found.append(remote(
                    field.at[pl.ds(base, 2), pl.ds(row_of(x, 0), by), :],
                    field.at[pl.ds(base, 2), pl.ds(row_of(to, 0), by), :],
                    b_send.at[q, i], b_recv.at[q, i], dx, dy,
                ))
        elif dx == 0:
            i = 0 if dy < 0 else 1
            found.append(remote(
                pb.at[i], rb.at[q, i], b_send.at[q, 4 + i], b_recv.at[q, 4 + i], dx, dy,
            ))
        else:
            i = corners.index((dx, dy))
            found.append(remote(
                pc.at[i], rc.at[q, i], b_send.at[q, 6 + i], b_recv.at[q, 6 + i], dx, dy,
            ))
        return found

    order_b = corners + sides_x + sides_y

    def send_b(field, base, q, current):
        for i, (dx, dy) in enumerate(corners):
            row = row_of(0 if dx < 0 else bx - 1, 0 if dy < 0 else by - 1)
            if current is not None:
                for c in range(3):
                    pc[i, pl.ds(c, 1), :] = u[current * 3 + c, pl.ds(row, 1), :]
            for f in range(2):
                pc[i, pl.ds(3 + f, 1), :] = field[base + f, pl.ds(row, 1), :]
        for i in range(2):
            for f in range(2):
                for layer in range(HALO):
                    y = layer if i == 0 else by - HALO + layer
                    pb[i, f * HALO + layer] = field[
                        base + f, pl.ds(row_of(0, y), bx, stride=PITCH), :
                    ]
        for dx, dy in order_b:
            @pl.when(there(dx, dy))
            def _(dx=dx, dy=dy):
                for copy in b_copies(field, base, q, dx, dy):
                    copy.start()

    def sent_b(field, base, q):
        for dx, dy in order_b:
            @pl.when(there(dx, dy))
            def _(dx=dx, dy=dy):
                for copy in b_copies(field, base, q, dx, dy):
                    copy.wait_send()

    def take_b(field, base, q, current):
        for dx, dy in order_b:
            @pl.when(there(-dx, -dy))
            def _(dx=dx, dy=dy):
                for copy in b_copies(field, base, q, dx, dy):
                    copy.wait_recv()
                if dx == 0:
                    i = 0 if dy < 0 else 1
                    for f in range(2):
                        for layer in range(HALO):
                            y = by + layer if i == 0 else layer - HALO
                            strip = pl.ds(row_of(0, y), bx, stride=PITCH)
                            value = rb[q, i, f * HALO + layer]
                            field[base + f, strip, :] = value
                            if current is not None and f == 0:
                                kk[strip, :] = (1.0 - value) * (1.0 - value) + stiff_floor
                elif dy != 0:
                    i = corners.index((dx, dy))
                    row = row_of(bx if dx < 0 else -1, by if dy < 0 else -1)
                    if current is not None:
                        for c in range(3):
                            u[current * 3 + c, pl.ds(row, 1), :] = rc[q, i, pl.ds(c, 1), :]
                        value = rc[q, i, pl.ds(3, 1), :]
                        kk[pl.ds(row, 1), :] = (1.0 - value) * (1.0 - value) + stiff_floor
                    for f in range(2):
                        field[base + f, pl.ds(row, 1), :] = rc[q, i, pl.ds(3 + f, 1), :]
        if current is not None:
            for x in (-2, -1, bx, bx + 1):
                here = pl.ds(row_of(x, 0), by)
                value = field[base, here, :]
                kk[here, :] = (1.0 - value) * (1.0 - value) + stiff_floor

    def a_copy(q, dx, dy):
        if dy == 0:
            i = 0 if dx < 0 else 1
            x, to = (1, bx + 1) if dx < 0 else (bx - 2, -2)
            return remote(
                u.at[pl.ds(q * 3, 3), pl.ds(row_of(x, 0), by), :],
                u.at[pl.ds(q * 3, 3), pl.ds(row_of(to, 0), by), :],
                a_send.at[q, i], a_recv.at[q, i], dx, dy,
            )
        i = 0 if dy < 0 else 1
        return remote(
            pa.at[i], ra.at[q, i], a_send.at[q, 2 + i], a_recv.at[q, 2 + i], dx, dy,
        )

    def send_a(q):
        for i in range(2):
            y = 1 if i == 0 else by - 2
            for c in range(3):
                pa[i, c] = u[q * 3 + c, pl.ds(row_of(0, y), bx, stride=PITCH), :]
        for dx, dy in sides_x + sides_y:
            @pl.when(there(dx, dy))
            def _(dx=dx, dy=dy):
                a_copy(q, dx, dy).start()

    def sent_a(q):
        for dx, dy in sides_x + sides_y:
            @pl.when(there(dx, dy))
            def _(dx=dx, dy=dy):
                a_copy(q, dx, dy).wait_send()

    def take_a(q):
        for dx, dy in sides_x + sides_y:
            @pl.when(there(-dx, -dy))
            def _(dx=dx, dy=dy):
                a_copy(q, dx, dy).wait_recv()
                if dx == 0:
                    i = 0 if dy < 0 else 1
                    y = by + 1 if i == 0 else -2
                    for c in range(3):
                        u[q * 3 + c, pl.ds(row_of(0, y), bx, stride=PITCH), :] = ra[q, i, c]

    def tough_copy(r):
        return pltpu.make_async_remote_copy(
            src_ref=tough_ref, dst_ref=g.at[r], send_sem=t_send.at[r], recv_sem=t_recv.at[r],
            device_id={"section": lax.rem(me_s + ns - r, ns)}, device_id_type=MESH,
        )

    send_b(lf, 0, 1, None)
    for r in range(1, ns):
        tough_copy(r).start()

    lane = lax.broadcasted_iota(jnp.int32, (by, nz), 1)
    at_low = lane == 0
    at_high = lane == nz - 1

    def from_low(value, edge):
        return jnp.where(at_low, edge, pltpu.roll(value, 1, 1))

    def from_high(value, edge):
        return jnp.where(at_high, edge, pltpu.roll(value, nz - 1, 1))

    def span(start, stride):
        return pl.ds(start, by) if stride == 1 else pl.ds(start, bx, stride=stride)

    case = index_ref[0]
    vector = [loads_ref[case, c] for c in range(3)]

    take_b(lf, 0, 1, None)

    def fill(x, carry):
        here = pl.ds(x * PITCH, PITCH)
        load = lf[0, here, :]
        for c in range(3):
            u[c, here, :] = load * vector[c]
        return carry

    lax.fori_loop(0, bx + 2 * HALO, fill, 0, unroll=2)
    tail = pl.ds((bx + 2 * HALO) * PITCH, 8)
    for c in range(3):
        u[c, tail, :] = lf[0, tail, :] * vector[c]

    def first_flow(x, carry):
        start = row_of(x, 0)
        trace = (
            u[0, pl.ds(start + PITCH, by), :] - u[0, pl.ds(start - PITCH, by), :]
            + u[1, pl.ds(start + 1, by), :] - u[1, pl.ds(start - 1, by), :]
        )
        value = u[2, pl.ds(start, by), :]
        trace = trace + (from_high(value, 0.0) - from_low(value, 0.0))
        df[1, pl.ds(start, by), :] = kk[pl.ds(start, by), :] * (0.5 * trace)
        return carry

    lax.fori_loop(0, bx, first_flow, 0, unroll=4)
    sent_b(lf, 0, 1)
    send_b(df, 0, 0, 0)
    copies[3].wait()

    def move(p, start, stride, out_x=None):
        q = 1 - p
        def at(ref, offset, *lead):
            return ref[(*lead, span(start + offset, stride), slice(None))]

        k = at(kk, 0)
        k_xm, k_xp = at(kk, -PITCH), at(kk, PITCH)
        k_ym, k_yp = at(kk, -1), at(kk, 1)
        k_zm, k_zp = from_low(k, outside_stiff), from_high(k, outside_stiff)
        pairs = (k_xm + k_xp, k_ym + k_yp, k_zm + k_zp)
        total = 6.0 * k + (pairs[0] + pairs[1] + pairs[2])
        w_xm, w_xp, w_ym, w_yp = k + k_xm, k + k_xp, k + k_ym, k + k_yp
        w_zm = jnp.where(at_low, 0.0, k + k_zm)
        w_zp = jnp.where(at_high, 0.0, k + k_zp)
        flow = 2 * p + 1
        middle_flow = at(df, 0, flow)
        slopes = (
            at(df, PITCH, flow) - at(df, -PITCH, flow),
            at(df, 1, flow) - at(df, -1, flow),
            from_high(middle_flow, 0.0) - from_low(middle_flow, 0.0),
        )
        fixed = at(lf, 0, 1) > 0.5
        load = at(lf, 0, 0)
        squares = None
        for c in range(3):
            f = p * 3 + c
            here = at(u, 0, f)
            total_c = (
                w_xm * at(u, -PITCH, f) + w_xp * at(u, PITCH, f)
                + w_ym * at(u, -1, f) + w_yp * at(u, 1, f)
                + w_zm * pltpu.roll(here, 1, 1) + w_zp * pltpu.roll(here, nz - 1, 1)
            )
            residual = total_c - total * here + 2.0 * slopes[c]
            relaxed = here + relax_weight * residual / (total + pairs[c])
            new = jnp.where(fixed, load * vector[c], relaxed)
            u[q * 3 + c, span(start, stride), :] = new
            if out_x is not None and out_x[0]:
                disp_ref[0, c, out_x[1]] = new
            square = residual * residual
            squares = square if squares is None else squares + square
        return jnp.where(fixed, 0.0, squares)

    def heal(p, r, x, last):
        q = 1 - p
        start = row_of(x, 0)
        def at(offset, f):
            return u[f, pl.ds(start + offset, by), :]

        grads = []
        for c in range(3):
            f = q * 3 + c
            here = at(0, f)
            grads.append((
                at(PITCH, f) - at(-PITCH, f),
                at(1, f) - at(-1, f),
                from_high(here, 0.0) - from_low(here, 0.0),
            ))
        energy, trace = twice_energy(
            grads[0][0], grads[1][1], grads[2][2],
            0.5 * (grads[0][1] + grads[1][0]),
            0.5 * (grads[0][2] + grads[2][0]),
            0.5 * (grads[1][2] + grads[2][1]),
        )
        def near(offset):
            return df[2 * p, pl.ds(start + offset, by), :]

        here = near(0)
        beside = (
            near(PITCH) + near(-PITCH) + near(1) + near(-1)
            + from_high(here, 0.0) + from_low(here, 0.0)
        )
        held = pl.ds(x * by, by)
        rate = g[r, held, :]
        renewed = (energy + rate * beside) / (energy + 7.0 * rate)
        renewed = jnp.where(crack_v[held, :] > 0, 1.0, renewed)
        if last:
            dam_ref[0, x] = renewed
        else:
            stiff = (1.0 - renewed) * (1.0 - renewed) + stiff_floor
            df[2 * q, pl.ds(start, by), :] = renewed
            kk[pl.ds(start, by), :] = stiff
            df[2 * q + 1, pl.ds(start, by), :] = stiff * (0.5 * trace)

    columns = lax.broadcasted_iota(jnp.int32, (1, nz), 1)

    def sweep(r, table, last):
        p = lax.rem(r, 2)
        q = 1 - p
        take_b(df, 2 * p, p, p)

        def move_own(x, total):
            return total + move(p, row_of(x, 0), 1, (last, x))

        squares = lax.fori_loop(
            0, bx, move_own, jnp.zeros((by, nz), jnp.float32), unroll=4
        )
        if not last:
            @pl.when(r > 0)
            def _():
                sent_a(p)
            send_a(q)
        else:
            sent_a(p)
        total = jnp.sum(jnp.sum(squares, axis=0, keepdims=True), axis=1, keepdims=True)
        column = lax.rem(me_s + r, ns)
        table = jnp.where(columns == column, jnp.broadcast_to(total, (1, nz)), table)
        if last:
            spread_sums(table)
        for x in (-1, bx):
            move(p, row_of(x, 0), 1)
        for y in (-1, by):
            move(p, row_of(0, y), PITCH)

        if last:
            tough_copy(r).wait_recv()
        else:
            @pl.when(r > 0)
            def _():
                tough_copy(r).wait_recv()

        def heal_own(x, carry):
            heal(p, r, x, last)
            return carry

        lax.fori_loop(0, bx, heal_own, 0, unroll=4)
        sent_b(df, 2 * p, p)
        if not last:
            send_b(df, 2 * q, q, q)
            take_a(q)
        return table

    def sums_copy(t):
        me = me_x * ny + me_y
        to = lax.rem(me + t, nx * ny)
        return pltpu.make_async_remote_copy(
            src_ref=row_v, dst_ref=rows_v.at[me], send_sem=s_send.at[t], recv_sem=s_recv.at[t],
            device_id={"gx": to // ny, "gy": lax.rem(to, ny)}, device_id_type=MESH,
        )

    def from_copy(t):
        me = me_x * ny + me_y
        source = lax.rem(me + nx * ny - t, nx * ny)
        return pltpu.make_async_remote_copy(
            src_ref=row_v, dst_ref=rows_v.at[source], send_sem=s_send.at[t], recv_sem=s_recv.at[t],
            device_id={"gx": me_x, "gy": me_y}, device_id_type=MESH,
        )

    def spread_sums(table):
        row_v[...] = table
        rows_v[me_x * ny + me_y] = table

        def start(t, carry):
            sums_copy(t).start()
            return carry

        lax.fori_loop(1, nx * ny, start, 0)

    table = lax.fori_loop(
        0, ns - 1, lambda r, t: sweep(r, t, False), jnp.zeros((1, nz), jnp.float32)
    )
    sweep(jnp.int32(ns - 1), table, True)

    for r in range(1, ns):
        tough_copy(r).wait_send()

    def finish(t, carry):
        sums_copy(t).wait_send()
        from_copy(t).wait_recv()
        return carry

    lax.fori_loop(1, nx * ny, finish, 0)
    everything = rows_v[0]
    for i in range(1, nx * ny):
        everything = everything + rows_v[i]
    result = jnp.sqrt(everything * (0.25 / (3.0 * cells)))
    table_ref[...] = result[:, :ns]


def on_device(sizes, load_index, load_table, toughness, clamp_mask, load_mask, crack_mask):
    ns, nx, ny = sizes
    bx, by, nz = clamp_mask.shape
    cells = float(clamp_mask.size * nx * ny)
    rows = (bx + 2 * HALO) * PITCH + LEAD
    flat = (bx * by, nz)
    f32 = jnp.float32
    scratch = [
        pltpu.VMEM((6, rows, nz), f32),
        pltpu.VMEM((4, rows, nz), f32),
        pltpu.VMEM((rows, nz), f32),
        pltpu.VMEM((2, rows, nz), f32),
        pltpu.VMEM(flat, jnp.int32),
        pltpu.VMEM(flat, jnp.int32),
        pltpu.VMEM(flat, jnp.int32),
        pltpu.VMEM((ns, *flat), f32),
        pltpu.VMEM((2, 3, bx, nz), f32),
        pltpu.VMEM((2, 2, 3, bx, nz), f32),
        pltpu.VMEM((2, 2 * HALO, bx, nz), f32),
        pltpu.VMEM((2, 2, 2 * HALO, bx, nz), f32),
        pltpu.VMEM((4, 8, nz), f32),
        pltpu.VMEM((2, 4, 8, nz), f32),
        pltpu.VMEM((1, nz), f32),
        pltpu.VMEM((nx * ny, 1, nz), f32),
        pltpu.SemaphoreType.DMA((4,)),
        pltpu.SemaphoreType.DMA((2, 4)),
        pltpu.SemaphoreType.DMA((2, 4)),
        pltpu.SemaphoreType.DMA((2, 10)),
        pltpu.SemaphoreType.DMA((2, 10)),
        pltpu.SemaphoreType.DMA((ns,)),
        pltpu.SemaphoreType.DMA((ns,)),
        pltpu.SemaphoreType.DMA((nx * ny,)),
        pltpu.SemaphoreType.DMA((nx * ny,)),
    ]
    smem = pl.BlockSpec(memory_space=pltpu.SMEM)
    vmem = pl.BlockSpec(memory_space=pltpu.VMEM)
    hbm = pl.BlockSpec(memory_space=pl.ANY)
    return pl.pallas_call(
        functools.partial(kernel, sizes, bx, by, cells),
        out_shape=(
            jax.ShapeDtypeStruct((1, 3, bx, by, nz), f32),
            jax.ShapeDtypeStruct((1, bx, by, nz), f32),
            jax.ShapeDtypeStruct((1, ns), f32),
        ),
        in_specs=[smem, smem, hbm, hbm, hbm, hbm],
        out_specs=(vmem, vmem, vmem),
        scratch_shapes=scratch,
        compiler_params=pltpu.CompilerParams(collective_id=0, has_side_effects=True),
        name="sweeps",
    )(
        load_index,
        load_table,
        toughness.reshape(flat),
        clamp_mask.reshape(flat),
        load_mask.reshape(flat),
        crack_mask.reshape(flat),
    )


def solution(mesh):
    sizes = (mesh.shape["section"], mesh.shape["gx"], mesh.shape["gy"])
    in_specs = (
        P("section"),
        P(),
        P("section", "gx", "gy", None),
        P("gx", "gy", None),
        P("gx", "gy", None),
        P("gx", "gy", None),
    )
    out_specs = (
        P("section", None, "gx", "gy", None),
        P("section", "gx", "gy", None),
        P("section", None),
    )
    return jax.shard_map(
        functools.partial(on_device, sizes),
        mesh=mesh, in_specs=in_specs, out_specs=out_specs, check_vma=False,
    )
```

```python
import functools

import jax
import jax.numpy as jnp
from jax import lax
from jax.experimental import pallas as pl
from jax.experimental.pallas import tpu as pltpu
from jax.sharding import PartitionSpec as P

MESH = pl.DeviceIdType.MESH
relax_weight = 0.6
stiff_floor = 0.001
eigen_guard = 1e-08
outside_stiff = 1.001

cos_third = (
    0.8660254053677892, 0.166666399623719, -0.0481050217302989, 0.024608831949810825,
    -0.015124763172089219, 0.009420074574188678, -0.004972568153766589,
    0.0017909605462136829, -0.0003093201852607309,
)
sin_third = (
    0.49999999939158213, -0.038675031951822925, 0.015381770818675887, -0.00862700282428075,
    0.005525819902144846, -0.0035154216998851246, 0.0018763805597984632,
    -0.0006797757027300123, 0.00011778274999869613,
)

PITCH = 24
LEAD = 8
HALO = 2
group = 8


def row_of(x, y):
    return (x + HALO) * PITCH + LEAD + y


def polynomial(coefficients, t):
    value = coefficients[-1]
    for coefficient in coefficients[-2::-1]:
        value = value * t + coefficient
    return value


def twice_energy(a, b, c, d, e, f):
    trace = a + b + c
    middle = trace * (1.0 / 3.0)
    a, b, c = a - middle, b - middle, c - middle
    dd, ee, ff = d * d, e * e, f * f
    spread = (a * a + b * b + c * c) * (1.0 / 6.0) + (dd + ee + ff) * (1.0 / 3.0)
    guarded = spread + 4.0 * eigen_guard
    determinant = a * (b * c - ff) - d * (d * c - f * e) + e * (d * f - b * e)
    inverse = lax.rsqrt(guarded)
    ratio = determinant * (0.5 * inverse) * (inverse * inverse)
    size = jnp.minimum(jnp.abs(ratio), 1.0)
    radius = jnp.sqrt(spread)
    first = radius * polynomial(cos_third, size)
    first = jnp.where(ratio < 0.0, -first, first)
    rest = radius * (1.7320508075688772 * jnp.sqrt(1.0 - size)) * polynomial(sin_third, size)
    largest = jnp.maximum(middle + 2.0 * first, 0.0)
    base = middle - first
    second = jnp.maximum(base + rest, 0.0)
    third = jnp.maximum(base - rest, 0.0)
    volume = jnp.maximum(trace, 0.0)
    energy = 0.25 * (volume * volume) + 0.5 * (
        largest * largest + second * second + third * third
    )
    return energy, trace


def kernel(
    sizes, bx, by, cells,
    index_ref, loads_ref, tough_ref, clamp_ref, load_ref, crack_ref,
    disp_ref, dam_ref, table_ref,
    u0, u1, df0, df1, kk, lf, clamp_v, load_v, crack_v, g,
    pa, ra, pb, rb, pc, rc, row_v, rows_v,
    local_sem, a_send, a_recv, b_send, b_recv, t_send, t_recv, s_send, s_recv,
):
    ns, nx, ny = sizes
    me_s = lax.axis_index("section")
    me_x = lax.axis_index("gx")
    me_y = lax.axis_index("gy")
    nz = u0.shape[-1]
    us, dfs = (u0, u1), (df0, df1)

    copies = [
        pltpu.make_async_copy(source, target, local_sem.at[i])
        for i, (source, target) in enumerate(
            ((load_ref, load_v), (clamp_ref, clamp_v), (crack_ref, crack_v), (tough_ref, g.at[0]))
        )
    ]
    for copy in copies:
        copy.start()

    halo_pieces = [(i * PITCH, 8) for i in range(bx + 2 * HALO + 1)]
    halo_pieces += [(row_of(x, 0), by) for x in (-2, -1, bx, bx + 1)]
    for start, size in halo_pieces:
        for ref in us + dfs:
            for i in range(ref.shape[0]):
                ref[i, pl.ds(start, size), :] = jnp.zeros((size, nz), jnp.float32)
        lf[0, pl.ds(start, size), :] = jnp.zeros((size, nz), jnp.float32)
        lf[1, pl.ds(start, size), :] = jnp.ones((size, nz), jnp.float32)
        kk[pl.ds(start, size), :] = jnp.full((size, nz), outside_stiff, jnp.float32)

    def there(dx, dy):
        return (
            (me_x + dx >= 0) & (me_x + dx < nx) & (me_y + dy >= 0) & (me_y + dy < ny)
        )

    corners = ((-1, -1), (-1, 1), (1, -1), (1, 1))
    sides_x = ((-1, 0), (1, 0))
    sides_y = ((0, -1), (0, 1))
    neighbours = sides_x + sides_y + corners

    barrier = pltpu.get_barrier_semaphore()
    for dx, dy in neighbours:
        @pl.when(there(dx, dy))
        def _(dx=dx, dy=dy):
            pl.semaphore_signal(
                barrier, inc=1, device_id={"gx": me_x + dx, "gy": me_y + dy}, device_id_type=MESH
            )
    for r in range(1, ns):
        pl.semaphore_signal(
            barrier, inc=1, device_id={"section": lax.rem(me_s + r, ns)}, device_id_type=MESH
        )

    for i in (0, 1, 2):
        copies[i].wait()

    def begin(x, carry):
        here = pl.ds(row_of(x, 0), by)
        held = pl.ds(x * by, by)
        load = load_v[held, :].astype(jnp.float32)
        clamp = clamp_v[held, :].astype(jnp.float32)
        crack = crack_v[held, :].astype(jnp.float32)
        lf[0, here, :] = load
        lf[1, here, :] = jnp.maximum(load, clamp)
        df0[0, here, :] = crack
        kk[here, :] = (1.0 - crack) * (1.0 - crack) + stiff_floor
        return carry

    lax.fori_loop(0, bx, begin, 0, unroll=4)

    across = 1 + (me_x > 0).astype(jnp.int32) + (me_x < nx - 1).astype(jnp.int32)
    along = 1 + (me_y > 0).astype(jnp.int32) + (me_y < ny - 1).astype(jnp.int32)
    pl.semaphore_wait(barrier, across * along - 1 + (ns - 1))

    def remote(source, target, send, recv, dx, dy):
        return pltpu.make_async_remote_copy(
            src_ref=source, dst_ref=target, send_sem=send, recv_sem=recv,
            device_id={"gx": me_x + dx, "gy": me_y + dy}, device_id_type=MESH,
        )

    def b_copies(field, q, dx, dy):
        found = []
        if dy == 0:
            for layer in range(HALO):
                x = layer if dx < 0 else bx - HALO + layer
                to = bx + layer if dx < 0 else layer - HALO
                i = (0 if dx < 0 else 2) + layer
                found.append(remote(
                    field.at[:, pl.ds(row_of(x, 0), by), :],
                    field.at[:, pl.ds(row_of(to, 0), by), :],
                    b_send.at[q, i], b_recv.at[q, i], dx, dy,
                ))
        elif dx == 0:
            i = 0 if dy < 0 else 1
            found.append(remote(
                pb.at[i], rb.at[q, i], b_send.at[q, 4 + i], b_recv.at[q, 4 + i], dx, dy,
            ))
        else:
            i = corners.index((dx, dy))
            found.append(remote(
                pc.at[i], rc.at[q, i], b_send.at[q, 6 + i], b_recv.at[q, 6 + i], dx, dy,
            ))
        return found

    order_b = corners + sides_x + sides_y

    def send_b(field, q, current):
        for i, (dx, dy) in enumerate(corners):
            row = row_of(0 if dx < 0 else bx - 1, 0 if dy < 0 else by - 1)
            if current is not None:
                for c in range(3):
                    pc[i, pl.ds(c, 1), :] = current[c, pl.ds(row, 1), :]
            for f in range(2):
                pc[i, pl.ds(3 + f, 1), :] = field[f, pl.ds(row, 1), :]
        for i in range(2):
            for f in range(2):
                for layer in range(HALO):
                    y = layer if i == 0 else by - HALO + layer
                    pb[i, f * HALO + layer] = field[
                        f, pl.ds(row_of(0, y), bx, stride=PITCH), :
                    ]
        for dx, dy in order_b:
            @pl.when(there(dx, dy))
            def _(dx=dx, dy=dy):
                for copy in b_copies(field, q, dx, dy):
                    copy.start()

    def sent_b(field, q):
        for dx, dy in order_b:
            @pl.when(there(dx, dy))
            def _(dx=dx, dy=dy):
                for copy in b_copies(field, q, dx, dy):
                    copy.wait_send()

    def take_b(field, q, current):
        for dx, dy in order_b:
            @pl.when(there(-dx, -dy))
            def _(dx=dx, dy=dy):
                for copy in b_copies(field, q, dx, dy):
                    copy.wait_recv()
                if dx == 0:
                    i = 0 if dy < 0 else 1
                    for f in range(2):
                        for layer in range(HALO):
                            y = by + layer if i == 0 else layer - HALO
                            strip = pl.ds(row_of(0, y), bx, stride=PITCH)
                            value = rb[q, i, f * HALO + layer]
                            field[f, strip, :] = value
                            if current is not None and f == 0:
                                kk[strip, :] = (1.0 - value) * (1.0 - value) + stiff_floor
                elif dy != 0:
                    i = corners.index((dx, dy))
                    row = row_of(bx if dx < 0 else -1, by if dy < 0 else -1)
                    if current is not None:
                        for c in range(3):
                            current[c, pl.ds(row, 1), :] = rc[q, i, pl.ds(c, 1), :]
                        value = rc[q, i, pl.ds(3, 1), :]
                        kk[pl.ds(row, 1), :] = (1.0 - value) * (1.0 - value) + stiff_floor
                    for f in range(2):
                        field[f, pl.ds(row, 1), :] = rc[q, i, pl.ds(3 + f, 1), :]
        if current is not None:
            for x in (-2, -1, bx, bx + 1):
                here = pl.ds(row_of(x, 0), by)
                value = field[0, here, :]
                kk[here, :] = (1.0 - value) * (1.0 - value) + stiff_floor

    def a_copy(q, dx, dy):
        if dy == 0:
            i = 0 if dx < 0 else 1
            x, to = (1, bx + 1) if dx < 0 else (bx - 2, -2)
            return remote(
                us[q].at[:, pl.ds(row_of(x, 0), by), :],
                us[q].at[:, pl.ds(row_of(to, 0), by), :],
                a_send.at[q, i], a_recv.at[q, i], dx, dy,
            )
        i = 0 if dy < 0 else 1
        return remote(
            pa.at[i], ra.at[q, i], a_send.at[q, 2 + i], a_recv.at[q, 2 + i], dx, dy,
        )

    def send_a(q):
        for i in range(2):
            y = 1 if i == 0 else by - 2
            for c in range(3):
                pa[i, c] = us[q][c, pl.ds(row_of(0, y), bx, stride=PITCH), :]
        for dx, dy in sides_x + sides_y:
            @pl.when(there(dx, dy))
            def _(dx=dx, dy=dy):
                a_copy(q, dx, dy).start()

    def sent_a(q):
        for dx, dy in sides_x + sides_y:
            @pl.when(there(dx, dy))
            def _(dx=dx, dy=dy):
                a_copy(q, dx, dy).wait_send()

    def take_a(q):
        for dx, dy in sides_x + sides_y:
            @pl.when(there(-dx, -dy))
            def _(dx=dx, dy=dy):
                a_copy(q, dx, dy).wait_recv()
                if dx == 0:
                    i = 0 if dy < 0 else 1
                    y = by + 1 if i == 0 else -2
                    for c in range(3):
                        us[q][c, pl.ds(row_of(0, y), bx, stride=PITCH), :] = ra[q, i, c]

    def tough_copy(r):
        return pltpu.make_async_remote_copy(
            src_ref=tough_ref, dst_ref=g.at[r], send_sem=t_send.at[r], recv_sem=t_recv.at[r],
            device_id={"section": lax.rem(me_s + ns - r, ns)}, device_id_type=MESH,
        )

    send_b(lf, 1, None)
    for r in range(1, ns):
        tough_copy(r).start()

    lane = lax.broadcasted_iota(jnp.int32, (by, nz), 1)
    at_low = lane == 0
    at_high = lane == nz - 1

    def from_low(value, edge):
        return jnp.where(at_low, edge, pltpu.roll(value, 1, 1))

    def from_high(value, edge):
        return jnp.where(at_high, edge, pltpu.roll(value, nz - 1, 1))

    def span(start, stride):
        return pl.ds(start, by) if stride == 1 else pl.ds(start, bx, stride=stride)

    case = index_ref[0]
    vector = [loads_ref[c, case] for c in range(3)]

    take_b(lf, 1, None)

    def fill(x, carry):
        here = pl.ds(x * PITCH, PITCH)
        load = lf[0, here, :]
        for c in range(3):
            u0[c, here, :] = load * vector[c]
        return carry

    lax.fori_loop(0, bx + 2 * HALO, fill, 0, unroll=2)
    tail = pl.ds((bx + 2 * HALO) * PITCH, 8)
    for c in range(3):
        u0[c, tail, :] = lf[0, tail, :] * vector[c]

    def first_flow(x, carry):
        start = row_of(x, 0)
        trace = (
            u0[0, pl.ds(start + PITCH, by), :] - u0[0, pl.ds(start - PITCH, by), :]
            + u0[1, pl.ds(start + 1, by), :] - u0[1, pl.ds(start - 1, by), :]
        )
        value = u0[2, pl.ds(start, by), :]
        trace = trace + (from_high(value, 0.0) - from_low(value, 0.0))
        df0[1, pl.ds(start, by), :] = kk[pl.ds(start, by), :] * (0.5 * trace)
        return carry

    lax.fori_loop(0, bx, first_flow, 0, unroll=4)
    sent_b(lf, 1)
    send_b(df0, 0, u0)
    copies[3].wait()

    def move(p, start, stride, out_x=None):
        q = 1 - p
        def at(ref, offset, *lead):
            return ref[(*lead, span(start + offset, stride), slice(None))]

        k = at(kk, 0)
        k_xm, k_xp = at(kk, -PITCH), at(kk, PITCH)
        k_ym, k_yp = at(kk, -1), at(kk, 1)
        k_zm, k_zp = from_low(k, outside_stiff), from_high(k, outside_stiff)
        pairs = (k_xm + k_xp, k_ym + k_yp, k_zm + k_zp)
        total = 6.0 * k + (pairs[0] + pairs[1] + pairs[2])
        w_xm, w_xp, w_ym, w_yp = k + k_xm, k + k_xp, k + k_ym, k + k_yp
        w_zm = jnp.where(at_low, 0.0, k + k_zm)
        w_zp = jnp.where(at_high, 0.0, k + k_zp)
        df, u = dfs[p], us[p]
        middle_flow = at(df, 0, 1)
        slopes = (
            at(df, PITCH, 1) - at(df, -PITCH, 1),
            at(df, 1, 1) - at(df, -1, 1),
            from_high(middle_flow, 0.0) - from_low(middle_flow, 0.0),
        )
        fixed = at(lf, 0, 1) > 0.5
        load = at(lf, 0, 0)
        squares = None
        for c in range(3):
            f = c
            here = at(u, 0, f)
            total_c = (
                w_xm * at(u, -PITCH, f) + w_xp * at(u, PITCH, f)
                + w_ym * at(u, -1, f) + w_yp * at(u, 1, f)
                + w_zm * pltpu.roll(here, 1, 1) + w_zp * pltpu.roll(here, nz - 1, 1)
            )
            residual = total_c - total * here + 2.0 * slopes[c]
            relaxed = here + relax_weight * residual / (total + pairs[c])
            new = jnp.where(fixed, load * vector[c], relaxed)
            us[q][c, span(start, stride), :] = new
            if out_x is not None and out_x[0]:
                disp_ref[0, c, out_x[1]] = new
            square = residual * residual
            squares = square if squares is None else squares + square
        return jnp.where(fixed, 0.0, squares)

    def heal(p, r, x, last):
        q = 1 - p
        start = row_of(x, 0)
        def at(offset, f):
            return us[q][f, pl.ds(start + offset, by), :]

        grads = []
        for c in range(3):
            f = c
            here = at(0, f)
            grads.append((
                at(PITCH, f) - at(-PITCH, f),
                at(1, f) - at(-1, f),
                from_high(here, 0.0) - from_low(here, 0.0),
            ))
        energy, trace = twice_energy(
            grads[0][0], grads[1][1], grads[2][2],
            0.5 * (grads[0][1] + grads[1][0]),
            0.5 * (grads[0][2] + grads[2][0]),
            0.5 * (grads[1][2] + grads[2][1]),
        )
        def near(offset):
            return dfs[p][0, pl.ds(start + offset, by), :]

        here = near(0)
        beside = (
            near(PITCH) + near(-PITCH) + near(1) + near(-1)
            + from_high(here, 0.0) + from_low(here, 0.0)
        )
        held = pl.ds(x * by, by)
        rate = g[r, held, :]
        renewed = (energy + rate * beside) / (energy + 7.0 * rate)
        renewed = jnp.where(crack_v[held, :] > 0, 1.0, renewed)
        if last:
            dam_ref[0, x] = renewed
        else:
            stiff = (1.0 - renewed) * (1.0 - renewed) + stiff_floor
            dfs[q][0, pl.ds(start, by), :] = renewed
            kk[pl.ds(start, by), :] = stiff
            dfs[q][1, pl.ds(start, by), :] = stiff * (0.5 * trace)

    columns = lax.broadcasted_iota(jnp.int32, (1, nz), 1)

    def sweep(r, p, table, first=False, last=False):
        q = 1 - p
        take_b(dfs[p], p, us[p])

        def move_own(i, total):
            for x in range(group):
                total = total + move(p, row_of(i * group + x, 0), 1, (last, i * group + x))
            return total

        squares = lax.fori_loop(
            0, bx // group, move_own, jnp.zeros((by, nz), jnp.float32)
        )
        if not last:
            if not first:
                sent_a(p)
            send_a(q)
        else:
            sent_a(p)
        total = jnp.sum(jnp.sum(squares, axis=0, keepdims=True), axis=1, keepdims=True)
        column = lax.rem(me_s + r, ns)
        table = jnp.where(columns == column, jnp.broadcast_to(total, (1, nz)), table)
        if last:
            spread_sums(table)
        for x in (-1, bx):
            move(p, row_of(x, 0), 1)
        for y in (-1, by):
            move(p, row_of(0, y), PITCH)

        if not first:
            tough_copy(r).wait_recv()

        def heal_own(x, carry):
            heal(p, r, x, last)
            return carry

        lax.fori_loop(0, bx, heal_own, 0, unroll=group)
        sent_b(dfs[p], p)
        if not last:
            send_b(dfs[q], q, us[q])
            take_a(q)
        return table

    def sums_copy(t):
        me = me_x * ny + me_y
        to = lax.rem(me + t, nx * ny)
        return pltpu.make_async_remote_copy(
            src_ref=row_v, dst_ref=rows_v.at[me], send_sem=s_send.at[t], recv_sem=s_recv.at[t],
            device_id={"gx": to // ny, "gy": lax.rem(to, ny)}, device_id_type=MESH,
        )

    def from_copy(t):
        me = me_x * ny + me_y
        source = lax.rem(me + nx * ny - t, nx * ny)
        return pltpu.make_async_remote_copy(
            src_ref=row_v, dst_ref=rows_v.at[source], send_sem=s_send.at[t], recv_sem=s_recv.at[t],
            device_id={"gx": me_x, "gy": me_y}, device_id_type=MESH,
        )

    def spread_sums(table):
        row_v[...] = table
        rows_v[me_x * ny + me_y] = table

        def start(t, carry):
            sums_copy(t).start()
            return carry

        lax.fori_loop(1, nx * ny, start, 0)

    def two_sweeps(i, table):
        return sweep(2 * i + 2, 0, sweep(2 * i + 1, 1, table))

    table = sweep(0, 0, jnp.zeros((1, nz), jnp.float32), first=True)
    table = lax.fori_loop(0, (ns - 2) // 2, two_sweeps, table)
    sweep(ns - 1, 1, table, last=True)

    for r in range(1, ns):
        tough_copy(r).wait_send()

    def finish(t, carry):
        sums_copy(t).wait_send()
        from_copy(t).wait_recv()
        return carry

    lax.fori_loop(1, nx * ny, finish, 0)
    everything = rows_v[0]
    for i in range(1, nx * ny):
        everything = everything + rows_v[i]
    result = jnp.sqrt(everything * (0.25 / (3.0 * cells)))
    table_ref[...] = result[:, :ns]


def on_device(sizes, load_index, load_table, toughness, clamp_mask, load_mask, crack_mask):
    ns, nx, ny = sizes
    bx, by, nz = clamp_mask.shape
    cells = float(clamp_mask.size * nx * ny)
    rows = (bx + 2 * HALO) * PITCH + LEAD
    flat = (bx * by, nz)
    f32 = jnp.float32
    scratch = [
        pltpu.VMEM((3, rows, nz), f32),
        pltpu.VMEM((3, rows, nz), f32),
        pltpu.VMEM((2, rows, nz), f32),
        pltpu.VMEM((2, rows, nz), f32),
        pltpu.VMEM((rows, nz), f32),
        pltpu.VMEM((2, rows, nz), f32),
        pltpu.VMEM(flat, jnp.int32),
        pltpu.VMEM(flat, jnp.int32),
        pltpu.VMEM(flat, jnp.int32),
        pltpu.VMEM((ns, *flat), f32),
        pltpu.VMEM((2, 3, bx, nz), f32),
        pltpu.VMEM((2, 2, 3, bx, nz), f32),
        pltpu.VMEM((2, 2 * HALO, bx, nz), f32),
        pltpu.VMEM((2, 2, 2 * HALO, bx, nz), f32),
        pltpu.VMEM((4, 8, nz), f32),
        pltpu.VMEM((2, 4, 8, nz), f32),
        pltpu.VMEM((1, nz), f32),
        pltpu.VMEM((nx * ny, 1, nz), f32),
        pltpu.SemaphoreType.DMA((4,)),
        pltpu.SemaphoreType.DMA((2, 4)),
        pltpu.SemaphoreType.DMA((2, 4)),
        pltpu.SemaphoreType.DMA((2, 10)),
        pltpu.SemaphoreType.DMA((2, 10)),
        pltpu.SemaphoreType.DMA((ns,)),
        pltpu.SemaphoreType.DMA((ns,)),
        pltpu.SemaphoreType.DMA((nx * ny,)),
        pltpu.SemaphoreType.DMA((nx * ny,)),
    ]
    smem = pl.BlockSpec(memory_space=pltpu.SMEM)
    vmem = pl.BlockSpec(memory_space=pltpu.VMEM)
    hbm = pl.BlockSpec(memory_space=pl.ANY)
    return pl.pallas_call(
        functools.partial(kernel, sizes, bx, by, cells),
        out_shape=(
            jax.ShapeDtypeStruct((1, 3, bx, by, nz), f32),
            jax.ShapeDtypeStruct((1, bx, by, nz), f32),
            jax.ShapeDtypeStruct((1, ns), f32),
        ),
        in_specs=[smem, smem, hbm, hbm, hbm, hbm],
        out_specs=(vmem, vmem, vmem),
        scratch_shapes=scratch,
        compiler_params=pltpu.CompilerParams(collective_id=0, has_side_effects=True),
        name="sweeps",
    )(
        load_index,
        load_table.T,
        toughness.reshape(flat),
        clamp_mask.reshape(flat),
        load_mask.reshape(flat),
        crack_mask.reshape(flat),
    )


def solution(mesh):
    sizes = (mesh.shape["section"], mesh.shape["gx"], mesh.shape["gy"])
    in_specs = (
        P("section"),
        P(),
        P("section", "gx", "gy", None),
        P("gx", "gy", None),
        P("gx", "gy", None),
        P("gx", "gy", None),
    )
    out_specs = (
        P("section", None, "gx", "gy", None),
        P("section", "gx", "gy", None),
        P("section", None),
    )
    return jax.shard_map(
        functools.partial(on_device, sizes),
        mesh=mesh, in_specs=in_specs, out_specs=out_specs, check_vma=False,
    )
```

```python
import functools

import jax
import jax.numpy as jnp
from jax import lax
from jax.experimental import pallas as pl
from jax.experimental.pallas import tpu as pltpu
from jax.sharding import PartitionSpec as P

MESH = pl.DeviceIdType.MESH
relax_weight = 0.6
stiff_floor = 0.001
eigen_guard = 1e-08
outside_stiff = 1.001

cos_third = (
    0.8660254053677892, 0.166666399623719, -0.0481050217302989, 0.024608831949810825,
    -0.015124763172089219, 0.009420074574188678, -0.004972568153766589,
    0.0017909605462136829, -0.0003093201852607309,
)
sin_third = (
    0.49999999939158213, -0.038675031951822925, 0.015381770818675887, -0.00862700282428075,
    0.005525819902144846, -0.0035154216998851246, 0.0018763805597984632,
    -0.0006797757027300123, 0.00011778274999869613,
)

PITCH = 24
LEAD = 8
HALO = 2


def row_of(x, y):
    return (x + HALO) * PITCH + LEAD + y


def polynomial(coefficients, t):
    value = coefficients[-1]
    for coefficient in coefficients[-2::-1]:
        value = value * t + coefficient
    return value


def twice_energy(a, b, c, d, e, f):
    trace = a + b + c
    middle = trace * (1.0 / 3.0)
    a, b, c = a - middle, b - middle, c - middle
    dd, ee, ff = d * d, e * e, f * f
    spread = (a * a + b * b + c * c) * (1.0 / 6.0) + (dd + ee + ff) * (1.0 / 3.0)
    guarded = spread + 4.0 * eigen_guard
    determinant = a * (b * c - ff) - d * (d * c - f * e) + e * (d * f - b * e)
    inverse = lax.rsqrt(guarded)
    ratio = determinant * (0.5 * inverse) * (inverse * inverse)
    size = jnp.minimum(jnp.abs(ratio), 1.0)
    radius = jnp.sqrt(spread)
    first = radius * polynomial(cos_third, size)
    first = jnp.where(ratio < 0.0, -first, first)
    rest = radius * (1.7320508075688772 * jnp.sqrt(1.0 - size)) * polynomial(sin_third, size)
    largest = jnp.maximum(middle + 2.0 * first, 0.0)
    base = middle - first
    second = jnp.maximum(base + rest, 0.0)
    third = jnp.maximum(base - rest, 0.0)
    volume = jnp.maximum(trace, 0.0)
    energy = 0.25 * (volume * volume) + 0.5 * (
        largest * largest + second * second + third * third
    )
    return energy, trace


def kernel(
    sizes, bx, by, cells,
    index_ref, loads_ref, tough_ref, clamp_ref, load_ref, crack_ref,
    disp_ref, dam_ref, table_ref,
    u0, u1, df0, df1, kk0, kk1, lf, clamp_v, load_v, crack_v, g,
    pa, ra, pb, rb, pc, rc, row_v, rows_v,
    local_sem, a_send, a_recv, b_send, b_recv, t_send, t_recv, s_send, s_recv,
):
    ns, nx, ny = sizes
    me_s = lax.axis_index("section")
    me_x = lax.axis_index("gx")
    me_y = lax.axis_index("gy")
    nz = u0.shape[-1]
    us, dfs, kks = (u0, u1), (df0, df1), (kk0, kk1)

    copies = [
        pltpu.make_async_copy(source, target, local_sem.at[i])
        for i, (source, target) in enumerate(
            ((load_ref, load_v), (clamp_ref, clamp_v), (crack_ref, crack_v), (tough_ref, g.at[0]))
        )
    ]
    for copy in copies:
        copy.start()

    halo_pieces = [(i * PITCH, 8) for i in range(bx + 2 * HALO + 1)]
    halo_pieces += [(row_of(x, 0), by) for x in (-2, -1, bx, bx + 1)]
    for start, size in halo_pieces:
        for ref in us + dfs:
            for i in range(ref.shape[0]):
                ref[i, pl.ds(start, size), :] = jnp.zeros((size, nz), jnp.float32)
        lf[0, pl.ds(start, size), :] = jnp.zeros((size, nz), jnp.float32)
        lf[1, pl.ds(start, size), :] = jnp.ones((size, nz), jnp.float32)
        for ref in kks:
            ref[pl.ds(start, size), :] = jnp.full((size, nz), outside_stiff, jnp.float32)

    def there(dx, dy):
        return (
            (me_x + dx >= 0) & (me_x + dx < nx) & (me_y + dy >= 0) & (me_y + dy < ny)
        )

    corners = ((-1, -1), (-1, 1), (1, -1), (1, 1))
    sides_x = ((-1, 0), (1, 0))
    sides_y = ((0, -1), (0, 1))
    neighbours = sides_x + sides_y + corners

    barrier = pltpu.get_barrier_semaphore()
    for dx, dy in neighbours:
        @pl.when(there(dx, dy))
        def _(dx=dx, dy=dy):
            pl.semaphore_signal(
                barrier, inc=1, device_id={"gx": me_x + dx, "gy": me_y + dy}, device_id_type=MESH
            )
    for r in range(1, ns):
        pl.semaphore_signal(
            barrier, inc=1, device_id={"section": lax.rem(me_s + r, ns)}, device_id_type=MESH
        )

    for i in (0, 1, 2):
        copies[i].wait()

    def begin(x, carry):
        here = pl.ds(row_of(x, 0), by)
        held = pl.ds(x * by, by)
        load = load_v[held, :].astype(jnp.float32)
        clamp = clamp_v[held, :].astype(jnp.float32)
        crack = crack_v[held, :].astype(jnp.float32)
        lf[0, here, :] = load
        lf[1, here, :] = jnp.maximum(load, clamp)
        df0[0, here, :] = crack
        kk0[here, :] = (1.0 - crack) * (1.0 - crack) + stiff_floor
        return carry

    lax.fori_loop(0, bx, begin, 0, unroll=4)

    across = 1 + (me_x > 0).astype(jnp.int32) + (me_x < nx - 1).astype(jnp.int32)
    along = 1 + (me_y > 0).astype(jnp.int32) + (me_y < ny - 1).astype(jnp.int32)
    pl.semaphore_wait(barrier, across * along - 1 + (ns - 1))

    def remote(source, target, send, recv, dx, dy):
        return pltpu.make_async_remote_copy(
            src_ref=source, dst_ref=target, send_sem=send, recv_sem=recv,
            device_id={"gx": me_x + dx, "gy": me_y + dy}, device_id_type=MESH,
        )

    def b_copies(field, q, dx, dy):
        found = []
        if dy == 0:
            for layer in range(HALO):
                x = layer if dx < 0 else bx - HALO + layer
                to = bx + layer if dx < 0 else layer - HALO
                i = (0 if dx < 0 else 2) + layer
                found.append(remote(
                    field.at[:, pl.ds(row_of(x, 0), by), :],
                    field.at[:, pl.ds(row_of(to, 0), by), :],
                    b_send.at[q, i], b_recv.at[q, i], dx, dy,
                ))
        elif dx == 0:
            i = 0 if dy < 0 else 1
            found.append(remote(
                pb.at[i], rb.at[q, i], b_send.at[q, 4 + i], b_recv.at[q, 4 + i], dx, dy,
            ))
        else:
            i = corners.index((dx, dy))
            found.append(remote(
                pc.at[i], rc.at[q, i], b_send.at[q, 6 + i], b_recv.at[q, 6 + i], dx, dy,
            ))
        return found

    order_b = corners + sides_x + sides_y

    def send_b(field, q, current):
        for i, (dx, dy) in enumerate(corners):
            row = row_of(0 if dx < 0 else bx - 1, 0 if dy < 0 else by - 1)
            if current is not None:
                for c in range(3):
                    pc[i, pl.ds(c, 1), :] = current[c, pl.ds(row, 1), :]
            for f in range(2):
                pc[i, pl.ds(3 + f, 1), :] = field[f, pl.ds(row, 1), :]
        for i in range(2):
            for f in range(2):
                for layer in range(HALO):
                    y = layer if i == 0 else by - HALO + layer
                    pb[i, f * HALO + layer] = field[
                        f, pl.ds(row_of(0, y), bx, stride=PITCH), :
                    ]
        for dx, dy in order_b:
            @pl.when(there(dx, dy))
            def _(dx=dx, dy=dy):
                for copy in b_copies(field, q, dx, dy):
                    copy.start()

    def sent_b(field, q):
        for dx, dy in order_b:
            @pl.when(there(dx, dy))
            def _(dx=dx, dy=dy):
                for copy in b_copies(field, q, dx, dy):
                    copy.wait_send()

    def take_b(field, q, current):
        for dx, dy in order_b:
            @pl.when(there(-dx, -dy))
            def _(dx=dx, dy=dy):
                for copy in b_copies(field, q, dx, dy):
                    copy.wait_recv()
                if dx == 0:
                    i = 0 if dy < 0 else 1
                    for f in range(2):
                        for layer in range(HALO):
                            y = by + layer if i == 0 else layer - HALO
                            strip = pl.ds(row_of(0, y), bx, stride=PITCH)
                            value = rb[q, i, f * HALO + layer]
                            field[f, strip, :] = value
                            if current is not None and f == 0:
                                kks[q][strip, :] = (1.0 - value) * (1.0 - value) + stiff_floor
                elif dy != 0:
                    i = corners.index((dx, dy))
                    row = row_of(bx if dx < 0 else -1, by if dy < 0 else -1)
                    if current is not None:
                        for c in range(3):
                            current[c, pl.ds(row, 1), :] = rc[q, i, pl.ds(c, 1), :]
                        value = rc[q, i, pl.ds(3, 1), :]
                        kks[q][pl.ds(row, 1), :] = (1.0 - value) * (1.0 - value) + stiff_floor
                    for f in range(2):
                        field[f, pl.ds(row, 1), :] = rc[q, i, pl.ds(3 + f, 1), :]
        if current is not None:
            for x in (-2, -1, bx, bx + 1):
                here = pl.ds(row_of(x, 0), by)
                value = field[0, here, :]
                kks[q][here, :] = (1.0 - value) * (1.0 - value) + stiff_floor

    def a_copy(q, dx, dy):
        if dy == 0:
            i = 0 if dx < 0 else 1
            x, to = (1, bx + 1) if dx < 0 else (bx - 2, -2)
            return remote(
                us[q].at[:, pl.ds(row_of(x, 0), by), :],
                us[q].at[:, pl.ds(row_of(to, 0), by), :],
                a_send.at[q, i], a_recv.at[q, i], dx, dy,
            )
        i = 0 if dy < 0 else 1
        return remote(
            pa.at[i], ra.at[q, i], a_send.at[q, 2 + i], a_recv.at[q, 2 + i], dx, dy,
        )

    def send_a(q):
        for i in range(2):
            y = 1 if i == 0 else by - 2
            for c in range(3):
                pa[i, c] = us[q][c, pl.ds(row_of(0, y), bx, stride=PITCH), :]
        for dx, dy in sides_x + sides_y:
            @pl.when(there(dx, dy))
            def _(dx=dx, dy=dy):
                a_copy(q, dx, dy).start()

    def sent_a(q):
        for dx, dy in sides_x + sides_y:
            @pl.when(there(dx, dy))
            def _(dx=dx, dy=dy):
                a_copy(q, dx, dy).wait_send()

    def take_a(q):
        for dx, dy in sides_x + sides_y:
            @pl.when(there(-dx, -dy))
            def _(dx=dx, dy=dy):
                a_copy(q, dx, dy).wait_recv()
                if dx == 0:
                    i = 0 if dy < 0 else 1
                    y = by + 1 if i == 0 else -2
                    for c in range(3):
                        us[q][c, pl.ds(row_of(0, y), bx, stride=PITCH), :] = ra[q, i, c]

    def tough_copy(r):
        return pltpu.make_async_remote_copy(
            src_ref=tough_ref, dst_ref=g.at[r], send_sem=t_send.at[r], recv_sem=t_recv.at[r],
            device_id={"section": lax.rem(me_s + ns - r, ns)}, device_id_type=MESH,
        )

    send_b(lf, 1, None)
    for r in range(1, ns):
        tough_copy(r).start()

    lane = lax.broadcasted_iota(jnp.int32, (by, nz), 1)
    at_low = lane == 0
    at_high = lane == nz - 1

    def from_low(value, edge):
        return jnp.where(at_low, edge, pltpu.roll(value, 1, 1))

    def from_high(value, edge):
        return jnp.where(at_high, edge, pltpu.roll(value, nz - 1, 1))

    def span(start, stride):
        return pl.ds(start, by) if stride == 1 else pl.ds(start, bx, stride=stride)

    case = index_ref[0]
    vector = [loads_ref[c, case] for c in range(3)]

    take_b(lf, 1, None)

    def fill(x, carry):
        here = pl.ds(x * PITCH, PITCH)
        load = lf[0, here, :]
        for c in range(3):
            u0[c, here, :] = load * vector[c]
        return carry

    lax.fori_loop(0, bx + 2 * HALO, fill, 0, unroll=2)
    tail = pl.ds((bx + 2 * HALO) * PITCH, 8)
    for c in range(3):
        u0[c, tail, :] = lf[0, tail, :] * vector[c]

    def first_flow(x, carry):
        start = row_of(x, 0)
        trace = (
            u0[0, pl.ds(start + PITCH, by), :] - u0[0, pl.ds(start - PITCH, by), :]
            + u0[1, pl.ds(start + 1, by), :] - u0[1, pl.ds(start - 1, by), :]
        )
        value = u0[2, pl.ds(start, by), :]
        trace = trace + (from_high(value, 0.0) - from_low(value, 0.0))
        df0[1, pl.ds(start, by), :] = kk0[pl.ds(start, by), :] * (0.5 * trace)
        return carry

    lax.fori_loop(0, bx, first_flow, 0, unroll=4)
    sent_b(lf, 1)
    send_b(df0, 0, u0)
    copies[3].wait()

    def move(p, start, stride):
        df, u, kk = dfs[p], us[p], kks[p]

        def at(ref, offset, *lead):
            return ref[(*lead, span(start + offset, stride), slice(None))]

        k = at(kk, 0)
        k_xm, k_xp = at(kk, -PITCH), at(kk, PITCH)
        k_ym, k_yp = at(kk, -1), at(kk, 1)
        k_zm, k_zp = from_low(k, outside_stiff), from_high(k, outside_stiff)
        pairs = (k_xm + k_xp, k_ym + k_yp, k_zm + k_zp)
        total = 6.0 * k + (pairs[0] + pairs[1] + pairs[2])
        w_xm, w_xp, w_ym, w_yp = k + k_xm, k + k_xp, k + k_ym, k + k_yp
        w_zm = jnp.where(at_low, 0.0, k + k_zm)
        w_zp = jnp.where(at_high, 0.0, k + k_zp)
        middle_flow = at(df, 0, 1)
        slopes = (
            at(df, PITCH, 1) - at(df, -PITCH, 1),
            at(df, 1, 1) - at(df, -1, 1),
            from_high(middle_flow, 0.0) - from_low(middle_flow, 0.0),
        )
        fixed = at(lf, 0, 1) > 0.5
        load = at(lf, 0, 0)
        squares = None
        for c in range(3):
            here = at(u, 0, c)
            total_c = (
                w_xm * at(u, -PITCH, c) + w_xp * at(u, PITCH, c)
                + w_ym * at(u, -1, c) + w_yp * at(u, 1, c)
                + w_zm * pltpu.roll(here, 1, 1) + w_zp * pltpu.roll(here, nz - 1, 1)
            )
            residual = total_c - total * here + 2.0 * slopes[c]
            relaxed = here + relax_weight * residual / (total + pairs[c])
            us[1 - p][c, span(start, stride), :] = jnp.where(fixed, load * vector[c], relaxed)
            square = residual * residual
            squares = square if squares is None else squares + square
        return jnp.where(fixed, 0.0, squares)

    def heal(p, r, start, stride, held):
        q = 1 - p
        df, u = dfs[p], us[q]

        def at(ref, offset, *lead):
            return ref[(*lead, span(start + offset, stride), slice(None))]

        grads = []
        for c in range(3):
            here = at(u, 0, c)
            grads.append((
                at(u, PITCH, c) - at(u, -PITCH, c),
                at(u, 1, c) - at(u, -1, c),
                from_high(here, 0.0) - from_low(here, 0.0),
            ))
        energy, trace = twice_energy(
            grads[0][0], grads[1][1], grads[2][2],
            0.5 * (grads[0][1] + grads[1][0]),
            0.5 * (grads[0][2] + grads[2][0]),
            0.5 * (grads[1][2] + grads[2][1]),
        )
        here = at(df, 0, 0)
        beside = (
            at(df, PITCH, 0) + at(df, -PITCH, 0) + at(df, 1, 0) + at(df, -1, 0)
            + from_high(here, 0.0) + from_low(here, 0.0)
        )
        rate = g[r, held, :]
        renewed = (energy + rate * beside) / (energy + 7.0 * rate)
        renewed = jnp.where(crack_v[held, :] > 0, 1.0, renewed)
        stiff = (1.0 - renewed) * (1.0 - renewed) + stiff_floor
        to = span(start, stride)
        dfs[q][0, to, :] = renewed
        dfs[q][1, to, :] = stiff * (0.5 * trace)
        kks[q][to, :] = stiff

    columns = lax.broadcasted_iota(jnp.int32, (1, nz), 1)
    y_of = lax.broadcasted_iota(jnp.int32, (by, nz), 0)
    at_rim = (y_of == 0) | (y_of == by - 1)

    def in_groups(low, high, body, total):
        steps = 2 if (high - low) % 2 == 0 else 1
        size = (high - low) // steps

        def step(i, total):
            for j in range(size):
                added = body(low + i * size + j)
                total = total if added is None else total + added
            return total

        return lax.fori_loop(0, steps, step, total)

    def sweep(r, p, table, first=False, last=False):
        q = 1 - p

        def move_slab(x):
            return move(p, row_of(x, 0), 1)

        def move_strip(y):
            return move(p, row_of(0, y), PITCH)

        def heal_slab(x):
            heal(p, r, row_of(x, 0), 1, pl.ds(x * by, by))

        def heal_strip(y):
            heal(p, r, row_of(0, y), PITCH, pl.ds(y, bx, stride=by))

        nothing = jnp.zeros((by, nz), jnp.float32)
        squares = in_groups(1, bx - 1, move_slab, nothing)
        if not first:
            tough_copy(r).wait_recv()
        in_groups(2, bx - 2, heal_slab, 0)

        if not first:
            take_a(p)
        take_b(dfs[p], p, us[p])
        for x in (0, bx - 1):
            squares = squares + move_slab(x)
        squares = jnp.where(at_rim, 0.0, squares)
        for y in (0, by - 1):
            squares = squares + move_strip(y)
        for x in (-1, bx):
            move_slab(x)
        for y in (-1, by):
            move_strip(y)
        if not first:
            sent_a(p)
        if not last:
            send_a(q)
        total = jnp.sum(jnp.sum(squares, axis=0, keepdims=True), axis=1, keepdims=True)
        column = lax.rem(me_s + r, ns)
        table = jnp.where(columns == column, jnp.broadcast_to(total, (1, nz)), table)
        if last:
            spread_sums(table)
        for x in (0, 1, bx - 2, bx - 1):
            heal_slab(x)
        for y in (0, 1, by - 2, by - 1):
            heal_strip(y)
        sent_b(dfs[p], p)
        if not last:
            send_b(dfs[q], q, us[q])
        else:
            for x in range(bx):
                here = pl.ds(row_of(x, 0), by)
                for c in range(3):
                    disp_ref[0, c, x] = us[q][c, here, :]
                dam_ref[0, x] = dfs[q][0, here, :]
        return table

    def sums_copy(t):
        me = me_x * ny + me_y
        to = lax.rem(me + t, nx * ny)
        return pltpu.make_async_remote_copy(
            src_ref=row_v, dst_ref=rows_v.at[me], send_sem=s_send.at[t], recv_sem=s_recv.at[t],
            device_id={"gx": to // ny, "gy": lax.rem(to, ny)}, device_id_type=MESH,
        )

    def from_copy(t):
        me = me_x * ny + me_y
        source = lax.rem(me + nx * ny - t, nx * ny)
        return pltpu.make_async_remote_copy(
            src_ref=row_v, dst_ref=rows_v.at[source], send_sem=s_send.at[t], recv_sem=s_recv.at[t],
            device_id={"gx": me_x, "gy": me_y}, device_id_type=MESH,
        )

    def spread_sums(table):
        row_v[...] = table
        rows_v[me_x * ny + me_y] = table

        def start(t, carry):
            sums_copy(t).start()
            return carry

        lax.fori_loop(1, nx * ny, start, 0)

    def two_sweeps(i, table):
        return sweep(2 * i + 2, 0, sweep(2 * i + 1, 1, table))

    table = sweep(0, 0, jnp.zeros((1, nz), jnp.float32), first=True)
    table = lax.fori_loop(0, (ns - 2) // 2, two_sweeps, table)
    sweep(ns - 1, 1, table, last=True)

    for r in range(1, ns):
        tough_copy(r).wait_send()

    def finish(t, carry):
        sums_copy(t).wait_send()
        from_copy(t).wait_recv()
        return carry

    lax.fori_loop(1, nx * ny, finish, 0)
    everything = rows_v[0]
    for i in range(1, nx * ny):
        everything = everything + rows_v[i]
    result = jnp.sqrt(everything * (0.25 / (3.0 * cells)))
    table_ref[...] = result[:, :ns]


def on_device(sizes, load_index, load_table, toughness, clamp_mask, load_mask, crack_mask):
    ns, nx, ny = sizes
    bx, by, nz = clamp_mask.shape
    cells = float(clamp_mask.size * nx * ny)
    rows = (bx + 2 * HALO) * PITCH + LEAD
    flat = (bx * by, nz)
    f32 = jnp.float32
    scratch = [
        pltpu.VMEM((3, rows, nz), f32),
        pltpu.VMEM((3, rows, nz), f32),
        pltpu.VMEM((2, rows, nz), f32),
        pltpu.VMEM((2, rows, nz), f32),
        pltpu.VMEM((rows, nz), f32),
        pltpu.VMEM((rows, nz), f32),
        pltpu.VMEM((2, rows, nz), f32),
        pltpu.VMEM(flat, jnp.int32),
        pltpu.VMEM(flat, jnp.int32),
        pltpu.VMEM(flat, jnp.int32),
        pltpu.VMEM((ns, *flat), f32),
        pltpu.VMEM((2, 3, bx, nz), f32),
        pltpu.VMEM((2, 2, 3, bx, nz), f32),
        pltpu.VMEM((2, 2 * HALO, bx, nz), f32),
        pltpu.VMEM((2, 2, 2 * HALO, bx, nz), f32),
        pltpu.VMEM((4, 8, nz), f32),
        pltpu.VMEM((2, 4, 8, nz), f32),
        pltpu.VMEM((1, nz), f32),
        pltpu.VMEM((nx * ny, 1, nz), f32),
        pltpu.SemaphoreType.DMA((4,)),
        pltpu.SemaphoreType.DMA((2, 4)),
        pltpu.SemaphoreType.DMA((2, 4)),
        pltpu.SemaphoreType.DMA((2, 10)),
        pltpu.SemaphoreType.DMA((2, 10)),
        pltpu.SemaphoreType.DMA((ns,)),
        pltpu.SemaphoreType.DMA((ns,)),
        pltpu.SemaphoreType.DMA((nx * ny,)),
        pltpu.SemaphoreType.DMA((nx * ny,)),
    ]
    smem = pl.BlockSpec(memory_space=pltpu.SMEM)
    vmem = pl.BlockSpec(memory_space=pltpu.VMEM)
    hbm = pl.BlockSpec(memory_space=pl.ANY)
    return pl.pallas_call(
        functools.partial(kernel, sizes, bx, by, cells),
        out_shape=(
            pltpu.VMEM((1, 3, bx, by, nz), f32),
            pltpu.VMEM((1, bx, by, nz), f32),
            pltpu.VMEM((1, ns), f32),
        ),
        in_specs=[smem, smem, hbm, hbm, hbm, hbm],
        out_specs=(vmem, vmem, vmem),
        scratch_shapes=scratch,
        compiler_params=pltpu.CompilerParams(collective_id=0, has_side_effects=True),
        name="sweeps",
    )(
        load_index,
        load_table.T,
        toughness.reshape(flat),
        clamp_mask.reshape(flat),
        load_mask.reshape(flat),
        crack_mask.reshape(flat),
    )


def solution(mesh):
    sizes = (mesh.shape["section"], mesh.shape["gx"], mesh.shape["gy"])
    in_specs = (
        P("section"),
        P(),
        P("section", "gx", "gy", None),
        P("gx", "gy", None),
        P("gx", "gy", None),
        P("gx", "gy", None),
    )
    out_specs = (
        P("section", None, "gx", "gy", None),
        P("section", "gx", "gy", None),
        P("section", None),
    )
    return jax.shard_map(
        functools.partial(on_device, sizes),
        mesh=mesh, in_specs=in_specs, out_specs=out_specs, check_vma=False,
    )
```

```python
import functools

import jax
import jax.numpy as jnp
from jax import lax
from jax.experimental import pallas as pl
from jax.experimental.pallas import tpu as pltpu
from jax.sharding import PartitionSpec as P

MESH = pl.DeviceIdType.MESH
relax_weight = 0.6
stiff_floor = 0.001
eigen_guard = 1e-08
outside_stiff = 1.001

cos_third = (
    0.8660254053677892, 0.166666399623719, -0.0481050217302989, 0.024608831949810825,
    -0.015124763172089219, 0.009420074574188678, -0.004972568153766589,
    0.0017909605462136829, -0.0003093201852607309,
)
sin_third = (
    0.49999999939158213, -0.038675031951822925, 0.015381770818675887, -0.00862700282428075,
    0.005525819902144846, -0.0035154216998851246, 0.0018763805597984632,
    -0.0006797757027300123, 0.00011778274999869613,
)

PITCH = 24
LEAD = 8
HALO = 2
BORDER = 3


def row_of(x, y):
    return (x + BORDER) * PITCH + LEAD + y


def polynomial(coefficients, t):
    value = coefficients[-1]
    for coefficient in coefficients[-2::-1]:
        value = value * t + coefficient
    return value


def twice_energy(a, b, c, d, e, f):
    trace = a + b + c
    middle = trace * (1.0 / 3.0)
    a, b, c = a - middle, b - middle, c - middle
    dd, ee, ff = d * d, e * e, f * f
    spread = (a * a + b * b + c * c) * (1.0 / 6.0) + (dd + ee + ff) * (1.0 / 3.0)
    guarded = spread + 4.0 * eigen_guard
    determinant = a * (b * c - ff) - d * (d * c - f * e) + e * (d * f - b * e)
    inverse = lax.rsqrt(guarded)
    ratio = determinant * (0.5 * inverse) * (inverse * inverse)
    size = jnp.minimum(jnp.abs(ratio), 1.0)
    radius = jnp.sqrt(spread)
    first = radius * polynomial(cos_third, size)
    first = jnp.where(ratio < 0.0, -first, first)
    rest = radius * (1.7320508075688772 * jnp.sqrt(1.0 - size)) * polynomial(sin_third, size)
    largest = jnp.maximum(middle + 2.0 * first, 0.0)
    base = middle - first
    second = jnp.maximum(base + rest, 0.0)
    third = jnp.maximum(base - rest, 0.0)
    volume = jnp.maximum(trace, 0.0)
    energy = 0.25 * (volume * volume) + 0.5 * (
        largest * largest + second * second + third * third
    )
    return energy, trace


def kernel(
    sizes, bx, by, cells,
    index_ref, loads_ref, tough_ref, clamp_ref, load_ref, crack_ref,
    disp_ref, dam_ref, table_ref,
    u0, u1, df0, df1, kk0, kk1, lf, clamp_v, load_v, crack_v, g,
    pa, ra, pb, rb, pc, rc, pm, pcm, hx, hm, hcm, row_v, rows_v, wv, stage_u, stage_d,
    local_sem, m_send, m_recv, w_sem, o_send, o_recv, a_send, a_recv, b_send, b_recv, t_send, t_recv, s_send, s_recv,
):
    ns, nx, ny = sizes
    me_s = lax.axis_index("section")
    me_x = lax.axis_index("gx")
    me_y = lax.axis_index("gy")
    swapped = lax.rem(me_x, 2)

    def place(case, x):
        return case + lax.rem(x + 2, 2) * (1 - 2 * lax.rem(case, 2))

    me_v = place(me_s, me_x)

    def neighbour_id(dx, dy):
        return {"section": place(me_v, me_x + dx), "gx": me_x + dx, "gy": me_y + dy}

    nz = u0.shape[-1]
    us, dfs, kks = (u0, u1), (df0, df1), (kk0, kk1)

    copies = [
        pltpu.make_async_copy(source, target, local_sem.at[i])
        for i, (source, target) in enumerate(
            ((load_ref, load_v), (clamp_ref, clamp_v), (crack_ref, crack_v))
        )
    ]
    for copy in copies:
        copy.start()

    halo_pieces = [(i * PITCH, 8) for i in range(bx + 2 * BORDER + 1)]
    halo_pieces += [(row_of(x, 0), by) for x in (-3, -2, -1, bx, bx + 1, bx + 2)]
    for start, size in halo_pieces:
        for ref in us + dfs:
            for i in range(ref.shape[0]):
                ref[i, pl.ds(start, size), :] = jnp.zeros((size, nz), jnp.float32)
        lf[0, pl.ds(start, size), :] = jnp.zeros((size, nz), jnp.float32)
        lf[1, pl.ds(start, size), :] = jnp.ones((size, nz), jnp.float32)
        for ref in kks:
            ref[pl.ds(start, size), :] = jnp.full((size, nz), outside_stiff, jnp.float32)

    def there(dx, dy):
        return (
            (me_x + dx >= 0) & (me_x + dx < nx) & (me_y + dy >= 0) & (me_y + dy < ny)
        )

    corners = ((-1, -1), (-1, 1), (1, -1), (1, 1))
    sides_x = ((-1, 0), (1, 0))
    sides_y = ((0, -1), (0, 1))
    neighbours = sides_x + sides_y + corners

    barrier = pltpu.get_barrier_semaphore()
    for dx, dy in neighbours:
        @pl.when(there(dx, dy))
        def _(dx=dx, dy=dy):
            pl.semaphore_signal(
                barrier, inc=1, device_id=neighbour_id(dx, dy), device_id_type=MESH
            )
    for r in range(1, ns):
        pl.semaphore_signal(
            barrier, inc=1, device_id={"section": lax.rem(me_s + r, ns)}, device_id_type=MESH
        )

    case = index_ref[0]
    for c in range(3):
        wv[0, c] = jnp.full((8, nz), loads_ref[c, case], jnp.float32)
    for i in (0, 1, 2):
        copies[i].wait()

    def begin(x, carry):
        here = pl.ds(row_of(x, 0), by)
        held = pl.ds(x * by, by)
        load = load_v[held, :].astype(jnp.float32)
        clamp = clamp_v[held, :].astype(jnp.float32)
        crack = crack_v[held, :].astype(jnp.float32)
        lf[0, here, :] = load
        lf[1, here, :] = jnp.maximum(load, clamp)
        df0[0, here, :] = crack
        kk0[here, :] = (1.0 - crack) * (1.0 - crack) + stiff_floor
        return carry

    lax.fori_loop(0, bx, begin, 0, unroll=4)

    for i in range(2):
        for ref, n, first in ((load_v, 3, 0), (crack_v, 2, 3), (clamp_v, 1, 5)):
            for layer in range(n):
                y = layer if i == 0 else by - n + layer
                pm[i, first + layer] = ref[pl.ds(y, bx, stride=by), :]
    for i, (dx, dy) in enumerate(corners):
        x, deep_x = (0, 1) if dx < 0 else (bx - 1, bx - 2)
        y, deep_y = (0, 1) if dy < 0 else (by - 1, by - 2)
        for j, (ref, at_x, at_y) in enumerate((
            (load_v, x, y), (load_v, deep_x, y), (load_v, x, deep_y), (crack_v, x, y),
        )):
            pcm[i, pl.ds(j, 1), :] = ref[pl.ds(at_x * by + at_y, 1), :]

    across = 1 + (me_x > 0).astype(jnp.int32) + (me_x < nx - 1).astype(jnp.int32)
    along = 1 + (me_y > 0).astype(jnp.int32) + (me_y < ny - 1).astype(jnp.int32)
    pl.semaphore_wait(barrier, across * along - 1 + (ns - 1))

    def remote(source, target, send, recv, dx, dy):
        return pltpu.make_async_remote_copy(
            src_ref=source, dst_ref=target, send_sem=send, recv_sem=recv,
            device_id=neighbour_id(dx, dy), device_id_type=MESH,
        )

    def b_copies(field, q, dx, dy):
        found = []
        if dy == 0:
            for layer in range(HALO):
                x = layer if dx < 0 else bx - HALO + layer
                to = bx + layer if dx < 0 else layer - HALO
                i = (0 if dx < 0 else 2) + layer
                found.append(remote(
                    field.at[:, pl.ds(row_of(x, 0), by), :],
                    field.at[:, pl.ds(row_of(to, 0), by), :],
                    b_send.at[q, i], b_recv.at[q, i], dx, dy,
                ))
        elif dx == 0:
            i = 0 if dy < 0 else 1
            found.append(remote(
                pb.at[i], rb.at[q, i], b_send.at[q, 4 + i], b_recv.at[q, 4 + i], dx, dy,
            ))
        else:
            i = corners.index((dx, dy))
            found.append(remote(
                pc.at[i], rc.at[q, i], b_send.at[q, 6 + i], b_recv.at[q, 6 + i], dx, dy,
            ))
        return found

    order_b = corners + sides_x + sides_y

    def send_b(field, q, current):
        for i, (dx, dy) in enumerate(corners):
            row = row_of(0 if dx < 0 else bx - 1, 0 if dy < 0 else by - 1)
            if current is not None:
                for c in range(3):
                    pc[i, pl.ds(c, 1), :] = current[c, pl.ds(row, 1), :]
            for f in range(2):
                pc[i, pl.ds(3 + f, 1), :] = field[f, pl.ds(row, 1), :]
        for i in range(2):
            for f in range(2):
                for layer in range(HALO):
                    y = layer if i == 0 else by - HALO + layer
                    pb[i, f * HALO + layer] = field[
                        f, pl.ds(row_of(0, y), bx, stride=PITCH), :
                    ]
        for dx, dy in order_b:
            @pl.when(there(dx, dy))
            def _(dx=dx, dy=dy):
                for copy in b_copies(field, q, dx, dy):
                    copy.start()

    def sent_b(field, q):
        for dx, dy in order_b:
            @pl.when(there(dx, dy))
            def _(dx=dx, dy=dy):
                for copy in b_copies(field, q, dx, dy):
                    copy.wait_send()

    def take_b(field, q, current):
        for dx, dy in order_b:
            @pl.when(there(-dx, -dy))
            def _(dx=dx, dy=dy):
                for copy in b_copies(field, q, dx, dy):
                    copy.wait_recv()
                if dx == 0:
                    i = 0 if dy < 0 else 1
                    for f in range(2):
                        for layer in range(HALO):
                            y = by + layer if i == 0 else layer - HALO
                            strip = pl.ds(row_of(0, y), bx, stride=PITCH)
                            value = rb[q, i, f * HALO + layer]
                            field[f, strip, :] = value
                            if current is not None and f == 0:
                                kks[q][strip, :] = (1.0 - value) * (1.0 - value) + stiff_floor
                elif dy != 0:
                    i = corners.index((dx, dy))
                    row = row_of(bx if dx < 0 else -1, by if dy < 0 else -1)
                    if current is not None:
                        for c in range(3):
                            current[c, pl.ds(row, 1), :] = rc[q, i, pl.ds(c, 1), :]
                        value = rc[q, i, pl.ds(3, 1), :]
                        kks[q][pl.ds(row, 1), :] = (1.0 - value) * (1.0 - value) + stiff_floor
                    for f in range(2):
                        field[f, pl.ds(row, 1), :] = rc[q, i, pl.ds(3 + f, 1), :]
        if current is not None:
            for x in (-2, -1, bx, bx + 1):
                here = pl.ds(row_of(x, 0), by)
                value = field[0, here, :]
                kks[q][here, :] = (1.0 - value) * (1.0 - value) + stiff_floor

    def a_copy(q, dx, dy):
        if dy == 0:
            i = 0 if dx < 0 else 1
            x, to = (1, bx + 1) if dx < 0 else (bx - 2, -2)
            return remote(
                us[q].at[:, pl.ds(row_of(x, 0), by), :],
                us[q].at[:, pl.ds(row_of(to, 0), by), :],
                a_send.at[q, i], a_recv.at[q, i], dx, dy,
            )
        i = 0 if dy < 0 else 1
        return remote(
            pa.at[i], ra.at[q, i], a_send.at[q, 2 + i], a_recv.at[q, 2 + i], dx, dy,
        )

    def send_a(q):
        for i in range(2):
            y = 1 if i == 0 else by - 2
            for c in range(3):
                pa[i, c] = us[q][c, pl.ds(row_of(0, y), bx, stride=PITCH), :]
        for dx, dy in sides_x + sides_y:
            @pl.when(there(dx, dy))
            def _(dx=dx, dy=dy):
                a_copy(q, dx, dy).start()

    def sent_a(q):
        for dx, dy in sides_x + sides_y:
            @pl.when(there(dx, dy))
            def _(dx=dx, dy=dy):
                a_copy(q, dx, dy).wait_send()

    def take_a(q):
        for dx, dy in sides_x + sides_y:
            @pl.when(there(-dx, -dy))
            def _(dx=dx, dy=dy):
                a_copy(q, dx, dy).wait_recv()
                if dx == 0:
                    i = 0 if dy < 0 else 1
                    y = by + 1 if i == 0 else -2
                    for c in range(3):
                        us[q][c, pl.ds(row_of(0, y), bx, stride=PITCH), :] = ra[q, i, c]

    def tough_target(r):
        return place(lax.rem(me_s + ns - r, ns), me_x)

    def tough_copy(r):
        return pltpu.make_async_remote_copy(
            src_ref=tough_ref, dst_ref=g.at[r], send_sem=t_send.at[r], recv_sem=t_recv.at[r],
            device_id={"section": tough_target(r)}, device_id_type=MESH,
        )

    def tough_arrived(r):
        pltpu.make_async_copy(tough_ref, g.at[r], t_recv.at[r]).wait()

    masks = (load_v, crack_v, clamp_v)
    layers = (3, 2, 1)
    parts = tuple((ref, n, sum(layers[:i])) for i, (ref, n) in enumerate(zip(masks, layers)))

    def m_copies(dx, dy):
        if dy == 0:
            i = 0 if dx < 0 else 1
            return [
                remote(
                    ref.at[pl.ds((0 if dx < 0 else bx - n) * by, n * by), :],
                    hx.at[i, pl.ds(first * by, n * by), :],
                    m_send.at[3 * i + j], m_recv.at[3 * i + j], dx, dy,
                )
                for j, (ref, n, first) in enumerate(parts)
            ]
        if dx == 0:
            i = 0 if dy < 0 else 1
            return [remote(pm.at[i], hm.at[i], m_send.at[6 + i], m_recv.at[6 + i], dx, dy)]
        i = corners.index((dx, dy))
        return [remote(pcm.at[i], hcm.at[i], m_send.at[8 + i], m_recv.at[8 + i], dx, dy)]

    for dx, dy in order_b:
        @pl.when(there(dx, dy))
        def _(dx=dx, dy=dy):
            for copy in m_copies(dx, dy):
                copy.start()
    partner = me_s + 1 - 2 * lax.rem(me_s, 2)
    w_copy = pltpu.make_async_remote_copy(
        src_ref=wv.at[0], dst_ref=wv.at[1], send_sem=w_sem.at[0], recv_sem=w_sem.at[1],
        device_id={"section": partner}, device_id_type=MESH,
    )
    w_copy.start()
    for r in range(ns):
        @pl.when(tough_target(r) == me_s)
        def _(r=r):
            pltpu.make_async_copy(tough_ref, g.at[r], t_recv.at[r]).start()

        @pl.when(tough_target(r) != me_s)
        def _(r=r):
            tough_copy(r).start()

    lane = lax.broadcasted_iota(jnp.int32, (by, nz), 1)
    at_low = lane == 0
    at_high = lane == nz - 1

    def from_low(value, edge):
        return jnp.where(at_low, edge, pltpu.roll(value, 1, 1))

    def from_high(value, edge):
        return jnp.where(at_high, edge, pltpu.roll(value, nz - 1, 1))

    def span(start, stride):
        return pl.ds(start, by) if stride == 1 else pl.ds(start, bx, stride=stride)

    def as_float(value):
        return value.astype(jnp.float32)

    def put_crack(where, crack):
        crack = as_float(crack)
        df0[0, where, :] = crack
        kk0[where, :] = (1.0 - crack) * (1.0 - crack) + stiff_floor

    def outward(low, n, layer, size):
        return size + layer if low else layer - n

    w_copy.wait_recv()
    for dx, dy in order_b:
        @pl.when(there(-dx, -dy))
        def _(dx=dx, dy=dy):
            for copy in m_copies(dx, dy):
                copy.wait_recv()
            if dy == 0:
                i, low = (0, True) if dx < 0 else (1, False)
                for layer in range(3):
                    here = pl.ds(row_of(outward(low, 3, layer, bx), 0), by)
                    lf[0, here, :] = as_float(hx[i, pl.ds(layer * by, by), :])
                for layer in range(2):
                    here = pl.ds(row_of(outward(low, 2, layer, bx), 0), by)
                    put_crack(here, hx[i, pl.ds((3 + layer) * by, by), :])
                near = 0 if low else 2
                here = pl.ds(row_of(bx if low else -1, 0), by)
                lf[1, here, :] = as_float(jnp.maximum(
                    hx[i, pl.ds(near * by, by), :], hx[i, pl.ds(5 * by, by), :]
                ))
            elif dx == 0:
                i, low = (0, True) if dy < 0 else (1, False)
                for layer in range(3):
                    y = outward(low, 3, layer, by)
                    lf[0, pl.ds(row_of(0, y), bx, stride=PITCH), :] = as_float(hm[i, layer])
                for layer in range(2):
                    y = outward(low, 2, layer, by)
                    put_crack(pl.ds(row_of(0, y), bx, stride=PITCH), hm[i, 3 + layer])
                near = 0 if low else 2
                y = by if low else -1
                lf[1, pl.ds(row_of(0, y), bx, stride=PITCH), :] = as_float(
                    jnp.maximum(hm[i, near], hm[i, 5])
                )
            else:
                i = corners.index((dx, dy))
                x, far_x = (bx, bx + 1) if dx < 0 else (-1, -2)
                y, far_y = (by, by + 1) if dy < 0 else (-1, -2)
                for j, (at_x, at_y) in enumerate(((x, y), (far_x, y), (x, far_y))):
                    lf[0, pl.ds(row_of(at_x, at_y), 1), :] = as_float(hcm[i, pl.ds(j, 1), :])
                put_crack(pl.ds(row_of(x, y), 1), hcm[i, pl.ds(3, 1), :])

    vector = [wv[swapped, c] for c in range(3)]

    def fill(x, carry):
        for here in (x * PITCH, x * PITCH + 8, x * PITCH + 16):
            load = lf[0, pl.ds(here, 8), :]
            for c in range(3):
                u0[c, pl.ds(here, 8), :] = load * vector[c]
        return carry

    lax.fori_loop(0, bx + 2 * BORDER, fill, 0, unroll=2)
    tail = pl.ds((bx + 2 * BORDER) * PITCH, 8)
    for c in range(3):
        u0[c, tail, :] = lf[0, tail, :] * vector[c]
    vector = [jnp.concatenate([v, v], axis=0) for v in vector]

    def first_flow(start, stride, count):
        def at(offset, c):
            if stride == 1:
                return u0[c, pl.ds(start + offset, count), :]
            return u0[c, pl.ds(start + offset, count, stride=stride), :]

        to = pl.ds(start, count) if stride == 1 else pl.ds(start, count, stride=stride)
        value = at(0, 2)
        high = jnp.where(at_high[:count], 0.0, pltpu.roll(value, nz - 1, 1))
        low = jnp.where(at_low[:count], 0.0, pltpu.roll(value, 1, 1))
        trace = at(PITCH, 0) - at(-PITCH, 0) + at(1, 1) - at(-1, 1) + (high - low)
        df0[1, to, :] = kk0[to, :] * (0.5 * trace)

    def first_flow_own(x, carry):
        first_flow(row_of(x, 0), 1, by)
        return carry

    lax.fori_loop(0, bx, first_flow_own, 0, unroll=4)
    for dx, dy in order_b:
        @pl.when(there(-dx, -dy))
        def _(dx=dx, dy=dy):
            xs = (bx, bx + 1) if dx < 0 else (-2, -1)
            ys = (by, by + 1) if dy < 0 else (-2, -1)
            if dy == 0:
                for x in xs:
                    first_flow(row_of(x, 0), 1, by)
            elif dx == 0:
                for y in ys:
                    first_flow(row_of(0, y), PITCH, bx)
            else:
                first_flow(row_of(bx if dx < 0 else -1, by if dy < 0 else -1), 1, 1)

    def move(p, start, stride):
        df, u, kk = dfs[p], us[p], kks[p]

        def at(ref, offset, *lead):
            return ref[(*lead, span(start + offset, stride), slice(None))]

        k = at(kk, 0)
        k_xm, k_xp = at(kk, -PITCH), at(kk, PITCH)
        k_ym, k_yp = at(kk, -1), at(kk, 1)
        k_zm, k_zp = from_low(k, outside_stiff), from_high(k, outside_stiff)
        pairs = (k_xm + k_xp, k_ym + k_yp, k_zm + k_zp)
        total = 6.0 * k + (pairs[0] + pairs[1] + pairs[2])
        w_xm, w_xp, w_ym, w_yp = k + k_xm, k + k_xp, k + k_ym, k + k_yp
        w_zm = jnp.where(at_low, 0.0, k + k_zm)
        w_zp = jnp.where(at_high, 0.0, k + k_zp)
        middle_flow = at(df, 0, 1)
        slopes = (
            at(df, PITCH, 1) - at(df, -PITCH, 1),
            at(df, 1, 1) - at(df, -1, 1),
            from_high(middle_flow, 0.0) - from_low(middle_flow, 0.0),
        )
        fixed = at(lf, 0, 1) > 0.5
        load = at(lf, 0, 0)
        squares = None
        for c in range(3):
            here = at(u, 0, c)
            total_c = (
                w_xm * at(u, -PITCH, c) + w_xp * at(u, PITCH, c)
                + w_ym * at(u, -1, c) + w_yp * at(u, 1, c)
                + w_zm * pltpu.roll(here, 1, 1) + w_zp * pltpu.roll(here, nz - 1, 1)
            )
            residual = total_c - total * here + 2.0 * slopes[c]
            relaxed = here + relax_weight * residual / (total + pairs[c])
            us[1 - p][c, span(start, stride), :] = jnp.where(fixed, load * vector[c], relaxed)
            square = residual * residual
            squares = square if squares is None else squares + square
        return jnp.where(fixed, 0.0, squares)

    def heal(p, r, start, stride, held):
        q = 1 - p
        df, u = dfs[p], us[q]

        def at(ref, offset, *lead):
            return ref[(*lead, span(start + offset, stride), slice(None))]

        grads = []
        for c in range(3):
            here = at(u, 0, c)
            grads.append((
                at(u, PITCH, c) - at(u, -PITCH, c),
                at(u, 1, c) - at(u, -1, c),
                from_high(here, 0.0) - from_low(here, 0.0),
            ))
        energy, trace = twice_energy(
            grads[0][0], grads[1][1], grads[2][2],
            0.5 * (grads[0][1] + grads[1][0]),
            0.5 * (grads[0][2] + grads[2][0]),
            0.5 * (grads[1][2] + grads[2][1]),
        )
        here = at(df, 0, 0)
        beside = (
            at(df, PITCH, 0) + at(df, -PITCH, 0) + at(df, 1, 0) + at(df, -1, 0)
            + from_high(here, 0.0) + from_low(here, 0.0)
        )
        rate = g[r, held, :]
        renewed = (energy + rate * beside) / (energy + 7.0 * rate)
        renewed = jnp.where(crack_v[held, :] > 0, 1.0, renewed)
        stiff = (1.0 - renewed) * (1.0 - renewed) + stiff_floor
        to = span(start, stride)
        dfs[q][0, to, :] = renewed
        dfs[q][1, to, :] = stiff * (0.5 * trace)
        kks[q][to, :] = stiff

    columns = lax.broadcasted_iota(jnp.int32, (1, nz), 1)
    y_of = lax.broadcasted_iota(jnp.int32, (by, nz), 0)
    at_rim = (y_of == 0) | (y_of == by - 1)

    def in_groups(low, high, body, total):
        steps = 2 if (high - low) % 2 == 0 else 1
        size = (high - low) // steps

        def step(i, total):
            for j in range(size):
                added = body(low + i * size + j)
                total = total if added is None else total + added
            return total

        return lax.fori_loop(0, steps, step, total)

    def sweep(r, p, table, first=False, last=False):
        q = 1 - p

        def move_slab(x):
            return move(p, row_of(x, 0), 1)

        def move_strip(y):
            return move(p, row_of(0, y), PITCH)

        def heal_slab(x):
            heal(p, r, row_of(x, 0), 1, pl.ds(x * by, by))

        def heal_strip(y):
            heal(p, r, row_of(0, y), PITCH, pl.ds(y, bx, stride=by))

        nothing = jnp.zeros((by, nz), jnp.float32)
        squares = in_groups(1, bx - 1, move_slab, nothing)
        tough_arrived(r)
        in_groups(2, bx - 2, heal_slab, 0)

        if not first:
            take_a(p)
            take_b(dfs[p], p, us[p])
        for x in (0, bx - 1):
            squares = squares + move_slab(x)
        squares = jnp.where(at_rim, 0.0, squares)
        for y in (0, by - 1):
            squares = squares + move_strip(y)
        for x in (-1, bx):
            move_slab(x)
        for y in (-1, by):
            move_strip(y)
        if not first:
            sent_a(p)
        if not last:
            send_a(q)
        total = jnp.sum(jnp.sum(squares, axis=0, keepdims=True), axis=1, keepdims=True)
        column = lax.rem(me_v + r, ns)
        table = jnp.where(columns == column, jnp.broadcast_to(total, (1, nz)), table)
        if last:
            spread_sums(table)
            give_displacement(us[q])
        for x in (0, 1, bx - 2, bx - 1):
            heal_slab(x)
        for y in (0, 1, by - 2, by - 1):
            heal_strip(y)
        if not first:
            sent_b(dfs[p], p)
        if not last:
            send_b(dfs[q], q, us[q])
        else:
            give_damage(dfs[q])
        return table

    def give(stage, out_ref, i):
        return pltpu.make_async_remote_copy(
            src_ref=stage, dst_ref=out_ref.at[0], send_sem=o_send.at[i], recv_sem=o_recv.at[i],
            device_id={"section": partner}, device_id_type=MESH,
        )

    give_u = give(stage_u, disp_ref, 0)
    give_d = give(stage_d, dam_ref, 1)

    def give_displacement(u):
        @pl.when(swapped == 0)
        def _():
            for x in range(bx):
                for c in range(3):
                    disp_ref[0, c, x] = u[c, pl.ds(row_of(x, 0), by), :]

        @pl.when(swapped == 1)
        def _():
            for x in range(bx):
                for c in range(3):
                    stage_u[c, x] = u[c, pl.ds(row_of(x, 0), by), :]
            give_u.start()

    def give_damage(df):
        @pl.when(swapped == 0)
        def _():
            for x in range(bx):
                dam_ref[0, x] = df[0, pl.ds(row_of(x, 0), by), :]

        @pl.when(swapped == 1)
        def _():
            for x in range(bx):
                stage_d[x] = df[0, pl.ds(row_of(x, 0), by), :]
            give_d.start()

    me = me_x * ny + me_y

    def sums_copy(t):
        to = lax.rem(me + t, nx * ny)
        return pltpu.make_async_remote_copy(
            src_ref=row_v, dst_ref=rows_v.at[me], send_sem=s_send.at[t], recv_sem=s_recv.at[t],
            device_id={"section": me_v, "gx": to // ny, "gy": lax.rem(to, ny)},
            device_id_type=MESH,
        )

    def sums_arrived(t):
        source = lax.rem(me + nx * ny - t, nx * ny)
        pltpu.make_async_copy(row_v, rows_v.at[source], s_recv.at[t]).wait()

    def spread_sums(table):
        row_v[...] = table

        @pl.when(swapped == 0)
        def _():
            rows_v[me] = table

        @pl.when(swapped == 1)
        def _():
            sums_copy(0).start()

        def start(t, carry):
            sums_copy(t).start()
            return carry

        lax.fori_loop(1, nx * ny, start, 0)

    def two_sweeps(i, table):
        return sweep(2 * i + 2, 0, sweep(2 * i + 1, 1, table))

    table = sweep(0, 0, jnp.zeros((1, nz), jnp.float32), first=True)
    table = lax.fori_loop(0, (ns - 2) // 2, two_sweeps, table)
    sweep(ns - 1, 1, table, last=True)

    w_copy.wait_send()
    for dx, dy in order_b:
        @pl.when(there(dx, dy))
        def _(dx=dx, dy=dy):
            for copy in m_copies(dx, dy):
                copy.wait_send()

    for r in range(ns):
        @pl.when(tough_target(r) != me_s)
        def _(r=r):
            tough_copy(r).wait_send()

    @pl.when(swapped == 1)
    def _():
        sums_copy(0).wait_send()
        sums_arrived(0)
        for copy in (give_u, give_d):
            copy.wait_send()
            copy.wait_recv()

    def finish(t, carry):
        sums_copy(t).wait_send()
        sums_arrived(t)
        return carry

    lax.fori_loop(1, nx * ny, finish, 0)
    everything = rows_v[0]
    for i in range(1, nx * ny):
        everything = everything + rows_v[i]
    result = jnp.sqrt(everything * (0.25 / (3.0 * cells)))
    table_ref[...] = result[:, :ns]


def on_device(sizes, load_index, load_table, toughness, clamp_mask, load_mask, crack_mask):
    ns, nx, ny = sizes
    bx, by, nz = clamp_mask.shape
    cells = float(clamp_mask.size * nx * ny)
    rows = (bx + 2 * BORDER) * PITCH + LEAD
    flat = (bx * by, nz)
    f32 = jnp.float32
    scratch = [
        pltpu.VMEM((3, rows, nz), f32),
        pltpu.VMEM((3, rows, nz), f32),
        pltpu.VMEM((2, rows, nz), f32),
        pltpu.VMEM((2, rows, nz), f32),
        pltpu.VMEM((rows, nz), f32),
        pltpu.VMEM((rows, nz), f32),
        pltpu.VMEM((2, rows, nz), f32),
        pltpu.VMEM(flat, jnp.int32),
        pltpu.VMEM(flat, jnp.int32),
        pltpu.VMEM(flat, jnp.int32),
        pltpu.VMEM((ns, *flat), f32),
        pltpu.VMEM((2, 3, bx, nz), f32),
        pltpu.VMEM((2, 2, 3, bx, nz), f32),
        pltpu.VMEM((2, 2 * HALO, bx, nz), f32),
        pltpu.VMEM((2, 2, 2 * HALO, bx, nz), f32),
        pltpu.VMEM((4, 8, nz), f32),
        pltpu.VMEM((2, 4, 8, nz), f32),
        pltpu.VMEM((2, 6, bx, nz), jnp.int32),
        pltpu.VMEM((4, 8, nz), jnp.int32),
        pltpu.VMEM((2, 6 * by, nz), jnp.int32),
        pltpu.VMEM((2, 6, bx, nz), jnp.int32),
        pltpu.VMEM((4, 8, nz), jnp.int32),
        pltpu.VMEM((1, nz), f32),
        pltpu.VMEM((nx * ny, 1, nz), f32),
        pltpu.VMEM((2, 3, 8, nz), f32),
        pltpu.VMEM((3, bx, by, nz), f32),
        pltpu.VMEM((bx, by, nz), f32),
        pltpu.SemaphoreType.DMA((3,)),
        pltpu.SemaphoreType.DMA((12,)),
        pltpu.SemaphoreType.DMA((12,)),
        pltpu.SemaphoreType.DMA((2,)),
        pltpu.SemaphoreType.DMA((2,)),
        pltpu.SemaphoreType.DMA((2,)),
        pltpu.SemaphoreType.DMA((2, 4)),
        pltpu.SemaphoreType.DMA((2, 4)),
        pltpu.SemaphoreType.DMA((2, 10)),
        pltpu.SemaphoreType.DMA((2, 10)),
        pltpu.SemaphoreType.DMA((ns,)),
        pltpu.SemaphoreType.DMA((ns,)),
        pltpu.SemaphoreType.DMA((nx * ny,)),
        pltpu.SemaphoreType.DMA((nx * ny,)),
    ]
    smem = pl.BlockSpec(memory_space=pltpu.SMEM)
    vmem = pl.BlockSpec(memory_space=pltpu.VMEM)
    hbm = pl.BlockSpec(memory_space=pl.ANY)
    return pl.pallas_call(
        functools.partial(kernel, sizes, bx, by, cells),
        out_shape=(
            pltpu.VMEM((1, 3, bx, by, nz), f32),
            pltpu.VMEM((1, bx, by, nz), f32),
            pltpu.VMEM((1, ns), f32),
        ),
        in_specs=[smem, smem, hbm, hbm, hbm, hbm],
        out_specs=(vmem, vmem, vmem),
        scratch_shapes=scratch,
        compiler_params=pltpu.CompilerParams(collective_id=0, has_side_effects=True),
        name="sweeps",
    )(
        load_index,
        load_table.T,
        toughness.reshape(flat),
        clamp_mask.reshape(flat),
        load_mask.reshape(flat),
        crack_mask.reshape(flat),
    )


def solution(mesh):
    sizes = (mesh.shape["section"], mesh.shape["gx"], mesh.shape["gy"])
    in_specs = (
        P("section"),
        P(),
        P("section", "gx", "gy", None),
        P("gx", "gy", None),
        P("gx", "gy", None),
        P("gx", "gy", None),
    )
    out_specs = (
        P("section", None, "gx", "gy", None),
        P("section", "gx", "gy", None),
        P("section", None),
    )
    return jax.shard_map(
        functools.partial(on_device, sizes),
        mesh=mesh, in_specs=in_specs, out_specs=out_specs, check_vma=False,
    )
```

```python
import functools

import jax
import jax.numpy as jnp
from jax import lax
from jax.experimental import pallas as pl
from jax.experimental.pallas import tpu as pltpu
from jax.sharding import PartitionSpec as P

MESH = pl.DeviceIdType.MESH
relax_weight = 0.6
stiff_floor = 0.001
eigen_guard = 1e-08
outside_stiff = 1.001

cos_third = (
    0.8660254053677892, 0.166666399623719, -0.0481050217302989, 0.024608831949810825,
    -0.015124763172089219, 0.009420074574188678, -0.004972568153766589,
    0.0017909605462136829, -0.0003093201852607309,
)
sin_third = (
    0.49999999939158213, -0.038675031951822925, 0.015381770818675887, -0.00862700282428075,
    0.005525819902144846, -0.0035154216998851246, 0.0018763805597984632,
    -0.0006797757027300123, 0.00011778274999869613,
)

PITCH = 24
LEAD = 8
HALO = 2
BORDER = 3


def row_of(x, y):
    return (x + BORDER) * PITCH + LEAD + y


def polynomial(coefficients, t):
    value = coefficients[-1]
    for coefficient in coefficients[-2::-1]:
        value = value * t + coefficient
    return value


def twice_energy(a, b, c, d, e, f):
    trace = a + b + c
    middle = trace * (1.0 / 3.0)
    a, b, c = a - middle, b - middle, c - middle
    dd, ee, ff = d * d, e * e, f * f
    spread = (a * a + b * b + c * c) * (1.0 / 6.0) + (dd + ee + ff) * (1.0 / 3.0)
    guarded = spread + 4.0 * eigen_guard
    determinant = a * (b * c - ff) - d * (d * c - f * e) + e * (d * f - b * e)
    inverse = lax.rsqrt(guarded)
    ratio = determinant * (0.5 * inverse) * (inverse * inverse)
    size = jnp.minimum(jnp.abs(ratio), 1.0)
    radius = jnp.sqrt(spread)
    first = radius * polynomial(cos_third, size)
    first = jnp.where(ratio < 0.0, -first, first)
    rest = radius * (1.7320508075688772 * jnp.sqrt(1.0 - size)) * polynomial(sin_third, size)
    largest = jnp.maximum(middle + 2.0 * first, 0.0)
    base = middle - first
    second = jnp.maximum(base + rest, 0.0)
    third = jnp.maximum(base - rest, 0.0)
    volume = jnp.maximum(trace, 0.0)
    energy = 0.25 * (volume * volume) + 0.5 * (
        largest * largest + second * second + third * third
    )
    return energy, trace


def kernel(
    sizes, bx, by, cells,
    index_ref, loads_ref, tough_ref, clamp_ref, load_ref, crack_ref,
    disp_ref, dam_ref, table_ref,
    u0, u1, df0, df1, kk0, kk1, lf, clamp_v, load_v, crack_v, g,
    pa, ra, pb, rb, pc, rc, pm, pcm, hx, hm, hcm, row_v, rows_v, wv, stage_u, stage_d,
    local_sem, m_send, m_recv, w_sem, o_send, o_recv, a_send, a_recv, b_send, b_recv, t_send, t_recv, s_send, s_recv,
):
    ns, nx, ny = sizes
    me_s = lax.axis_index("section")
    me_x = lax.axis_index("gx")
    me_y = lax.axis_index("gy")
    swapped = lax.rem(me_x, 2)

    def place(case, x):
        return case + lax.rem(x + 2, 2) * (1 - 2 * lax.rem(case, 2))

    me_v = place(me_s, me_x)

    def neighbour_id(dx, dy):
        return {"section": place(me_v, me_x + dx), "gx": me_x + dx, "gy": me_y + dy}

    nz = u0.shape[-1]
    us, dfs, kks = (u0, u1), (df0, df1), (kk0, kk1)

    copies = [
        pltpu.make_async_copy(source, target, local_sem.at[i])
        for i, (source, target) in enumerate(
            ((load_ref, load_v), (clamp_ref, clamp_v), (crack_ref, crack_v))
        )
    ]
    for copy in copies:
        copy.start()

    halo_pieces = [(i * PITCH, 8) for i in range(bx + 2 * BORDER + 1)]
    halo_pieces += [(row_of(x, 0), by) for x in (-3, -2, -1, bx, bx + 1, bx + 2)]
    for start, size in halo_pieces:
        for ref in us + dfs:
            for i in range(ref.shape[0]):
                ref[i, pl.ds(start, size), :] = jnp.zeros((size, nz), jnp.float32)
        lf[0, pl.ds(start, size), :] = jnp.zeros((size, nz), jnp.float32)
        lf[1, pl.ds(start, size), :] = jnp.ones((size, nz), jnp.float32)
        for ref in kks:
            ref[pl.ds(start, size), :] = jnp.full((size, nz), outside_stiff, jnp.float32)

    def there(dx, dy):
        return (
            (me_x + dx >= 0) & (me_x + dx < nx) & (me_y + dy >= 0) & (me_y + dy < ny)
        )

    corners = ((-1, -1), (-1, 1), (1, -1), (1, 1))
    sides_x = ((-1, 0), (1, 0))
    sides_y = ((0, -1), (0, 1))
    neighbours = sides_x + sides_y + corners

    barrier = pltpu.get_barrier_semaphore()
    for dx, dy in neighbours:
        @pl.when(there(dx, dy))
        def _(dx=dx, dy=dy):
            pl.semaphore_signal(
                barrier, inc=1, device_id=neighbour_id(dx, dy), device_id_type=MESH
            )
    for r in range(1, ns):
        pl.semaphore_signal(
            barrier, inc=1, device_id={"section": lax.rem(me_s + r, ns)}, device_id_type=MESH
        )

    case = index_ref[0]
    for c in range(3):
        wv[0, c] = jnp.full((8, nz), loads_ref[c, case], jnp.float32)
    for i in (0, 1, 2):
        copies[i].wait()

    def begin(x, carry):
        here = pl.ds(row_of(x, 0), by)
        held = pl.ds(x * by, by)
        load = load_v[held, :].astype(jnp.float32)
        clamp = clamp_v[held, :].astype(jnp.float32)
        crack = crack_v[held, :].astype(jnp.float32)
        lf[0, here, :] = load
        lf[1, here, :] = jnp.maximum(load, clamp)
        df0[0, here, :] = crack
        kk0[here, :] = (1.0 - crack) * (1.0 - crack) + stiff_floor
        return carry

    lax.fori_loop(0, bx, begin, 0, unroll=4)

    for i in range(2):
        for ref, n, first in ((load_v, 3, 0), (crack_v, 2, 3), (clamp_v, 1, 5)):
            for layer in range(n):
                y = layer if i == 0 else by - n + layer
                pm[i, first + layer] = ref[pl.ds(y, bx, stride=by), :]
    for i, (dx, dy) in enumerate(corners):
        x, deep_x = (0, 1) if dx < 0 else (bx - 1, bx - 2)
        y, deep_y = (0, 1) if dy < 0 else (by - 1, by - 2)
        for j, (ref, at_x, at_y) in enumerate((
            (load_v, x, y), (load_v, deep_x, y), (load_v, x, deep_y), (crack_v, x, y),
        )):
            pcm[i, pl.ds(j, 1), :] = ref[pl.ds(at_x * by + at_y, 1), :]

    across = 1 + (me_x > 0).astype(jnp.int32) + (me_x < nx - 1).astype(jnp.int32)
    along = 1 + (me_y > 0).astype(jnp.int32) + (me_y < ny - 1).astype(jnp.int32)
    pl.semaphore_wait(barrier, across * along - 1 + (ns - 1))

    def remote(source, target, send, recv, dx, dy):
        return pltpu.make_async_remote_copy(
            src_ref=source, dst_ref=target, send_sem=send, recv_sem=recv,
            device_id=neighbour_id(dx, dy), device_id_type=MESH,
        )

    def b_copies(field, q, dx, dy):
        found = []
        if dy == 0:
            for layer in range(HALO):
                x = layer if dx < 0 else bx - HALO + layer
                to = bx + layer if dx < 0 else layer - HALO
                i = (0 if dx < 0 else 2) + layer
                found.append(remote(
                    field.at[:, pl.ds(row_of(x, 0), by), :],
                    field.at[:, pl.ds(row_of(to, 0), by), :],
                    b_send.at[q, i], b_recv.at[q, i], dx, dy,
                ))
        elif dx == 0:
            i = 0 if dy < 0 else 1
            found.append(remote(
                pb.at[i], rb.at[q, i], b_send.at[q, 4 + i], b_recv.at[q, 4 + i], dx, dy,
            ))
        else:
            i = corners.index((dx, dy))
            found.append(remote(
                pc.at[i], rc.at[q, i], b_send.at[q, 6 + i], b_recv.at[q, 6 + i], dx, dy,
            ))
        return found

    order_b = corners + sides_x + sides_y

    def send_b(field, q, current):
        for i, (dx, dy) in enumerate(corners):
            row = row_of(0 if dx < 0 else bx - 1, 0 if dy < 0 else by - 1)
            if current is not None:
                for c in range(3):
                    pc[i, pl.ds(c, 1), :] = current[c, pl.ds(row, 1), :]
            for f in range(2):
                pc[i, pl.ds(3 + f, 1), :] = field[f, pl.ds(row, 1), :]
        for i in range(2):
            for f in range(2):
                for layer in range(HALO):
                    y = layer if i == 0 else by - HALO + layer
                    pb[i, f * HALO + layer] = field[
                        f, pl.ds(row_of(0, y), bx, stride=PITCH), :
                    ]
        for dx, dy in order_b:
            @pl.when(there(dx, dy))
            def _(dx=dx, dy=dy):
                for copy in b_copies(field, q, dx, dy):
                    copy.start()

    def sent_b(field, q):
        for dx, dy in order_b:
            @pl.when(there(dx, dy))
            def _(dx=dx, dy=dy):
                for copy in b_copies(field, q, dx, dy):
                    copy.wait_send()

    def take_b(field, q, current, directions):
        for dx, dy in directions:
            @pl.when(there(-dx, -dy))
            def _(dx=dx, dy=dy):
                for copy in b_copies(field, q, dx, dy):
                    copy.wait_recv()
                if dx == 0:
                    i = 0 if dy < 0 else 1
                    for f in range(2):
                        for layer in range(HALO):
                            y = by + layer if i == 0 else layer - HALO
                            strip = pl.ds(row_of(0, y), bx, stride=PITCH)
                            value = rb[q, i, f * HALO + layer]
                            field[f, strip, :] = value
                            if current is not None and f == 0:
                                kks[q][strip, :] = (1.0 - value) * (1.0 - value) + stiff_floor
                elif dy != 0:
                    i = corners.index((dx, dy))
                    row = row_of(bx if dx < 0 else -1, by if dy < 0 else -1)
                    if current is not None:
                        for c in range(3):
                            current[c, pl.ds(row, 1), :] = rc[q, i, pl.ds(c, 1), :]
                        value = rc[q, i, pl.ds(3, 1), :]
                        kks[q][pl.ds(row, 1), :] = (1.0 - value) * (1.0 - value) + stiff_floor
                    for f in range(2):
                        field[f, pl.ds(row, 1), :] = rc[q, i, pl.ds(3 + f, 1), :]
        if directions is not corners:
            for x in (-2, -1, bx, bx + 1):
                here = pl.ds(row_of(x, 0), by)
                value = field[0, here, :]
                kks[q][here, :] = (1.0 - value) * (1.0 - value) + stiff_floor

    def a_copy(q, dx, dy):
        if dy == 0:
            i = 0 if dx < 0 else 1
            x, to = (1, bx + 1) if dx < 0 else (bx - 2, -2)
            return remote(
                us[q].at[:, pl.ds(row_of(x, 0), by), :],
                us[q].at[:, pl.ds(row_of(to, 0), by), :],
                a_send.at[q, i], a_recv.at[q, i], dx, dy,
            )
        i = 0 if dy < 0 else 1
        return remote(
            pa.at[i], ra.at[q, i], a_send.at[q, 2 + i], a_recv.at[q, 2 + i], dx, dy,
        )

    def send_a(q):
        for i in range(2):
            y = 1 if i == 0 else by - 2
            for c in range(3):
                pa[i, c] = us[q][c, pl.ds(row_of(0, y), bx, stride=PITCH), :]
        for dx, dy in sides_x + sides_y:
            @pl.when(there(dx, dy))
            def _(dx=dx, dy=dy):
                a_copy(q, dx, dy).start()

    def sent_a(q):
        for dx, dy in sides_x + sides_y:
            @pl.when(there(dx, dy))
            def _(dx=dx, dy=dy):
                a_copy(q, dx, dy).wait_send()

    def take_a(q):
        for dx, dy in sides_x + sides_y:
            @pl.when(there(-dx, -dy))
            def _(dx=dx, dy=dy):
                a_copy(q, dx, dy).wait_recv()
                if dx == 0:
                    i = 0 if dy < 0 else 1
                    y = by + 1 if i == 0 else -2
                    for c in range(3):
                        us[q][c, pl.ds(row_of(0, y), bx, stride=PITCH), :] = ra[q, i, c]

    def tough_target(r):
        return place(lax.rem(me_s + ns - r, ns), me_x)

    def tough_copy(r):
        return pltpu.make_async_remote_copy(
            src_ref=tough_ref, dst_ref=g.at[r], send_sem=t_send.at[r], recv_sem=t_recv.at[r],
            device_id={"section": tough_target(r)}, device_id_type=MESH,
        )

    def tough_arrived(r):
        pltpu.make_async_copy(tough_ref, g.at[r], t_recv.at[r]).wait()

    masks = (load_v, crack_v, clamp_v)
    layers = (3, 2, 1)
    parts = tuple((ref, n, sum(layers[:i])) for i, (ref, n) in enumerate(zip(masks, layers)))

    def m_copies(dx, dy):
        if dy == 0:
            i = 0 if dx < 0 else 1
            return [
                remote(
                    ref.at[pl.ds((0 if dx < 0 else bx - n) * by, n * by), :],
                    hx.at[i, pl.ds(first * by, n * by), :],
                    m_send.at[3 * i + j], m_recv.at[3 * i + j], dx, dy,
                )
                for j, (ref, n, first) in enumerate(parts)
            ]
        if dx == 0:
            i = 0 if dy < 0 else 1
            return [remote(pm.at[i], hm.at[i], m_send.at[6 + i], m_recv.at[6 + i], dx, dy)]
        i = corners.index((dx, dy))
        return [remote(pcm.at[i], hcm.at[i], m_send.at[8 + i], m_recv.at[8 + i], dx, dy)]

    for dx, dy in order_b:
        @pl.when(there(dx, dy))
        def _(dx=dx, dy=dy):
            for copy in m_copies(dx, dy):
                copy.start()
    partner = me_s + 1 - 2 * lax.rem(me_s, 2)
    w_copy = pltpu.make_async_remote_copy(
        src_ref=wv.at[0], dst_ref=wv.at[1], send_sem=w_sem.at[0], recv_sem=w_sem.at[1],
        device_id={"section": partner}, device_id_type=MESH,
    )
    w_copy.start()
    for r in range(ns):
        @pl.when(tough_target(r) == me_s)
        def _(r=r):
            pltpu.make_async_copy(tough_ref, g.at[r], t_recv.at[r]).start()

        @pl.when(tough_target(r) != me_s)
        def _(r=r):
            tough_copy(r).start()

    lane = lax.broadcasted_iota(jnp.int32, (by, nz), 1)
    at_low = lane == 0
    at_high = lane == nz - 1

    def from_low(value, edge):
        return jnp.where(at_low, edge, pltpu.roll(value, 1, 1))

    def from_high(value, edge):
        return jnp.where(at_high, edge, pltpu.roll(value, nz - 1, 1))

    def span(start, stride):
        return pl.ds(start, by) if stride == 1 else pl.ds(start, bx, stride=stride)

    def as_float(value):
        return value.astype(jnp.float32)

    def put_crack(where, crack):
        crack = as_float(crack)
        df0[0, where, :] = crack
        kk0[where, :] = (1.0 - crack) * (1.0 - crack) + stiff_floor

    def outward(low, n, layer, size):
        return size + layer if low else layer - n

    w_copy.wait_recv()
    for dx, dy in order_b:
        @pl.when(there(-dx, -dy))
        def _(dx=dx, dy=dy):
            for copy in m_copies(dx, dy):
                copy.wait_recv()
            if dy == 0:
                i, low = (0, True) if dx < 0 else (1, False)
                for layer in range(3):
                    here = pl.ds(row_of(outward(low, 3, layer, bx), 0), by)
                    lf[0, here, :] = as_float(hx[i, pl.ds(layer * by, by), :])
                for layer in range(2):
                    here = pl.ds(row_of(outward(low, 2, layer, bx), 0), by)
                    put_crack(here, hx[i, pl.ds((3 + layer) * by, by), :])
                near = 0 if low else 2
                here = pl.ds(row_of(bx if low else -1, 0), by)
                lf[1, here, :] = as_float(jnp.maximum(
                    hx[i, pl.ds(near * by, by), :], hx[i, pl.ds(5 * by, by), :]
                ))
            elif dx == 0:
                i, low = (0, True) if dy < 0 else (1, False)
                for layer in range(3):
                    y = outward(low, 3, layer, by)
                    lf[0, pl.ds(row_of(0, y), bx, stride=PITCH), :] = as_float(hm[i, layer])
                for layer in range(2):
                    y = outward(low, 2, layer, by)
                    put_crack(pl.ds(row_of(0, y), bx, stride=PITCH), hm[i, 3 + layer])
                near = 0 if low else 2
                y = by if low else -1
                lf[1, pl.ds(row_of(0, y), bx, stride=PITCH), :] = as_float(
                    jnp.maximum(hm[i, near], hm[i, 5])
                )
            else:
                i = corners.index((dx, dy))
                x, far_x = (bx, bx + 1) if dx < 0 else (-1, -2)
                y, far_y = (by, by + 1) if dy < 0 else (-1, -2)
                for j, (at_x, at_y) in enumerate(((x, y), (far_x, y), (x, far_y))):
                    lf[0, pl.ds(row_of(at_x, at_y), 1), :] = as_float(hcm[i, pl.ds(j, 1), :])
                put_crack(pl.ds(row_of(x, y), 1), hcm[i, pl.ds(3, 1), :])

    vector = [wv[swapped, c] for c in range(3)]

    def fill(x, carry):
        for here in (x * PITCH, x * PITCH + 8, x * PITCH + 16):
            load = lf[0, pl.ds(here, 8), :]
            for c in range(3):
                u0[c, pl.ds(here, 8), :] = load * vector[c]
        return carry

    lax.fori_loop(0, bx + 2 * BORDER, fill, 0, unroll=2)
    tail = pl.ds((bx + 2 * BORDER) * PITCH, 8)
    for c in range(3):
        u0[c, tail, :] = lf[0, tail, :] * vector[c]
    vector = [jnp.concatenate([v, v], axis=0) for v in vector]

    def first_flow(start, stride, count):
        def at(offset, c):
            if stride == 1:
                return u0[c, pl.ds(start + offset, count), :]
            return u0[c, pl.ds(start + offset, count, stride=stride), :]

        to = pl.ds(start, count) if stride == 1 else pl.ds(start, count, stride=stride)
        value = at(0, 2)
        high = jnp.where(at_high[:count], 0.0, pltpu.roll(value, nz - 1, 1))
        low = jnp.where(at_low[:count], 0.0, pltpu.roll(value, 1, 1))
        trace = at(PITCH, 0) - at(-PITCH, 0) + at(1, 1) - at(-1, 1) + (high - low)
        df0[1, to, :] = kk0[to, :] * (0.5 * trace)

    def first_flow_own(x, carry):
        first_flow(row_of(x, 0), 1, by)
        return carry

    lax.fori_loop(0, bx, first_flow_own, 0, unroll=4)
    for dx, dy in order_b:
        @pl.when(there(-dx, -dy))
        def _(dx=dx, dy=dy):
            xs = (bx, bx + 1) if dx < 0 else (-2, -1)
            ys = (by, by + 1) if dy < 0 else (-2, -1)
            if dy == 0:
                for x in xs:
                    first_flow(row_of(x, 0), 1, by)
            elif dx == 0:
                for y in ys:
                    first_flow(row_of(0, y), PITCH, bx)
            else:
                first_flow(row_of(bx if dx < 0 else -1, by if dy < 0 else -1), 1, 1)

    def move(p, start, stride):
        df, u, kk = dfs[p], us[p], kks[p]

        def at(ref, offset, *lead):
            return ref[(*lead, span(start + offset, stride), slice(None))]

        k = at(kk, 0)
        k_xm, k_xp = at(kk, -PITCH), at(kk, PITCH)
        k_ym, k_yp = at(kk, -1), at(kk, 1)
        k_zm, k_zp = from_low(k, outside_stiff), from_high(k, outside_stiff)
        pairs = (k_xm + k_xp, k_ym + k_yp, k_zm + k_zp)
        total = 6.0 * k + (pairs[0] + pairs[1] + pairs[2])
        w_xm, w_xp, w_ym, w_yp = k + k_xm, k + k_xp, k + k_ym, k + k_yp
        w_zm = jnp.where(at_low, 0.0, k + k_zm)
        w_zp = jnp.where(at_high, 0.0, k + k_zp)
        middle_flow = at(df, 0, 1)
        slopes = (
            at(df, PITCH, 1) - at(df, -PITCH, 1),
            at(df, 1, 1) - at(df, -1, 1),
            from_high(middle_flow, 0.0) - from_low(middle_flow, 0.0),
        )
        fixed = at(lf, 0, 1) > 0.5
        load = at(lf, 0, 0)
        squares = None
        for c in range(3):
            here = at(u, 0, c)
            total_c = (
                w_xm * at(u, -PITCH, c) + w_xp * at(u, PITCH, c)
                + w_ym * at(u, -1, c) + w_yp * at(u, 1, c)
                + w_zm * pltpu.roll(here, 1, 1) + w_zp * pltpu.roll(here, nz - 1, 1)
            )
            residual = total_c - total * here + 2.0 * slopes[c]
            relaxed = here + relax_weight * residual / (total + pairs[c])
            us[1 - p][c, span(start, stride), :] = jnp.where(fixed, load * vector[c], relaxed)
            square = residual * residual
            squares = square if squares is None else squares + square
        return jnp.where(fixed, 0.0, squares)

    def heal(p, r, start, stride, held):
        q = 1 - p
        df, u = dfs[p], us[q]

        def at(ref, offset, *lead):
            return ref[(*lead, span(start + offset, stride), slice(None))]

        grads = []
        for c in range(3):
            here = at(u, 0, c)
            grads.append((
                at(u, PITCH, c) - at(u, -PITCH, c),
                at(u, 1, c) - at(u, -1, c),
                from_high(here, 0.0) - from_low(here, 0.0),
            ))
        energy, trace = twice_energy(
            grads[0][0], grads[1][1], grads[2][2],
            0.5 * (grads[0][1] + grads[1][0]),
            0.5 * (grads[0][2] + grads[2][0]),
            0.5 * (grads[1][2] + grads[2][1]),
        )
        here = at(df, 0, 0)
        beside = (
            at(df, PITCH, 0) + at(df, -PITCH, 0) + at(df, 1, 0) + at(df, -1, 0)
            + from_high(here, 0.0) + from_low(here, 0.0)
        )
        rate = g[r, held, :]
        renewed = (energy + rate * beside) / (energy + 7.0 * rate)
        renewed = jnp.where(crack_v[held, :] > 0, 1.0, renewed)
        stiff = (1.0 - renewed) * (1.0 - renewed) + stiff_floor
        to = span(start, stride)
        dfs[q][0, to, :] = renewed
        dfs[q][1, to, :] = stiff * (0.5 * trace)
        kks[q][to, :] = stiff

    columns = lax.broadcasted_iota(jnp.int32, (1, nz), 1)
    y_of = lax.broadcasted_iota(jnp.int32, (by, nz), 0)
    at_rim = (y_of == 0) | (y_of == by - 1)

    def in_groups(low, high, body, total):
        steps = 2 if (high - low) % 2 == 0 else 1
        size = (high - low) // steps

        def step(i, total):
            for j in range(size):
                added = body(low + i * size + j)
                total = total if added is None else total + added
            return total

        return lax.fori_loop(0, steps, step, total)

    def sweep(r, p, table, first=False, last=False):
        q = 1 - p

        def move_slab(x):
            return move(p, row_of(x, 0), 1)

        def move_strip(y):
            return move(p, row_of(0, y), PITCH)

        def heal_slab(x):
            heal(p, r, row_of(x, 0), 1, pl.ds(x * by, by))

        def heal_strip(y):
            heal(p, r, row_of(0, y), PITCH, pl.ds(y, bx, stride=by))

        nothing = jnp.zeros((by, nz), jnp.float32)
        squares = in_groups(1, bx - 1, move_slab, nothing)
        tough_arrived(r)
        in_groups(2, bx - 2, heal_slab, 0)

        if not first:
            take_b(dfs[p], p, us[p], sides_x + sides_y)
        for x in (0, bx - 1):
            squares = squares + move_slab(x)
        squares = jnp.where(at_rim, 0.0, squares)
        for y in (0, by - 1):
            squares = squares + move_strip(y)
        if not first:
            sent_a(p)
        if not last:
            send_a(q)
        if not first:
            take_a(p)
            take_b(dfs[p], p, us[p], corners)
        for x in (-1, bx):
            move_slab(x)
        for y in (-1, by):
            move_strip(y)
        total = jnp.sum(jnp.sum(squares, axis=0, keepdims=True), axis=1, keepdims=True)
        column = lax.rem(me_v + r, ns)
        table = jnp.where(columns == column, jnp.broadcast_to(total, (1, nz)), table)
        if last:
            spread_sums(table)
            give_displacement(us[q])
        for x in (0, 1, bx - 2, bx - 1):
            heal_slab(x)
        for y in (0, 1, by - 2, by - 1):
            heal_strip(y)
        if not first:
            sent_b(dfs[p], p)
        if not last:
            send_b(dfs[q], q, us[q])
        else:
            give_damage(dfs[q])
        return table

    def give(stage, out_ref, i):
        return pltpu.make_async_remote_copy(
            src_ref=stage, dst_ref=out_ref.at[0], send_sem=o_send.at[i], recv_sem=o_recv.at[i],
            device_id={"section": partner}, device_id_type=MESH,
        )

    give_u = give(stage_u, disp_ref, 0)
    give_d = give(stage_d, dam_ref, 1)

    def give_displacement(u):
        @pl.when(swapped == 0)
        def _():
            for x in range(bx):
                for c in range(3):
                    disp_ref[0, c, x] = u[c, pl.ds(row_of(x, 0), by), :]

        @pl.when(swapped == 1)
        def _():
            for x in range(bx):
                for c in range(3):
                    stage_u[c, x] = u[c, pl.ds(row_of(x, 0), by), :]
            give_u.start()

    def give_damage(df):
        @pl.when(swapped == 0)
        def _():
            for x in range(bx):
                dam_ref[0, x] = df[0, pl.ds(row_of(x, 0), by), :]

        @pl.when(swapped == 1)
        def _():
            for x in range(bx):
                stage_d[x] = df[0, pl.ds(row_of(x, 0), by), :]
            give_d.start()

    me = me_x * ny + me_y

    def hops(offset):
        return sum(min(o, n - o) for o, n in zip(offset, (nx, ny)))

    offsets = sorted(
        ((tx, ty) for tx in range(nx) for ty in range(ny)), key=lambda o: (-hops(o), o)
    )

    def sums_copy(t):
        tx, ty = offsets[t]
        return pltpu.make_async_remote_copy(
            src_ref=row_v, dst_ref=rows_v.at[me], send_sem=s_send.at[t], recv_sem=s_recv.at[t],
            device_id={
                "section": me_v, "gx": lax.rem(me_x + tx, nx), "gy": lax.rem(me_y + ty, ny),
            },
            device_id_type=MESH,
        )

    def sums_arrived(t):
        tx, ty = offsets[t]
        source = lax.rem(me_x + nx - tx, nx) * ny + lax.rem(me_y + ny - ty, ny)
        pltpu.make_async_copy(row_v, rows_v.at[source], s_recv.at[t]).wait()

    here_t = nx * ny - 1

    def spread_sums(table):
        row_v[...] = table
        for t in range(here_t):
            sums_copy(t).start()

        @pl.when(swapped == 0)
        def _():
            rows_v[me] = table

        @pl.when(swapped == 1)
        def _():
            sums_copy(here_t).start()

    def two_sweeps(i, table):
        return sweep(2 * i + 2, 0, sweep(2 * i + 1, 1, table))

    table = sweep(0, 0, jnp.zeros((1, nz), jnp.float32), first=True)
    table = lax.fori_loop(0, (ns - 2) // 2, two_sweeps, table)
    sweep(ns - 1, 1, table, last=True)

    w_copy.wait_send()
    for dx, dy in order_b:
        @pl.when(there(dx, dy))
        def _(dx=dx, dy=dy):
            for copy in m_copies(dx, dy):
                copy.wait_send()

    for r in range(ns):
        @pl.when(tough_target(r) != me_s)
        def _(r=r):
            tough_copy(r).wait_send()

    @pl.when(swapped == 1)
    def _():
        sums_copy(here_t).wait_send()
        sums_arrived(here_t)
        for copy in (give_u, give_d):
            copy.wait_send()
            copy.wait_recv()

    for t in range(here_t):
        sums_copy(t).wait_send()
        sums_arrived(t)
    everything = rows_v[0]
    for i in range(1, nx * ny):
        everything = everything + rows_v[i]
    result = jnp.sqrt(everything * (0.25 / (3.0 * cells)))
    table_ref[...] = result[:, :ns]


def write_out(*refs):
    sources, targets, sem = refs[:3], refs[3:6], refs[6]
    copies = [
        pltpu.make_async_copy(source, target, sem.at[i])
        for i, (source, target) in enumerate(zip(sources, targets))
    ]
    for copy in copies:
        copy.start()
    for copy in copies:
        copy.wait()


def on_device(sizes, load_index, load_table, toughness, clamp_mask, load_mask, crack_mask):
    ns, nx, ny = sizes
    bx, by, nz = clamp_mask.shape
    cells = float(clamp_mask.size * nx * ny)
    rows = (bx + 2 * BORDER) * PITCH + LEAD
    flat = (bx * by, nz)
    f32 = jnp.float32
    scratch = [
        pltpu.VMEM((3, rows, nz), f32),
        pltpu.VMEM((3, rows, nz), f32),
        pltpu.VMEM((2, rows, nz), f32),
        pltpu.VMEM((2, rows, nz), f32),
        pltpu.VMEM((rows, nz), f32),
        pltpu.VMEM((rows, nz), f32),
        pltpu.VMEM((2, rows, nz), f32),
        pltpu.VMEM(flat, jnp.int32),
        pltpu.VMEM(flat, jnp.int32),
        pltpu.VMEM(flat, jnp.int32),
        pltpu.VMEM((ns, *flat), f32),
        pltpu.VMEM((2, 3, bx, nz), f32),
        pltpu.VMEM((2, 2, 3, bx, nz), f32),
        pltpu.VMEM((2, 2 * HALO, bx, nz), f32),
        pltpu.VMEM((2, 2, 2 * HALO, bx, nz), f32),
        pltpu.VMEM((4, 8, nz), f32),
        pltpu.VMEM((2, 4, 8, nz), f32),
        pltpu.VMEM((2, 6, bx, nz), jnp.int32),
        pltpu.VMEM((4, 8, nz), jnp.int32),
        pltpu.VMEM((2, 6 * by, nz), jnp.int32),
        pltpu.VMEM((2, 6, bx, nz), jnp.int32),
        pltpu.VMEM((4, 8, nz), jnp.int32),
        pltpu.VMEM((1, nz), f32),
        pltpu.VMEM((nx * ny, 1, nz), f32),
        pltpu.VMEM((2, 3, 8, nz), f32),
        pltpu.VMEM((3, bx, by, nz), f32),
        pltpu.VMEM((bx, by, nz), f32),
        pltpu.SemaphoreType.DMA((3,)),
        pltpu.SemaphoreType.DMA((12,)),
        pltpu.SemaphoreType.DMA((12,)),
        pltpu.SemaphoreType.DMA((2,)),
        pltpu.SemaphoreType.DMA((2,)),
        pltpu.SemaphoreType.DMA((2,)),
        pltpu.SemaphoreType.DMA((2, 4)),
        pltpu.SemaphoreType.DMA((2, 4)),
        pltpu.SemaphoreType.DMA((2, 10)),
        pltpu.SemaphoreType.DMA((2, 10)),
        pltpu.SemaphoreType.DMA((ns,)),
        pltpu.SemaphoreType.DMA((ns,)),
        pltpu.SemaphoreType.DMA((nx * ny,)),
        pltpu.SemaphoreType.DMA((nx * ny,)),
    ]
    smem = pl.BlockSpec(memory_space=pltpu.SMEM)
    vmem = pl.BlockSpec(memory_space=pltpu.VMEM)
    hbm = pl.BlockSpec(memory_space=pl.ANY)
    results = pl.pallas_call(
        functools.partial(kernel, sizes, bx, by, cells),
        out_shape=(
            pltpu.VMEM((1, 3, bx, by, nz), f32),
            pltpu.VMEM((1, bx, by, nz), f32),
            pltpu.VMEM((1, ns), f32),
        ),
        in_specs=[smem, smem, hbm, hbm, hbm, hbm],
        out_specs=(vmem, vmem, vmem),
        scratch_shapes=scratch,
        compiler_params=pltpu.CompilerParams(collective_id=0, has_side_effects=True),
        name="sweeps",
    )(
        load_index,
        load_table.T,
        toughness.reshape(flat),
        clamp_mask.reshape(flat),
        load_mask.reshape(flat),
        crack_mask.reshape(flat),
    )
    results = [pltpu.with_memory_space_constraint(value, pltpu.VMEM) for value in results]
    return pl.pallas_call(
        write_out,
        out_shape=tuple(pltpu.HBM(value.shape, f32) for value in results),
        in_specs=[vmem] * 3,
        out_specs=(hbm,) * 3,
        scratch_shapes=[pltpu.SemaphoreType.DMA((3,))],
        name="write_out",
    )(*results)


def solution(mesh):
    sizes = (mesh.shape["section"], mesh.shape["gx"], mesh.shape["gy"])
    in_specs = (
        P("section"),
        P(),
        P("section", "gx", "gy", None),
        P("gx", "gy", None),
        P("gx", "gy", None),
        P("gx", "gy", None),
    )
    out_specs = (
        P("section", None, "gx", "gy", None),
        P("section", "gx", "gy", None),
        P("section", None),
    )
    return jax.shard_map(
        functools.partial(on_device, sizes),
        mesh=mesh, in_specs=in_specs, out_specs=out_specs, check_vma=False,
    )
```

```python
import functools

import jax
import jax.numpy as jnp
from jax import lax
from jax.experimental import pallas as pl
from jax.experimental.pallas import tpu as pltpu
from jax.sharding import PartitionSpec as P

MESH = pl.DeviceIdType.MESH
relax_weight = 0.6
stiff_floor = 0.001
eigen_guard = 1e-08
outside_stiff = 1.001

cos_third = (
    0.8660254053677892, 0.166666399623719, -0.0481050217302989, 0.024608831949810825,
    -0.015124763172089219, 0.009420074574188678, -0.004972568153766589,
    0.0017909605462136829, -0.0003093201852607309,
)
sin_third = (
    0.49999999939158213, -0.038675031951822925, 0.015381770818675887, -0.00862700282428075,
    0.005525819902144846, -0.0035154216998851246, 0.0018763805597984632,
    -0.0006797757027300123, 0.00011778274999869613,
)

PITCH = 24
LEAD = 8
HALO = 2
BORDER = 3


def row_of(x, y):
    return (x + BORDER) * PITCH + LEAD + y


def polynomial(coefficients, t):
    value = coefficients[-1]
    for coefficient in coefficients[-2::-1]:
        value = value * t + coefficient
    return value


def twice_energy(a, b, c, d, e, f):
    trace = a + b + c
    middle = trace * (1.0 / 3.0)
    a, b, c = a - middle, b - middle, c - middle
    dd, ee, ff = d * d, e * e, f * f
    spread = (a * a + b * b + c * c) * (1.0 / 6.0) + (dd + ee + ff) * (1.0 / 3.0)
    guarded = spread + 4.0 * eigen_guard
    determinant = a * (b * c - ff) - d * (d * c - f * e) + e * (d * f - b * e)
    inverse = lax.rsqrt(guarded)
    ratio = determinant * (0.5 * inverse) * (inverse * inverse)
    size = jnp.minimum(jnp.abs(ratio), 1.0)
    radius = jnp.sqrt(spread)
    first = radius * polynomial(cos_third, size)
    first = jnp.where(ratio < 0.0, -first, first)
    rest = radius * (1.7320508075688772 * jnp.sqrt(1.0 - size)) * polynomial(sin_third, size)
    largest = jnp.maximum(middle + 2.0 * first, 0.0)
    base = middle - first
    second = jnp.maximum(base + rest, 0.0)
    third = jnp.maximum(base - rest, 0.0)
    volume = jnp.maximum(trace, 0.0)
    energy = 0.25 * (volume * volume) + 0.5 * (
        largest * largest + second * second + third * third
    )
    return energy, trace


def kernel(
    sizes, bx, by, cells,
    index_ref, loads_hbm, tough_ref, clamp_ref, load_ref, crack_ref,
    disp_ref, dam_ref, table_ref,
    u0, u1, df0, df1, kk0, kk1, lf, clamp_v, load_v, crack_v, g,
    pa, ra, pb, rb, pc, rc, pm, pcm, hx, hm, hcm, row_v, rows_v, wv, stage_u, stage_d, loads_ref,
    local_sem, m_send, m_recv, w_sem, o_send, o_recv, a_send, a_recv, b_send, b_recv, t_send, t_recv, s_send, s_recv,
):
    ns, nx, ny = sizes
    me_s = lax.axis_index("section")
    me_x = lax.axis_index("gx")
    me_y = lax.axis_index("gy")
    swapped = lax.rem(me_x, 2)

    def place(case, x):
        return case + lax.rem(x + 2, 2) * (1 - 2 * lax.rem(case, 2))

    me_v = place(me_s, me_x)

    def neighbour_id(dx, dy):
        return {"section": place(me_v, me_x + dx), "gx": me_x + dx, "gy": me_y + dy}

    nz = u0.shape[-1]
    us, dfs, kks = (u0, u1), (df0, df1), (kk0, kk1)

    copies = [
        pltpu.make_async_copy(source, target, local_sem.at[i])
        for i, (source, target) in enumerate(
            (
                (load_ref, load_v), (clamp_ref, clamp_v), (crack_ref, crack_v),
                (loads_hbm, loads_ref),
            )
        )
    ]
    for copy in copies:
        copy.start()

    halo_pieces = [(i * PITCH, 8) for i in range(bx + 2 * BORDER + 1)]
    halo_pieces += [(row_of(x, 0), by) for x in (-3, -2, -1, bx, bx + 1, bx + 2)]
    for start, size in halo_pieces:
        for ref in us + dfs:
            for i in range(ref.shape[0]):
                ref[i, pl.ds(start, size), :] = jnp.zeros((size, nz), jnp.float32)
        lf[0, pl.ds(start, size), :] = jnp.zeros((size, nz), jnp.float32)
        lf[1, pl.ds(start, size), :] = jnp.ones((size, nz), jnp.float32)
        for ref in kks:
            ref[pl.ds(start, size), :] = jnp.full((size, nz), outside_stiff, jnp.float32)

    def there(dx, dy):
        return (
            (me_x + dx >= 0) & (me_x + dx < nx) & (me_y + dy >= 0) & (me_y + dy < ny)
        )

    corners = ((-1, -1), (-1, 1), (1, -1), (1, 1))
    sides_x = ((-1, 0), (1, 0))
    sides_y = ((0, -1), (0, 1))
    neighbours = sides_x + sides_y + corners

    barrier = pltpu.get_barrier_semaphore()
    for dx, dy in neighbours:
        @pl.when(there(dx, dy))
        def _(dx=dx, dy=dy):
            pl.semaphore_signal(
                barrier, inc=1, device_id=neighbour_id(dx, dy), device_id_type=MESH
            )
    for r in range(1, ns):
        pl.semaphore_signal(
            barrier, inc=1, device_id={"section": lax.rem(me_s + r, ns)}, device_id_type=MESH
        )

    copies[3].wait()
    case = index_ref[0]
    for c in range(3):
        wv[0, c] = jnp.full((8, nz), loads_ref[c, case], jnp.float32)
    for i in (0, 1, 2):
        copies[i].wait()

    def begin(x, carry):
        here = pl.ds(row_of(x, 0), by)
        held = pl.ds(x * by, by)
        load = load_v[held, :].astype(jnp.float32)
        clamp = clamp_v[held, :].astype(jnp.float32)
        crack = crack_v[held, :].astype(jnp.float32)
        lf[0, here, :] = load
        lf[1, here, :] = jnp.maximum(load, clamp)
        df0[0, here, :] = crack
        kk0[here, :] = (1.0 - crack) * (1.0 - crack) + stiff_floor
        return carry

    lax.fori_loop(0, bx, begin, 0, unroll=4)

    for i in range(2):
        for ref, n, first in ((load_v, 3, 0), (crack_v, 2, 3), (clamp_v, 1, 5)):
            for layer in range(n):
                y = layer if i == 0 else by - n + layer
                pm[i, first + layer] = ref[pl.ds(y, bx, stride=by), :]
    for i, (dx, dy) in enumerate(corners):
        x, deep_x = (0, 1) if dx < 0 else (bx - 1, bx - 2)
        y, deep_y = (0, 1) if dy < 0 else (by - 1, by - 2)
        for j, (ref, at_x, at_y) in enumerate((
            (load_v, x, y), (load_v, deep_x, y), (load_v, x, deep_y), (crack_v, x, y),
        )):
            pcm[i, pl.ds(j, 1), :] = ref[pl.ds(at_x * by + at_y, 1), :]

    across = 1 + (me_x > 0).astype(jnp.int32) + (me_x < nx - 1).astype(jnp.int32)
    along = 1 + (me_y > 0).astype(jnp.int32) + (me_y < ny - 1).astype(jnp.int32)
    pl.semaphore_wait(barrier, across * along - 1 + (ns - 1))

    def remote(source, target, send, recv, dx, dy):
        return pltpu.make_async_remote_copy(
            src_ref=source, dst_ref=target, send_sem=send, recv_sem=recv,
            device_id=neighbour_id(dx, dy), device_id_type=MESH,
        )

    def b_copies(field, q, dx, dy):
        found = []
        if dy == 0:
            for layer in range(HALO):
                x = layer if dx < 0 else bx - HALO + layer
                to = bx + layer if dx < 0 else layer - HALO
                i = (0 if dx < 0 else 2) + layer
                found.append(remote(
                    field.at[:, pl.ds(row_of(x, 0), by), :],
                    field.at[:, pl.ds(row_of(to, 0), by), :],
                    b_send.at[q, i], b_recv.at[q, i], dx, dy,
                ))
        elif dx == 0:
            i = 0 if dy < 0 else 1
            found.append(remote(
                pb.at[i], rb.at[q, i], b_send.at[q, 4 + i], b_recv.at[q, 4 + i], dx, dy,
            ))
        else:
            i = corners.index((dx, dy))
            found.append(remote(
                pc.at[i], rc.at[q, i], b_send.at[q, 6 + i], b_recv.at[q, 6 + i], dx, dy,
            ))
        return found

    order_b = corners + sides_x + sides_y

    def send_b(field, q, current):
        for i, (dx, dy) in enumerate(corners):
            row = row_of(0 if dx < 0 else bx - 1, 0 if dy < 0 else by - 1)
            if current is not None:
                for c in range(3):
                    pc[i, pl.ds(c, 1), :] = current[c, pl.ds(row, 1), :]
            for f in range(2):
                pc[i, pl.ds(3 + f, 1), :] = field[f, pl.ds(row, 1), :]
        for i in range(2):
            for f in range(2):
                for layer in range(HALO):
                    y = layer if i == 0 else by - HALO + layer
                    pb[i, f * HALO + layer] = field[
                        f, pl.ds(row_of(0, y), bx, stride=PITCH), :
                    ]
        for dx, dy in order_b:
            @pl.when(there(dx, dy))
            def _(dx=dx, dy=dy):
                for copy in b_copies(field, q, dx, dy):
                    copy.start()

    def sent_b(field, q):
        for dx, dy in order_b:
            @pl.when(there(dx, dy))
            def _(dx=dx, dy=dy):
                for copy in b_copies(field, q, dx, dy):
                    copy.wait_send()

    def take_b(field, q, current, directions):
        for dx, dy in directions:
            @pl.when(there(-dx, -dy))
            def _(dx=dx, dy=dy):
                for copy in b_copies(field, q, dx, dy):
                    copy.wait_recv()
                if dx == 0:
                    i = 0 if dy < 0 else 1
                    for f in range(2):
                        for layer in range(HALO):
                            y = by + layer if i == 0 else layer - HALO
                            strip = pl.ds(row_of(0, y), bx, stride=PITCH)
                            value = rb[q, i, f * HALO + layer]
                            field[f, strip, :] = value
                            if current is not None and f == 0:
                                kks[q][strip, :] = (1.0 - value) * (1.0 - value) + stiff_floor
                elif dy != 0:
                    i = corners.index((dx, dy))
                    row = row_of(bx if dx < 0 else -1, by if dy < 0 else -1)
                    if current is not None:
                        for c in range(3):
                            current[c, pl.ds(row, 1), :] = rc[q, i, pl.ds(c, 1), :]
                        value = rc[q, i, pl.ds(3, 1), :]
                        kks[q][pl.ds(row, 1), :] = (1.0 - value) * (1.0 - value) + stiff_floor
                    for f in range(2):
                        field[f, pl.ds(row, 1), :] = rc[q, i, pl.ds(3 + f, 1), :]
        if directions is not corners:
            for x in (-2, -1, bx, bx + 1):
                here = pl.ds(row_of(x, 0), by)
                value = field[0, here, :]
                kks[q][here, :] = (1.0 - value) * (1.0 - value) + stiff_floor

    def a_copy(q, dx, dy):
        if dy == 0:
            i = 0 if dx < 0 else 1
            x, to = (1, bx + 1) if dx < 0 else (bx - 2, -2)
            return remote(
                us[q].at[:, pl.ds(row_of(x, 0), by), :],
                us[q].at[:, pl.ds(row_of(to, 0), by), :],
                a_send.at[q, i], a_recv.at[q, i], dx, dy,
            )
        i = 0 if dy < 0 else 1
        return remote(
            pa.at[i], ra.at[q, i], a_send.at[q, 2 + i], a_recv.at[q, 2 + i], dx, dy,
        )

    def send_a(q):
        for i in range(2):
            y = 1 if i == 0 else by - 2
            for c in range(3):
                pa[i, c] = us[q][c, pl.ds(row_of(0, y), bx, stride=PITCH), :]
        for dx, dy in sides_x + sides_y:
            @pl.when(there(dx, dy))
            def _(dx=dx, dy=dy):
                a_copy(q, dx, dy).start()

    def sent_a(q):
        for dx, dy in sides_x + sides_y:
            @pl.when(there(dx, dy))
            def _(dx=dx, dy=dy):
                a_copy(q, dx, dy).wait_send()

    def take_a(q):
        for dx, dy in sides_x + sides_y:
            @pl.when(there(-dx, -dy))
            def _(dx=dx, dy=dy):
                a_copy(q, dx, dy).wait_recv()
                if dx == 0:
                    i = 0 if dy < 0 else 1
                    y = by + 1 if i == 0 else -2
                    for c in range(3):
                        us[q][c, pl.ds(row_of(0, y), bx, stride=PITCH), :] = ra[q, i, c]

    def tough_target(r):
        return place(lax.rem(me_s + ns - r, ns), me_x)

    def tough_copy(r):
        return pltpu.make_async_remote_copy(
            src_ref=tough_ref, dst_ref=g.at[r], send_sem=t_send.at[r], recv_sem=t_recv.at[r],
            device_id={"section": tough_target(r)}, device_id_type=MESH,
        )

    def tough_arrived(r):
        pltpu.make_async_copy(tough_ref, g.at[r], t_recv.at[r]).wait()

    masks = (load_v, crack_v, clamp_v)
    layers = (3, 2, 1)
    parts = tuple((ref, n, sum(layers[:i])) for i, (ref, n) in enumerate(zip(masks, layers)))

    def m_copies(dx, dy):
        if dy == 0:
            i = 0 if dx < 0 else 1
            return [
                remote(
                    ref.at[pl.ds((0 if dx < 0 else bx - n) * by, n * by), :],
                    hx.at[i, pl.ds(first * by, n * by), :],
                    m_send.at[3 * i + j], m_recv.at[3 * i + j], dx, dy,
                )
                for j, (ref, n, first) in enumerate(parts)
            ]
        if dx == 0:
            i = 0 if dy < 0 else 1
            return [remote(pm.at[i], hm.at[i], m_send.at[6 + i], m_recv.at[6 + i], dx, dy)]
        i = corners.index((dx, dy))
        return [remote(pcm.at[i], hcm.at[i], m_send.at[8 + i], m_recv.at[8 + i], dx, dy)]

    for dx, dy in order_b:
        @pl.when(there(dx, dy))
        def _(dx=dx, dy=dy):
            for copy in m_copies(dx, dy):
                copy.start()
    partner = me_s + 1 - 2 * lax.rem(me_s, 2)
    w_copy = pltpu.make_async_remote_copy(
        src_ref=wv.at[0], dst_ref=wv.at[1], send_sem=w_sem.at[0], recv_sem=w_sem.at[1],
        device_id={"section": partner}, device_id_type=MESH,
    )
    w_copy.start()
    for r in range(ns):
        @pl.when(tough_target(r) == me_s)
        def _(r=r):
            pltpu.make_async_copy(tough_ref, g.at[r], t_recv.at[r]).start()

        @pl.when(tough_target(r) != me_s)
        def _(r=r):
            tough_copy(r).start()

    lane = lax.broadcasted_iota(jnp.int32, (by, nz), 1)
    at_low = lane == 0
    at_high = lane == nz - 1

    def from_low(value, edge):
        return jnp.where(at_low, edge, pltpu.roll(value, 1, 1))

    def from_high(value, edge):
        return jnp.where(at_high, edge, pltpu.roll(value, nz - 1, 1))

    def span(start, stride):
        return pl.ds(start, by) if stride == 1 else pl.ds(start, bx, stride=stride)

    def as_float(value):
        return value.astype(jnp.float32)

    def put_crack(where, crack):
        crack = as_float(crack)
        df0[0, where, :] = crack
        kk0[where, :] = (1.0 - crack) * (1.0 - crack) + stiff_floor

    def outward(low, n, layer, size):
        return size + layer if low else layer - n

    w_copy.wait_recv()
    for dx, dy in order_b:
        @pl.when(there(-dx, -dy))
        def _(dx=dx, dy=dy):
            for copy in m_copies(dx, dy):
                copy.wait_recv()
            if dy == 0:
                i, low = (0, True) if dx < 0 else (1, False)
                for layer in range(3):
                    here = pl.ds(row_of(outward(low, 3, layer, bx), 0), by)
                    lf[0, here, :] = as_float(hx[i, pl.ds(layer * by, by), :])
                for layer in range(2):
                    here = pl.ds(row_of(outward(low, 2, layer, bx), 0), by)
                    put_crack(here, hx[i, pl.ds((3 + layer) * by, by), :])
                near = 0 if low else 2
                here = pl.ds(row_of(bx if low else -1, 0), by)
                lf[1, here, :] = as_float(jnp.maximum(
                    hx[i, pl.ds(near * by, by), :], hx[i, pl.ds(5 * by, by), :]
                ))
            elif dx == 0:
                i, low = (0, True) if dy < 0 else (1, False)
                for layer in range(3):
                    y = outward(low, 3, layer, by)
                    lf[0, pl.ds(row_of(0, y), bx, stride=PITCH), :] = as_float(hm[i, layer])
                for layer in range(2):
                    y = outward(low, 2, layer, by)
                    put_crack(pl.ds(row_of(0, y), bx, stride=PITCH), hm[i, 3 + layer])
                near = 0 if low else 2
                y = by if low else -1
                lf[1, pl.ds(row_of(0, y), bx, stride=PITCH), :] = as_float(
                    jnp.maximum(hm[i, near], hm[i, 5])
                )
            else:
                i = corners.index((dx, dy))
                x, far_x = (bx, bx + 1) if dx < 0 else (-1, -2)
                y, far_y = (by, by + 1) if dy < 0 else (-1, -2)
                for j, (at_x, at_y) in enumerate(((x, y), (far_x, y), (x, far_y))):
                    lf[0, pl.ds(row_of(at_x, at_y), 1), :] = as_float(hcm[i, pl.ds(j, 1), :])
                put_crack(pl.ds(row_of(x, y), 1), hcm[i, pl.ds(3, 1), :])

    vector = [wv[swapped, c] for c in range(3)]

    def fill(x, carry):
        for here in (x * PITCH, x * PITCH + 8, x * PITCH + 16):
            load = lf[0, pl.ds(here, 8), :]
            for c in range(3):
                u0[c, pl.ds(here, 8), :] = load * vector[c]
        return carry

    lax.fori_loop(0, bx + 2 * BORDER, fill, 0, unroll=2)
    tail = pl.ds((bx + 2 * BORDER) * PITCH, 8)
    for c in range(3):
        u0[c, tail, :] = lf[0, tail, :] * vector[c]
    vector = [jnp.concatenate([v, v], axis=0) for v in vector]

    def first_flow(start, stride, count):
        def at(offset, c):
            if stride == 1:
                return u0[c, pl.ds(start + offset, count), :]
            return u0[c, pl.ds(start + offset, count, stride=stride), :]

        to = pl.ds(start, count) if stride == 1 else pl.ds(start, count, stride=stride)
        value = at(0, 2)
        high = jnp.where(at_high[:count], 0.0, pltpu.roll(value, nz - 1, 1))
        low = jnp.where(at_low[:count], 0.0, pltpu.roll(value, 1, 1))
        trace = at(PITCH, 0) - at(-PITCH, 0) + at(1, 1) - at(-1, 1) + (high - low)
        df0[1, to, :] = kk0[to, :] * (0.5 * trace)

    def first_flow_own(x, carry):
        first_flow(row_of(x, 0), 1, by)
        return carry

    lax.fori_loop(0, bx, first_flow_own, 0, unroll=4)
    for dx, dy in order_b:
        @pl.when(there(-dx, -dy))
        def _(dx=dx, dy=dy):
            xs = (bx, bx + 1) if dx < 0 else (-2, -1)
            ys = (by, by + 1) if dy < 0 else (-2, -1)
            if dy == 0:
                for x in xs:
                    first_flow(row_of(x, 0), 1, by)
            elif dx == 0:
                for y in ys:
                    first_flow(row_of(0, y), PITCH, bx)
            else:
                first_flow(row_of(bx if dx < 0 else -1, by if dy < 0 else -1), 1, 1)

    def move(p, start, stride):
        df, u, kk = dfs[p], us[p], kks[p]

        def at(ref, offset, *lead):
            return ref[(*lead, span(start + offset, stride), slice(None))]

        k = at(kk, 0)
        k_xm, k_xp = at(kk, -PITCH), at(kk, PITCH)
        k_ym, k_yp = at(kk, -1), at(kk, 1)
        k_zm, k_zp = from_low(k, outside_stiff), from_high(k, outside_stiff)
        pairs = (k_xm + k_xp, k_ym + k_yp, k_zm + k_zp)
        total = 6.0 * k + (pairs[0] + pairs[1] + pairs[2])
        w_xm, w_xp, w_ym, w_yp = k + k_xm, k + k_xp, k + k_ym, k + k_yp
        w_zm = jnp.where(at_low, 0.0, k + k_zm)
        w_zp = jnp.where(at_high, 0.0, k + k_zp)
        middle_flow = at(df, 0, 1)
        slopes = (
            at(df, PITCH, 1) - at(df, -PITCH, 1),
            at(df, 1, 1) - at(df, -1, 1),
            from_high(middle_flow, 0.0) - from_low(middle_flow, 0.0),
        )
        fixed = at(lf, 0, 1) > 0.5
        load = at(lf, 0, 0)
        squares = None
        for c in range(3):
            here = at(u, 0, c)
            total_c = (
                w_xm * at(u, -PITCH, c) + w_xp * at(u, PITCH, c)
                + w_ym * at(u, -1, c) + w_yp * at(u, 1, c)
                + w_zm * pltpu.roll(here, 1, 1) + w_zp * pltpu.roll(here, nz - 1, 1)
            )
            residual = total_c - total * here + 2.0 * slopes[c]
            relaxed = here + relax_weight * residual / (total + pairs[c])
            us[1 - p][c, span(start, stride), :] = jnp.where(fixed, load * vector[c], relaxed)
            square = residual * residual
            squares = square if squares is None else squares + square
        return jnp.where(fixed, 0.0, squares)

    def heal(p, r, start, stride, held):
        q = 1 - p
        df, u = dfs[p], us[q]

        def at(ref, offset, *lead):
            return ref[(*lead, span(start + offset, stride), slice(None))]

        grads = []
        for c in range(3):
            here = at(u, 0, c)
            grads.append((
                at(u, PITCH, c) - at(u, -PITCH, c),
                at(u, 1, c) - at(u, -1, c),
                from_high(here, 0.0) - from_low(here, 0.0),
            ))
        energy, trace = twice_energy(
            grads[0][0], grads[1][1], grads[2][2],
            0.5 * (grads[0][1] + grads[1][0]),
            0.5 * (grads[0][2] + grads[2][0]),
            0.5 * (grads[1][2] + grads[2][1]),
        )
        here = at(df, 0, 0)
        beside = (
            at(df, PITCH, 0) + at(df, -PITCH, 0) + at(df, 1, 0) + at(df, -1, 0)
            + from_high(here, 0.0) + from_low(here, 0.0)
        )
        rate = g[r, held, :]
        renewed = (energy + rate * beside) / (energy + 7.0 * rate)
        renewed = jnp.where(crack_v[held, :] > 0, 1.0, renewed)
        stiff = (1.0 - renewed) * (1.0 - renewed) + stiff_floor
        to = span(start, stride)
        dfs[q][0, to, :] = renewed
        dfs[q][1, to, :] = stiff * (0.5 * trace)
        kks[q][to, :] = stiff

    columns = lax.broadcasted_iota(jnp.int32, (1, nz), 1)
    y_of = lax.broadcasted_iota(jnp.int32, (by, nz), 0)
    at_rim = (y_of == 0) | (y_of == by - 1)

    def in_groups(low, high, body, total):
        steps = 2 if (high - low) % 2 == 0 else 1
        size = (high - low) // steps

        def step(i, total):
            for j in range(size):
                added = body(low + i * size + j)
                total = total if added is None else total + added
            return total

        return lax.fori_loop(0, steps, step, total)

    def sweep(r, p, table, first=False, last=False):
        q = 1 - p

        def move_slab(x):
            return move(p, row_of(x, 0), 1)

        def move_strip(y):
            return move(p, row_of(0, y), PITCH)

        def heal_slab(x):
            heal(p, r, row_of(x, 0), 1, pl.ds(x * by, by))

        def heal_strip(y):
            heal(p, r, row_of(0, y), PITCH, pl.ds(y, bx, stride=by))

        nothing = jnp.zeros((by, nz), jnp.float32)
        squares = in_groups(1, bx - 1, move_slab, nothing)
        tough_arrived(r)
        in_groups(2, bx - 2, heal_slab, 0)

        if not first:
            take_b(dfs[p], p, us[p], sides_x + sides_y)
        for x in (0, bx - 1):
            squares = squares + move_slab(x)
        squares = jnp.where(at_rim, 0.0, squares)
        for y in (0, by - 1):
            squares = squares + move_strip(y)

        def with_sums(table):
            total = jnp.sum(jnp.sum(squares, axis=0, keepdims=True), axis=1, keepdims=True)
            column = lax.rem(me_v + r, ns)
            return jnp.where(columns == column, jnp.broadcast_to(total, (1, nz)), table)

        if last:
            spread_sums(with_sums(table))
        if not first:
            sent_a(p)
        if not last:
            send_a(q)
        if not first:
            take_a(p)
            take_b(dfs[p], p, us[p], corners)
        for x in (-1, bx):
            move_slab(x)
        for y in (-1, by):
            move_strip(y)
        if last:
            give_displacement(us[q])
        for x in (0, 1, bx - 2, bx - 1):
            heal_slab(x)
        for y in (0, 1, by - 2, by - 1):
            heal_strip(y)
        if not first:
            sent_b(dfs[p], p)
        if not last:
            send_b(dfs[q], q, us[q])
            table = with_sums(table)
        else:
            give_damage(dfs[q])
        return table

    def give(stage, out_ref, i):
        return pltpu.make_async_remote_copy(
            src_ref=stage, dst_ref=out_ref.at[0], send_sem=o_send.at[i], recv_sem=o_recv.at[i],
            device_id={"section": partner}, device_id_type=MESH,
        )

    give_u = give(stage_u, disp_ref, 0)
    give_d = give(stage_d, dam_ref, 1)

    def give_displacement(u):
        @pl.when(swapped == 0)
        def _():
            for x in range(bx):
                for c in range(3):
                    disp_ref[0, c, x] = u[c, pl.ds(row_of(x, 0), by), :]

        @pl.when(swapped == 1)
        def _():
            for x in range(bx):
                for c in range(3):
                    stage_u[c, x] = u[c, pl.ds(row_of(x, 0), by), :]
            give_u.start()

    def give_damage(df):
        @pl.when(swapped == 0)
        def _():
            for x in range(bx):
                dam_ref[0, x] = df[0, pl.ds(row_of(x, 0), by), :]

        @pl.when(swapped == 1)
        def _():
            for x in range(bx):
                stage_d[x] = df[0, pl.ds(row_of(x, 0), by), :]
            give_d.start()

    me = me_x * ny + me_y

    def hops(offset):
        return sum(min(o, n - o) for o, n in zip(offset, (nx, ny)))

    offsets = sorted(
        ((tx, ty) for tx in range(nx) for ty in range(ny)), key=lambda o: (-hops(o), o)
    )

    def sums_copy(t):
        tx, ty = offsets[t]
        return pltpu.make_async_remote_copy(
            src_ref=row_v, dst_ref=rows_v.at[me], send_sem=s_send.at[t], recv_sem=s_recv.at[t],
            device_id={
                "section": me_v, "gx": lax.rem(me_x + tx, nx), "gy": lax.rem(me_y + ty, ny),
            },
            device_id_type=MESH,
        )

    def sums_arrived(t):
        tx, ty = offsets[t]
        source = lax.rem(me_x + nx - tx, nx) * ny + lax.rem(me_y + ny - ty, ny)
        pltpu.make_async_copy(row_v, rows_v.at[source], s_recv.at[t]).wait()

    here_t = nx * ny - 1

    def spread_sums(table):
        row_v[...] = table
        for t in range(here_t):
            sums_copy(t).start()

        @pl.when(swapped == 0)
        def _():
            rows_v[me] = table

        @pl.when(swapped == 1)
        def _():
            sums_copy(here_t).start()

    def two_sweeps(i, table):
        return sweep(2 * i + 2, 0, sweep(2 * i + 1, 1, table))

    table = sweep(0, 0, jnp.zeros((1, nz), jnp.float32), first=True)
    table = lax.fori_loop(0, (ns - 2) // 2, two_sweeps, table)
    sweep(ns - 1, 1, table, last=True)

    w_copy.wait_send()
    for dx, dy in order_b:
        @pl.when(there(dx, dy))
        def _(dx=dx, dy=dy):
            for copy in m_copies(dx, dy):
                copy.wait_send()

    for r in range(ns):
        @pl.when(tough_target(r) != me_s)
        def _(r=r):
            tough_copy(r).wait_send()

    @pl.when(swapped == 1)
    def _():
        sums_copy(here_t).wait_send()
        sums_arrived(here_t)
        for copy in (give_u, give_d):
            copy.wait_send()
            copy.wait_recv()

    for t in range(here_t):
        sums_copy(t).wait_send()
        sums_arrived(t)
    everything = rows_v[0]
    for i in range(1, nx * ny):
        everything = everything + rows_v[i]
    result = jnp.sqrt(everything * (0.25 / (3.0 * cells)))
    table_ref[...] = result[:, :ns]


def write_out(*refs):
    sources, targets, sem = refs[:3], refs[3:6], refs[6]
    copies = [
        pltpu.make_async_copy(source, target, sem.at[i])
        for i, (source, target) in enumerate(zip(sources, targets))
    ]
    for copy in copies:
        copy.start()
    for copy in copies:
        copy.wait()


def on_device(sizes, load_index, load_table, toughness, clamp_mask, load_mask, crack_mask):
    ns, nx, ny = sizes
    bx, by, nz = clamp_mask.shape
    cells = float(clamp_mask.size * nx * ny)
    rows = (bx + 2 * BORDER) * PITCH + LEAD
    flat = (bx * by, nz)
    f32 = jnp.float32
    scratch = [
        pltpu.VMEM((3, rows, nz), f32),
        pltpu.VMEM((3, rows, nz), f32),
        pltpu.VMEM((2, rows, nz), f32),
        pltpu.VMEM((2, rows, nz), f32),
        pltpu.VMEM((rows, nz), f32),
        pltpu.VMEM((rows, nz), f32),
        pltpu.VMEM((2, rows, nz), f32),
        pltpu.VMEM(flat, jnp.int32),
        pltpu.VMEM(flat, jnp.int32),
        pltpu.VMEM(flat, jnp.int32),
        pltpu.VMEM((ns, *flat), f32),
        pltpu.VMEM((2, 3, bx, nz), f32),
        pltpu.VMEM((2, 2, 3, bx, nz), f32),
        pltpu.VMEM((2, 2 * HALO, bx, nz), f32),
        pltpu.VMEM((2, 2, 2 * HALO, bx, nz), f32),
        pltpu.VMEM((4, 8, nz), f32),
        pltpu.VMEM((2, 4, 8, nz), f32),
        pltpu.VMEM((2, 6, bx, nz), jnp.int32),
        pltpu.VMEM((4, 8, nz), jnp.int32),
        pltpu.VMEM((2, 6 * by, nz), jnp.int32),
        pltpu.VMEM((2, 6, bx, nz), jnp.int32),
        pltpu.VMEM((4, 8, nz), jnp.int32),
        pltpu.VMEM((1, nz), f32),
        pltpu.VMEM((nx * ny, 1, nz), f32),
        pltpu.VMEM((2, 3, 8, nz), f32),
        pltpu.VMEM((3, bx, by, nz), f32),
        pltpu.VMEM((bx, by, nz), f32),
        pltpu.SMEM(load_table.shape[::-1], f32),
        pltpu.SemaphoreType.DMA((4,)),
        pltpu.SemaphoreType.DMA((12,)),
        pltpu.SemaphoreType.DMA((12,)),
        pltpu.SemaphoreType.DMA((2,)),
        pltpu.SemaphoreType.DMA((2,)),
        pltpu.SemaphoreType.DMA((2,)),
        pltpu.SemaphoreType.DMA((2, 4)),
        pltpu.SemaphoreType.DMA((2, 4)),
        pltpu.SemaphoreType.DMA((2, 10)),
        pltpu.SemaphoreType.DMA((2, 10)),
        pltpu.SemaphoreType.DMA((ns,)),
        pltpu.SemaphoreType.DMA((ns,)),
        pltpu.SemaphoreType.DMA((nx * ny,)),
        pltpu.SemaphoreType.DMA((nx * ny,)),
    ]
    vmem = pl.BlockSpec(memory_space=pltpu.VMEM)
    hbm = pl.BlockSpec(memory_space=pl.ANY)
    results = pl.pallas_call(
        functools.partial(kernel, sizes, bx, by, cells),
        out_shape=(
            pltpu.VMEM((1, 3, bx, by, nz), f32),
            pltpu.VMEM((1, bx, by, nz), f32),
            pltpu.VMEM((1, ns), f32),
        ),
        in_specs=[pl.BlockSpec(memory_space=pltpu.SMEM)] + [hbm] * 5,
        out_specs=(vmem, vmem, vmem),
        scratch_shapes=scratch,
        compiler_params=pltpu.CompilerParams(collective_id=0, has_side_effects=True),
        name="sweeps",
    )(
        load_index,
        load_table.T,
        toughness.reshape(flat),
        clamp_mask.reshape(flat),
        load_mask.reshape(flat),
        crack_mask.reshape(flat),
    )
    results = [pltpu.with_memory_space_constraint(value, pltpu.VMEM) for value in results]
    return pl.pallas_call(
        write_out,
        out_shape=tuple(pltpu.HBM(value.shape, f32) for value in results),
        in_specs=[vmem] * 3,
        out_specs=(hbm,) * 3,
        scratch_shapes=[pltpu.SemaphoreType.DMA((3,))],
        name="write_out",
    )(*results)


def solution(mesh):
    sizes = (mesh.shape["section"], mesh.shape["gx"], mesh.shape["gy"])
    in_specs = (
        P("section"),
        P(),
        P("section", "gx", "gy", None),
        P("gx", "gy", None),
        P("gx", "gy", None),
        P("gx", "gy", None),
    )
    out_specs = (
        P("section", None, "gx", "gy", None),
        P("section", "gx", "gy", None),
        P("section", None),
    )
    return jax.shard_map(
        functools.partial(on_device, sizes),
        mesh=mesh, in_specs=in_specs, out_specs=out_specs, check_vma=False,
    )
```

```python
import functools

import jax
import jax.numpy as jnp
from jax import lax
from jax.experimental import pallas as pl
from jax.experimental.pallas import tpu as pltpu
from jax.sharding import PartitionSpec as P

MESH = pl.DeviceIdType.MESH
relax_weight = 0.6
stiff_floor = 0.001
eigen_guard = 1e-08
outside_stiff = 1.001

cos_third = (
    0.8660254053677892, 0.166666399623719, -0.0481050217302989, 0.024608831949810825,
    -0.015124763172089219, 0.009420074574188678, -0.004972568153766589,
    0.0017909605462136829, -0.0003093201852607309,
)
sin_third = (
    0.49999999939158213, -0.038675031951822925, 0.015381770818675887, -0.00862700282428075,
    0.005525819902144846, -0.0035154216998851246, 0.0018763805597984632,
    -0.0006797757027300123, 0.00011778274999869613,
)

PITCH = 24
LEAD = 8
HALO = 2
BORDER = 3


def row_of(x, y):
    return (x + BORDER) * PITCH + LEAD + y


def polynomial(coefficients, t):
    value = coefficients[-1]
    for coefficient in coefficients[-2::-1]:
        value = value * t + coefficient
    return value


def twice_energy(a, b, c, d, e, f):
    trace = a + b + c
    middle = trace * (1.0 / 3.0)
    a, b, c = a - middle, b - middle, c - middle
    dd, ee, ff = d * d, e * e, f * f
    spread = (a * a + b * b + c * c) * (1.0 / 6.0) + (dd + ee + ff) * (1.0 / 3.0)
    guarded = spread + 4.0 * eigen_guard
    determinant = a * (b * c - ff) - d * (d * c - f * e) + e * (d * f - b * e)
    inverse = lax.rsqrt(guarded)
    ratio = determinant * (0.5 * inverse) * (inverse * inverse)
    size = jnp.minimum(jnp.abs(ratio), 1.0)
    radius = jnp.sqrt(spread)
    first = radius * polynomial(cos_third, size)
    first = jnp.where(ratio < 0.0, -first, first)
    rest = radius * (1.7320508075688772 * jnp.sqrt(1.0 - size)) * polynomial(sin_third, size)
    largest = jnp.maximum(middle + 2.0 * first, 0.0)
    base = middle - first
    second = jnp.maximum(base + rest, 0.0)
    third = jnp.maximum(base - rest, 0.0)
    volume = jnp.maximum(trace, 0.0)
    energy = 0.25 * (volume * volume) + 0.5 * (
        largest * largest + second * second + third * third
    )
    return energy, trace


def kernel(
    sizes, bx, by, cells,
    index_ref, loads_hbm, tough_ref, clamp_ref, load_ref, crack_ref,
    disp_ref, dam_ref, table_ref,
    u0, u1, df0, df1, kk0, kk1, lf, clamp_v, load_v, crack_v, g,
    pa, ra, pb, rb, pc, rc, pm, pcm, hx, hm, hcm, row_v, rows_v, wv, stage_u, stage_d, loads_ref,
    local_sem, m_send, m_recv, w_sem, o_send, o_recv, a_send, a_recv, b_send, b_recv, t_send, t_recv, s_send, s_recv,
):
    ns, nx, ny = sizes
    me_s = lax.axis_index("section")
    me_x = lax.axis_index("gx")
    me_y = lax.axis_index("gy")
    swapped = lax.rem(me_x, 2)

    def place(case, x):
        return case + lax.rem(x + 2, 2) * (1 - 2 * lax.rem(case, 2))

    me_v = place(me_s, me_x)

    def neighbour_id(dx, dy):
        return {"section": place(me_v, me_x + dx), "gx": me_x + dx, "gy": me_y + dy}

    nz = u0.shape[-1]
    us, dfs, kks = (u0, u1), (df0, df1), (kk0, kk1)

    copies = [
        pltpu.make_async_copy(source, target, local_sem.at[i])
        for i, (source, target) in enumerate(
            (
                (load_ref, load_v), (clamp_ref, clamp_v), (crack_ref, crack_v),
                (loads_hbm, loads_ref),
            )
        )
    ]
    for copy in copies:
        copy.start()

    halo_pieces = [(i * PITCH, 8) for i in range(bx + 2 * BORDER + 1)]
    halo_pieces += [(row_of(x, 0), by) for x in (-3, -2, -1, bx, bx + 1, bx + 2)]
    for start, size in halo_pieces:
        for ref in (u1,) + dfs:
            for i in range(ref.shape[0]):
                ref[i, pl.ds(start, size), :] = jnp.zeros((size, nz), jnp.float32)
        lf[0, pl.ds(start, size), :] = jnp.zeros((size, nz), jnp.float32)
        lf[1, pl.ds(start, size), :] = jnp.ones((size, nz), jnp.float32)
        for ref in kks:
            ref[pl.ds(start, size), :] = jnp.full((size, nz), outside_stiff, jnp.float32)

    def there(dx, dy):
        return (
            (me_x + dx >= 0) & (me_x + dx < nx) & (me_y + dy >= 0) & (me_y + dy < ny)
        )

    corners = ((-1, -1), (-1, 1), (1, -1), (1, 1))
    sides_x = ((-1, 0), (1, 0))
    sides_y = ((0, -1), (0, 1))
    neighbours = sides_x + sides_y + corners

    barrier = pltpu.get_barrier_semaphore()
    for dx, dy in neighbours:
        @pl.when(there(dx, dy))
        def _(dx=dx, dy=dy):
            pl.semaphore_signal(
                barrier, inc=1, device_id=neighbour_id(dx, dy), device_id_type=MESH
            )
    for r in range(1, ns):
        pl.semaphore_signal(
            barrier, inc=1, device_id={"section": lax.rem(me_s + r, ns)}, device_id_type=MESH
        )

    copies[3].wait()
    case = index_ref[0]
    for c in range(3):
        wv[0, c] = jnp.full((8, nz), loads_ref[c, case], jnp.float32)
    for i in (0, 1, 2):
        copies[i].wait()

    def begin(x, carry):
        here = pl.ds(row_of(x, 0), by)
        held = pl.ds(x * by, by)
        load = load_v[held, :].astype(jnp.float32)
        clamp = clamp_v[held, :].astype(jnp.float32)
        crack = crack_v[held, :].astype(jnp.float32)
        lf[0, here, :] = load
        lf[1, here, :] = jnp.maximum(load, clamp)
        df0[0, here, :] = crack
        kk0[here, :] = (1.0 - crack) * (1.0 - crack) + stiff_floor
        return carry

    lax.fori_loop(0, bx, begin, 0, unroll=4)

    for i in range(2):
        for ref, n, first in ((load_v, 3, 0), (crack_v, 2, 3), (clamp_v, 1, 5)):
            for layer in range(n):
                y = layer if i == 0 else by - n + layer
                pm[i, first + layer] = ref[pl.ds(y, bx, stride=by), :]
    for i, (dx, dy) in enumerate(corners):
        x, deep_x = (0, 1) if dx < 0 else (bx - 1, bx - 2)
        y, deep_y = (0, 1) if dy < 0 else (by - 1, by - 2)
        for j, (ref, at_x, at_y) in enumerate((
            (load_v, x, y), (load_v, deep_x, y), (load_v, x, deep_y), (crack_v, x, y),
        )):
            pcm[i, pl.ds(j, 1), :] = ref[pl.ds(at_x * by + at_y, 1), :]

    across = 1 + (me_x > 0).astype(jnp.int32) + (me_x < nx - 1).astype(jnp.int32)
    along = 1 + (me_y > 0).astype(jnp.int32) + (me_y < ny - 1).astype(jnp.int32)
    pl.semaphore_wait(barrier, across * along - 1 + (ns - 1))

    def remote(source, target, send, recv, dx, dy):
        return pltpu.make_async_remote_copy(
            src_ref=source, dst_ref=target, send_sem=send, recv_sem=recv,
            device_id=neighbour_id(dx, dy), device_id_type=MESH,
        )

    def b_copies(field, q, dx, dy):
        found = []
        if dy == 0:
            for layer in range(HALO):
                x = layer if dx < 0 else bx - HALO + layer
                to = bx + layer if dx < 0 else layer - HALO
                i = (0 if dx < 0 else 2) + layer
                found.append(remote(
                    field.at[:, pl.ds(row_of(x, 0), by), :],
                    field.at[:, pl.ds(row_of(to, 0), by), :],
                    b_send.at[q, i], b_recv.at[q, i], dx, dy,
                ))
        elif dx == 0:
            i = 0 if dy < 0 else 1
            found.append(remote(
                pb.at[i], rb.at[q, i], b_send.at[q, 4 + i], b_recv.at[q, 4 + i], dx, dy,
            ))
        else:
            i = corners.index((dx, dy))
            found.append(remote(
                pc.at[i], rc.at[q, i], b_send.at[q, 6 + i], b_recv.at[q, 6 + i], dx, dy,
            ))
        return found

    order_b = corners + sides_x + sides_y

    def send_b(field, q, current):
        for i, (dx, dy) in enumerate(corners):
            row = row_of(0 if dx < 0 else bx - 1, 0 if dy < 0 else by - 1)
            if current is not None:
                for c in range(3):
                    pc[i, pl.ds(c, 1), :] = current[c, pl.ds(row, 1), :]
            for f in range(2):
                pc[i, pl.ds(3 + f, 1), :] = field[f, pl.ds(row, 1), :]
        for i in range(2):
            for f in range(2):
                for layer in range(HALO):
                    y = layer if i == 0 else by - HALO + layer
                    pb[i, f * HALO + layer] = field[
                        f, pl.ds(row_of(0, y), bx, stride=PITCH), :
                    ]
        for dx, dy in order_b:
            @pl.when(there(dx, dy))
            def _(dx=dx, dy=dy):
                for copy in b_copies(field, q, dx, dy):
                    copy.start()

    def sent_b(field, q):
        for dx, dy in order_b:
            @pl.when(there(dx, dy))
            def _(dx=dx, dy=dy):
                for copy in b_copies(field, q, dx, dy):
                    copy.wait_send()

    def take_b(field, q, current, directions):
        for dx, dy in directions:
            @pl.when(there(-dx, -dy))
            def _(dx=dx, dy=dy):
                for copy in b_copies(field, q, dx, dy):
                    copy.wait_recv()
                if dx == 0:
                    i = 0 if dy < 0 else 1
                    for f in range(2):
                        for layer in range(HALO):
                            y = by + layer if i == 0 else layer - HALO
                            strip = pl.ds(row_of(0, y), bx, stride=PITCH)
                            value = rb[q, i, f * HALO + layer]
                            field[f, strip, :] = value
                            if current is not None and f == 0:
                                kks[q][strip, :] = (1.0 - value) * (1.0 - value) + stiff_floor
                elif dy != 0:
                    i = corners.index((dx, dy))
                    row = row_of(bx if dx < 0 else -1, by if dy < 0 else -1)
                    if current is not None:
                        for c in range(3):
                            current[c, pl.ds(row, 1), :] = rc[q, i, pl.ds(c, 1), :]
                        value = rc[q, i, pl.ds(3, 1), :]
                        kks[q][pl.ds(row, 1), :] = (1.0 - value) * (1.0 - value) + stiff_floor
                    for f in range(2):
                        field[f, pl.ds(row, 1), :] = rc[q, i, pl.ds(3 + f, 1), :]
        if directions is not corners:
            for x in (-2, -1, bx, bx + 1):
                here = pl.ds(row_of(x, 0), by)
                value = field[0, here, :]
                kks[q][here, :] = (1.0 - value) * (1.0 - value) + stiff_floor

    def a_copy(q, dx, dy):
        if dy == 0:
            i = 0 if dx < 0 else 1
            x, to = (1, bx + 1) if dx < 0 else (bx - 2, -2)
            return remote(
                us[q].at[:, pl.ds(row_of(x, 0), by), :],
                us[q].at[:, pl.ds(row_of(to, 0), by), :],
                a_send.at[q, i], a_recv.at[q, i], dx, dy,
            )
        i = 0 if dy < 0 else 1
        return remote(
            pa.at[i], ra.at[q, i], a_send.at[q, 2 + i], a_recv.at[q, 2 + i], dx, dy,
        )

    def send_a(q):
        for i in range(2):
            y = 1 if i == 0 else by - 2
            for c in range(3):
                pa[i, c] = us[q][c, pl.ds(row_of(0, y), bx, stride=PITCH), :]
        for dx, dy in sides_x + sides_y:
            @pl.when(there(dx, dy))
            def _(dx=dx, dy=dy):
                a_copy(q, dx, dy).start()

    def sent_a(q):
        for dx, dy in sides_x + sides_y:
            @pl.when(there(dx, dy))
            def _(dx=dx, dy=dy):
                a_copy(q, dx, dy).wait_send()

    def take_a(q):
        for dx, dy in sides_x + sides_y:
            @pl.when(there(-dx, -dy))
            def _(dx=dx, dy=dy):
                a_copy(q, dx, dy).wait_recv()
                if dx == 0:
                    i = 0 if dy < 0 else 1
                    y = by + 1 if i == 0 else -2
                    for c in range(3):
                        us[q][c, pl.ds(row_of(0, y), bx, stride=PITCH), :] = ra[q, i, c]

    def tough_target(r):
        return place(lax.rem(me_s + ns - r, ns), me_x)

    def tough_copy(r):
        return pltpu.make_async_remote_copy(
            src_ref=tough_ref, dst_ref=g.at[r], send_sem=t_send.at[r], recv_sem=t_recv.at[r],
            device_id={"section": tough_target(r)}, device_id_type=MESH,
        )

    def tough_arrived(r):
        pltpu.make_async_copy(tough_ref, g.at[r], t_recv.at[r]).wait()

    masks = (load_v, crack_v, clamp_v)
    layers = (3, 2, 1)
    parts = tuple((ref, n, sum(layers[:i])) for i, (ref, n) in enumerate(zip(masks, layers)))

    def m_copies(dx, dy):
        if dy == 0:
            i = 0 if dx < 0 else 1
            return [
                remote(
                    ref.at[pl.ds((0 if dx < 0 else bx - n) * by, n * by), :],
                    hx.at[i, pl.ds(first * by, n * by), :],
                    m_send.at[3 * i + j], m_recv.at[3 * i + j], dx, dy,
                )
                for j, (ref, n, first) in enumerate(parts)
            ]
        if dx == 0:
            i = 0 if dy < 0 else 1
            return [remote(pm.at[i], hm.at[i], m_send.at[6 + i], m_recv.at[6 + i], dx, dy)]
        i = corners.index((dx, dy))
        return [remote(pcm.at[i], hcm.at[i], m_send.at[8 + i], m_recv.at[8 + i], dx, dy)]

    for dx, dy in order_b:
        @pl.when(there(dx, dy))
        def _(dx=dx, dy=dy):
            for copy in m_copies(dx, dy):
                copy.start()
    partner = me_s + 1 - 2 * lax.rem(me_s, 2)
    w_copy = pltpu.make_async_remote_copy(
        src_ref=wv.at[0], dst_ref=wv.at[1], send_sem=w_sem.at[0], recv_sem=w_sem.at[1],
        device_id={"section": partner}, device_id_type=MESH,
    )
    w_copy.start()
    for r in range(ns):
        @pl.when(tough_target(r) == me_s)
        def _(r=r):
            pltpu.make_async_copy(tough_ref, g.at[r], t_recv.at[r]).start()

        @pl.when(tough_target(r) != me_s)
        def _(r=r):
            tough_copy(r).start()

    lane = lax.broadcasted_iota(jnp.int32, (by, nz), 1)
    at_low = lane == 0
    at_high = lane == nz - 1

    def from_low(value, edge):
        return jnp.where(at_low, edge, pltpu.roll(value, 1, 1))

    def from_high(value, edge):
        return jnp.where(at_high, edge, pltpu.roll(value, nz - 1, 1))

    def span(start, stride):
        return pl.ds(start, by) if stride == 1 else pl.ds(start, bx, stride=stride)

    def as_float(value):
        return value.astype(jnp.float32)

    def put_crack(where, crack):
        crack = as_float(crack)
        df0[0, where, :] = crack
        kk0[where, :] = (1.0 - crack) * (1.0 - crack) + stiff_floor

    def outward(low, n, layer, size):
        return size + layer if low else layer - n

    w_copy.wait_recv()
    narrow = [wv[swapped, c] for c in range(3)]

    def fill(x, carry):
        for here in (x * PITCH, x * PITCH + 8, x * PITCH + 16):
            load = lf[0, pl.ds(here, 8), :]
            for c in range(3):
                u0[c, pl.ds(here, 8), :] = load * narrow[c]
        return carry

    lax.fori_loop(0, bx + 2 * BORDER, fill, 0, unroll=2)
    tail = pl.ds((bx + 2 * BORDER) * PITCH, 8)
    for c in range(3):
        u0[c, tail, :] = lf[0, tail, :] * narrow[c]
    vector = [jnp.concatenate([v, v], axis=0) for v in narrow]

    def first_flow(start, stride, count):
        def at(offset, c):
            if stride == 1:
                return u0[c, pl.ds(start + offset, count), :]
            return u0[c, pl.ds(start + offset, count, stride=stride), :]

        to = pl.ds(start, count) if stride == 1 else pl.ds(start, count, stride=stride)
        value = at(0, 2)
        high = jnp.where(at_high[:count], 0.0, pltpu.roll(value, nz - 1, 1))
        low = jnp.where(at_low[:count], 0.0, pltpu.roll(value, 1, 1))
        trace = at(PITCH, 0) - at(-PITCH, 0) + at(1, 1) - at(-1, 1) + (high - low)
        df0[1, to, :] = kk0[to, :] * (0.5 * trace)

    def first_flow_own(x, carry):
        first_flow(row_of(x, 0), 1, by)
        return carry

    lax.fori_loop(1, bx - 1, first_flow_own, 0, unroll=2)
    for dx, dy in order_b:
        @pl.when(there(-dx, -dy))
        def _(dx=dx, dy=dy):
            for copy in m_copies(dx, dy):
                copy.wait_recv()
            if dy == 0:
                i, low = (0, True) if dx < 0 else (1, False)
                for layer in range(3):
                    here = pl.ds(row_of(outward(low, 3, layer, bx), 0), by)
                    lf[0, here, :] = as_float(hx[i, pl.ds(layer * by, by), :])
                for layer in range(2):
                    here = pl.ds(row_of(outward(low, 2, layer, bx), 0), by)
                    put_crack(here, hx[i, pl.ds((3 + layer) * by, by), :])
                near = 0 if low else 2
                here = pl.ds(row_of(bx if low else -1, 0), by)
                lf[1, here, :] = as_float(jnp.maximum(
                    hx[i, pl.ds(near * by, by), :], hx[i, pl.ds(5 * by, by), :]
                ))
            elif dx == 0:
                i, low = (0, True) if dy < 0 else (1, False)
                for layer in range(3):
                    y = outward(low, 3, layer, by)
                    lf[0, pl.ds(row_of(0, y), bx, stride=PITCH), :] = as_float(hm[i, layer])
                for layer in range(2):
                    y = outward(low, 2, layer, by)
                    put_crack(pl.ds(row_of(0, y), bx, stride=PITCH), hm[i, 3 + layer])
                near = 0 if low else 2
                y = by if low else -1
                lf[1, pl.ds(row_of(0, y), bx, stride=PITCH), :] = as_float(
                    jnp.maximum(hm[i, near], hm[i, 5])
                )
            else:
                i = corners.index((dx, dy))
                x, far_x = (bx, bx + 1) if dx < 0 else (-1, -2)
                y, far_y = (by, by + 1) if dy < 0 else (-1, -2)
                for j, (at_x, at_y) in enumerate(((x, y), (far_x, y), (x, far_y))):
                    lf[0, pl.ds(row_of(at_x, at_y), 1), :] = as_float(hcm[i, pl.ds(j, 1), :])
                put_crack(pl.ds(row_of(x, y), 1), hcm[i, pl.ds(3, 1), :])

    for x in (0, 1, 2, bx + 3, bx + 4, bx + 5):
        fill(x, 0)
    for x in range(bx + 2 * BORDER + 1):
        lead = pl.ds(x * PITCH, 8)
        for c in range(3):
            u0[c, lead, :] = lf[0, lead, :] * narrow[c]
    for x in (0, bx - 1):
        first_flow(row_of(x, 0), 1, by)
    for y in (0, by - 1):
        first_flow(row_of(0, y), PITCH, bx)
    for dx, dy in order_b:
        @pl.when(there(-dx, -dy))
        def _(dx=dx, dy=dy):
            xs = (bx, bx + 1) if dx < 0 else (-2, -1)
            ys = (by, by + 1) if dy < 0 else (-2, -1)
            if dy == 0:
                for x in xs:
                    first_flow(row_of(x, 0), 1, by)
            elif dx == 0:
                for y in ys:
                    first_flow(row_of(0, y), PITCH, bx)
            else:
                first_flow(row_of(bx if dx < 0 else -1, by if dy < 0 else -1), 1, 1)

    def move(p, start, stride):
        df, u, kk = dfs[p], us[p], kks[p]

        def at(ref, offset, *lead):
            return ref[(*lead, span(start + offset, stride), slice(None))]

        k = at(kk, 0)
        k_xm, k_xp = at(kk, -PITCH), at(kk, PITCH)
        k_ym, k_yp = at(kk, -1), at(kk, 1)
        k_zm, k_zp = from_low(k, outside_stiff), from_high(k, outside_stiff)
        pairs = (k_xm + k_xp, k_ym + k_yp, k_zm + k_zp)
        total = 6.0 * k + (pairs[0] + pairs[1] + pairs[2])
        w_xm, w_xp, w_ym, w_yp = k + k_xm, k + k_xp, k + k_ym, k + k_yp
        w_zm = jnp.where(at_low, 0.0, k + k_zm)
        w_zp = jnp.where(at_high, 0.0, k + k_zp)
        middle_flow = at(df, 0, 1)
        slopes = (
            at(df, PITCH, 1) - at(df, -PITCH, 1),
            at(df, 1, 1) - at(df, -1, 1),
            from_high(middle_flow, 0.0) - from_low(middle_flow, 0.0),
        )
        fixed = at(lf, 0, 1) > 0.5
        load = at(lf, 0, 0)
        squares = None
        for c in range(3):
            here = at(u, 0, c)
            total_c = (
                w_xm * at(u, -PITCH, c) + w_xp * at(u, PITCH, c)
                + w_ym * at(u, -1, c) + w_yp * at(u, 1, c)
                + w_zm * pltpu.roll(here, 1, 1) + w_zp * pltpu.roll(here, nz - 1, 1)
            )
            residual = total_c - total * here + 2.0 * slopes[c]
            relaxed = here + relax_weight * residual / (total + pairs[c])
            us[1 - p][c, span(start, stride), :] = jnp.where(fixed, load * vector[c], relaxed)
            square = residual * residual
            squares = square if squares is None else squares + square
        return jnp.where(fixed, 0.0, squares)

    def heal(p, r, start, stride, held):
        q = 1 - p
        df, u = dfs[p], us[q]

        def at(ref, offset, *lead):
            return ref[(*lead, span(start + offset, stride), slice(None))]

        grads = []
        for c in range(3):
            here = at(u, 0, c)
            grads.append((
                at(u, PITCH, c) - at(u, -PITCH, c),
                at(u, 1, c) - at(u, -1, c),
                from_high(here, 0.0) - from_low(here, 0.0),
            ))
        energy, trace = twice_energy(
            grads[0][0], grads[1][1], grads[2][2],
            0.5 * (grads[0][1] + grads[1][0]),
            0.5 * (grads[0][2] + grads[2][0]),
            0.5 * (grads[1][2] + grads[2][1]),
        )
        here = at(df, 0, 0)
        beside = (
            at(df, PITCH, 0) + at(df, -PITCH, 0) + at(df, 1, 0) + at(df, -1, 0)
            + from_high(here, 0.0) + from_low(here, 0.0)
        )
        rate = g[r, held, :]
        renewed = (energy + rate * beside) / (energy + 7.0 * rate)
        renewed = jnp.where(crack_v[held, :] > 0, 1.0, renewed)
        stiff = (1.0 - renewed) * (1.0 - renewed) + stiff_floor
        to = span(start, stride)
        dfs[q][0, to, :] = renewed
        dfs[q][1, to, :] = stiff * (0.5 * trace)
        kks[q][to, :] = stiff

    columns = lax.broadcasted_iota(jnp.int32, (1, nz), 1)
    y_of = lax.broadcasted_iota(jnp.int32, (by, nz), 0)
    at_rim = (y_of == 0) | (y_of == by - 1)

    def in_groups(low, high, body, total):
        steps = 2 if (high - low) % 2 == 0 else 1
        size = (high - low) // steps

        def step(i, total):
            for j in range(size):
                added = body(low + i * size + j)
                total = total if added is None else total + added
            return total

        return lax.fori_loop(0, steps, step, total)

    def sweep(r, p, table, first=False, last=False):
        q = 1 - p

        def move_slab(x):
            return move(p, row_of(x, 0), 1)

        def move_strip(y):
            return move(p, row_of(0, y), PITCH)

        def heal_slab(x):
            heal(p, r, row_of(x, 0), 1, pl.ds(x * by, by))

        def heal_strip(y):
            heal(p, r, row_of(0, y), PITCH, pl.ds(y, bx, stride=by))

        nothing = jnp.zeros((by, nz), jnp.float32)
        squares = in_groups(1, bx - 1, move_slab, nothing)
        tough_arrived(r)
        in_groups(2, bx - 2, heal_slab, 0)

        if not first:
            take_b(dfs[p], p, us[p], sides_x + sides_y)
        for x in (0, bx - 1):
            squares = squares + move_slab(x)
        squares = jnp.where(at_rim, 0.0, squares)
        for y in (0, by - 1):
            squares = squares + move_strip(y)

        def with_sums(table):
            total = jnp.sum(jnp.sum(squares, axis=0, keepdims=True), axis=1, keepdims=True)
            column = lax.rem(me_v + r, ns)
            return jnp.where(columns == column, jnp.broadcast_to(total, (1, nz)), table)

        if last:
            spread_sums(with_sums(table))
        if not first:
            sent_a(p)
        if not last:
            send_a(q)
        if not first:
            take_a(p)
            take_b(dfs[p], p, us[p], corners)
        for x in (-1, bx):
            move_slab(x)
        for y in (-1, by):
            move_strip(y)
        if last:
            give_displacement(us[q])
        for x in (0, 1, bx - 2, bx - 1):
            heal_slab(x)
        for y in (0, 1, by - 2, by - 1):
            heal_strip(y)
        if not first:
            sent_b(dfs[p], p)
        if not last:
            send_b(dfs[q], q, us[q])
            table = with_sums(table)
        else:
            give_damage(dfs[q])
        return table

    def give(stage, out_ref, i):
        return pltpu.make_async_remote_copy(
            src_ref=stage, dst_ref=out_ref.at[0], send_sem=o_send.at[i], recv_sem=o_recv.at[i],
            device_id={"section": partner}, device_id_type=MESH,
        )

    give_u = give(stage_u, disp_ref, 0)
    give_d = give(stage_d, dam_ref, 1)

    def give_displacement(u):
        @pl.when(swapped == 0)
        def _():
            for x in range(bx):
                for c in range(3):
                    disp_ref[0, c, x] = u[c, pl.ds(row_of(x, 0), by), :]

        @pl.when(swapped == 1)
        def _():
            for x in range(bx):
                for c in range(3):
                    stage_u[c, x] = u[c, pl.ds(row_of(x, 0), by), :]
            give_u.start()

    def give_damage(df):
        @pl.when(swapped == 0)
        def _():
            for x in range(bx):
                dam_ref[0, x] = df[0, pl.ds(row_of(x, 0), by), :]

        @pl.when(swapped == 1)
        def _():
            for x in range(bx):
                stage_d[x] = df[0, pl.ds(row_of(x, 0), by), :]
            give_d.start()

    me = me_x * ny + me_y

    def hops(offset):
        return sum(min(o, n - o) for o, n in zip(offset, (nx, ny)))

    offsets = sorted(
        ((tx, ty) for tx in range(nx) for ty in range(ny)), key=lambda o: (-hops(o), o)
    )

    def sums_copy(t):
        tx, ty = offsets[t]
        return pltpu.make_async_remote_copy(
            src_ref=row_v, dst_ref=rows_v.at[me], send_sem=s_send.at[t], recv_sem=s_recv.at[t],
            device_id={
                "section": me_v, "gx": lax.rem(me_x + tx, nx), "gy": lax.rem(me_y + ty, ny),
            },
            device_id_type=MESH,
        )

    def sums_arrived(t):
        tx, ty = offsets[t]
        source = lax.rem(me_x + nx - tx, nx) * ny + lax.rem(me_y + ny - ty, ny)
        pltpu.make_async_copy(row_v, rows_v.at[source], s_recv.at[t]).wait()

    here_t = nx * ny - 1

    def spread_sums(table):
        row_v[...] = table
        for t in range(here_t):
            sums_copy(t).start()

        @pl.when(swapped == 0)
        def _():
            rows_v[me] = table

        @pl.when(swapped == 1)
        def _():
            sums_copy(here_t).start()

    def two_sweeps(i, table):
        return sweep(2 * i + 2, 0, sweep(2 * i + 1, 1, table))

    table = sweep(0, 0, jnp.zeros((1, nz), jnp.float32), first=True)
    table = lax.fori_loop(0, (ns - 2) // 2, two_sweeps, table)
    sweep(ns - 1, 1, table, last=True)

    w_copy.wait_send()
    for dx, dy in order_b:
        @pl.when(there(dx, dy))
        def _(dx=dx, dy=dy):
            for copy in m_copies(dx, dy):
                copy.wait_send()

    for r in range(ns):
        @pl.when(tough_target(r) != me_s)
        def _(r=r):
            tough_copy(r).wait_send()

    @pl.when(swapped == 1)
    def _():
        sums_copy(here_t).wait_send()
        sums_arrived(here_t)
        for copy in (give_u, give_d):
            copy.wait_send()
            copy.wait_recv()

    for t in range(here_t):
        sums_copy(t).wait_send()
        sums_arrived(t)
    everything = rows_v[0]
    for i in range(1, nx * ny):
        everything = everything + rows_v[i]
    result = jnp.sqrt(everything * (0.25 / (3.0 * cells)))
    table_ref[...] = result[:, :ns]


def write_out(*refs):
    sources, targets, sem = refs[:3], refs[3:6], refs[6]
    copies = [
        pltpu.make_async_copy(source, target, sem.at[i])
        for i, (source, target) in enumerate(zip(sources, targets))
    ]
    for copy in copies:
        copy.start()
    for copy in copies:
        copy.wait()


def on_device(sizes, load_index, load_table, toughness, clamp_mask, load_mask, crack_mask):
    ns, nx, ny = sizes
    bx, by, nz = clamp_mask.shape
    cells = float(clamp_mask.size * nx * ny)
    rows = (bx + 2 * BORDER) * PITCH + LEAD
    flat = (bx * by, nz)
    f32 = jnp.float32
    scratch = [
        pltpu.VMEM((3, rows, nz), f32),
        pltpu.VMEM((3, rows, nz), f32),
        pltpu.VMEM((2, rows, nz), f32),
        pltpu.VMEM((2, rows, nz), f32),
        pltpu.VMEM((rows, nz), f32),
        pltpu.VMEM((rows, nz), f32),
        pltpu.VMEM((2, rows, nz), f32),
        pltpu.VMEM(flat, jnp.int32),
        pltpu.VMEM(flat, jnp.int32),
        pltpu.VMEM(flat, jnp.int32),
        pltpu.VMEM((ns, *flat), f32),
        pltpu.VMEM((2, 3, bx, nz), f32),
        pltpu.VMEM((2, 2, 3, bx, nz), f32),
        pltpu.VMEM((2, 2 * HALO, bx, nz), f32),
        pltpu.VMEM((2, 2, 2 * HALO, bx, nz), f32),
        pltpu.VMEM((4, 8, nz), f32),
        pltpu.VMEM((2, 4, 8, nz), f32),
        pltpu.VMEM((2, 6, bx, nz), jnp.int32),
        pltpu.VMEM((4, 8, nz), jnp.int32),
        pltpu.VMEM((2, 6 * by, nz), jnp.int32),
        pltpu.VMEM((2, 6, bx, nz), jnp.int32),
        pltpu.VMEM((4, 8, nz), jnp.int32),
        pltpu.VMEM((1, nz), f32),
        pltpu.VMEM((nx * ny, 1, nz), f32),
        pltpu.VMEM((2, 3, 8, nz), f32),
        pltpu.VMEM((3, bx, by, nz), f32),
        pltpu.VMEM((bx, by, nz), f32),
        pltpu.SMEM(load_table.shape[::-1], f32),
        pltpu.SemaphoreType.DMA((4,)),
        pltpu.SemaphoreType.DMA((12,)),
        pltpu.SemaphoreType.DMA((12,)),
        pltpu.SemaphoreType.DMA((2,)),
        pltpu.SemaphoreType.DMA((2,)),
        pltpu.SemaphoreType.DMA((2,)),
        pltpu.SemaphoreType.DMA((2, 4)),
        pltpu.SemaphoreType.DMA((2, 4)),
        pltpu.SemaphoreType.DMA((2, 10)),
        pltpu.SemaphoreType.DMA((2, 10)),
        pltpu.SemaphoreType.DMA((ns,)),
        pltpu.SemaphoreType.DMA((ns,)),
        pltpu.SemaphoreType.DMA((nx * ny,)),
        pltpu.SemaphoreType.DMA((nx * ny,)),
    ]
    vmem = pl.BlockSpec(memory_space=pltpu.VMEM)
    hbm = pl.BlockSpec(memory_space=pl.ANY)
    results = pl.pallas_call(
        functools.partial(kernel, sizes, bx, by, cells),
        out_shape=(
            pltpu.VMEM((1, 3, bx, by, nz), f32),
            pltpu.VMEM((1, bx, by, nz), f32),
            pltpu.VMEM((1, ns), f32),
        ),
        in_specs=[pl.BlockSpec(memory_space=pltpu.SMEM)] + [hbm] * 5,
        out_specs=(vmem, vmem, vmem),
        scratch_shapes=scratch,
        compiler_params=pltpu.CompilerParams(collective_id=0, has_side_effects=True),
        name="sweeps",
    )(
        load_index,
        load_table.T,
        toughness.reshape(flat),
        clamp_mask.reshape(flat),
        load_mask.reshape(flat),
        crack_mask.reshape(flat),
    )
    results = [pltpu.with_memory_space_constraint(value, pltpu.VMEM) for value in results]
    return pl.pallas_call(
        write_out,
        out_shape=tuple(pltpu.HBM(value.shape, f32) for value in results),
        in_specs=[vmem] * 3,
        out_specs=(hbm,) * 3,
        scratch_shapes=[pltpu.SemaphoreType.DMA((3,))],
        name="write_out",
    )(*results)


def solution(mesh):
    sizes = (mesh.shape["section"], mesh.shape["gx"], mesh.shape["gy"])
    in_specs = (
        P("section"),
        P(),
        P("section", "gx", "gy", None),
        P("gx", "gy", None),
        P("gx", "gy", None),
        P("gx", "gy", None),
    )
    out_specs = (
        P("section", None, "gx", "gy", None),
        P("section", "gx", "gy", None),
        P("section", None),
    )
    return jax.shard_map(
        functools.partial(on_device, sizes),
        mesh=mesh, in_specs=in_specs, out_specs=out_specs, check_vma=False,
    )
```
